32 devices in a mesh: dp: 4 (over y, x), row: 2 (over core), col: 4 (over z).
Axes of the slice: x: 2, y: 2, z: 4, core: 2. Of those that a mesh axis runs over, the one named last changes fastest.
Arguments:
- layer_input: bfloat16 [16384, 768], P(('dp', 'col'), 'row'), may hold values from -6 to 6
- lengths: int32 [8, 16], P('dp'), may hold values from 1 to 1024, 2048 in all within a row
- w_qkv: bfloat16 [768, 3, 768], P('col', None, 'row'), may hold values from -0.21875 to 0.21875
- bias_qv: bfloat16 [2, 768], P(None, ('row', 'col')), may hold values from -3 to 3
- w_out: bfloat16 [768, 768], P(('row', 'col')), may hold values from -0.875 to 0.875
- bias_out: bfloat16 [768], P(('row', 'col')), may hold values from -3 to 3
- gain_attn: bfloat16 [768], P(('row', 'col')), may hold values from 0.25 to 1.75
- shift_attn: bfloat16 [768], P(('row', 'col')), may hold values from -3 to 3
- w_in: bfloat16 [768, 3072], P('col', 'row'), may hold values from -0.21875 to 0.21875
- bias_in: bfloat16 [3072], P(('row', 'col')), may hold values from -3 to 3
- w_down: bfloat16 [3072, 768], P(('row', 'col')), may hold values from -0.109375 to 0.109375
- bias_down: bfloat16 [768], P(('row', 'col')), may hold values from -3 to 3
- gain_ffn: bfloat16 [768], P(('row', 'col')), may hold values from 0.25 to 1.75
- shift_ffn: bfloat16 [768], P(('row', 'col')), may hold values from -3 to 3
- cotangent: bfloat16 [16384, 768], P(('dp', 'col'), 'row'), may hold values from -6 to 6
Outputs:
- output: bfloat16 [16384, 768], P(('dp', 'col'), 'row')
- grad_input: float32 [16384, 768], P(('dp', 'col'), 'row')
- grad_w_qkv: float32 [768, 3, 768], P('col', None, 'row')
- grad_bias_qv: float32 [2, 768], P(None, ('row', 'col'))
- grad_w_out: float32 [768, 768], P(('row', 'col'))
- grad_bias_out: float32 [768], P(('row', 'col'))
- grad_gain_attn: float32 [768], P(('row', 'col'))
- grad_shift_attn: float32 [768], P(('row', 'col'))
- grad_w_in: float32 [768, 3072], P('col', 'row')
- grad_bias_in: float32 [3072], P(('row', 'col'))
- grad_w_down: float32 [3072, 768], P(('row', 'col'))
- grad_bias_down: float32 [768], P(('row', 'col'))
- grad_gain_ffn: float32 [768], P(('row', 'col'))
- grad_shift_ffn: float32 [768], P(('row', 'col'))
The draws below stay inside these ranges and needn't reach their ends.
Inputs may be any that keep to these rules, and one draw needn't show every extreme that they name: Row s gives, in order, the lengths of the 16 documents packed into sequence s; they sum to 2048, and in every row the longest is exactly half of 2048.
All inputs are finite; a program needn't handle non-finite values.
Results may differ from the reference program's by a relative error of at most 0.04.
Values may be sent and summed in bfloat16 or wider, within the bound.
A program may use at most 256 MiB of HBM per device.

```python
import math
import jax
import jax.numpy as jnp
import numpy as np
from jax import lax

D = 768
HEADS = 12
HD = 64
FF = 3072
LEN = 2048
DOCS = 16
SEQS = 8
TOKENS = 16384


def levels(rng, dims, shards, smallest, top_value):
    level, own = 1.0, jax.random.fold_in(rng, 6)
    for axis_at, shards_of in shards:
        heights = jnp.exp(jax.random.uniform(jax.random.fold_in(own, axis_at), (shards_of,), jnp.float32, smallest / len(shards), top_value / len(shards)))
        level = level * jnp.repeat(heights, dims[axis_at] // shards_of).reshape([-1 if axis == axis_at else 1 for axis in range(len(dims))])
    return level


def split_up(number_of, total, reach, slope):
    portions = [(1 << 20) // math.isqrt(grade ** slope) + 1 for grade in range(2, number_of + 1)]
    rest, holding = total - reach - (number_of - 1), [1] * (number_of - 1)
    while rest > 0:
        free = [i for i in range(number_of - 1) if holding[i] < reach]
        mass, remaining = sum([portions[i] for i in free]), rest
        for i in free:
            addition = min(reach - holding[i], max(1, remaining * portions[i] // mass), rest)
            holding[i] = holding[i] + addition
            rest = rest - addition
    return np.array([reach] + holding)


def ragged_sizes(key, number_of, total, most, slope):
    if number_of == 2:
        one = jax.random.randint(key, (), max(1, total - most), min(most, total - 1) + 1)
        return jnp.stack([one, total - one])
    sizes = jnp.asarray(split_up(number_of, total, most, slope), jnp.int32)
    twos = (number_of - 1) // 2
    donor, sink = sizes[1:1 + 2 * twos:2], sizes[2:2 + 2 * twos:2]
    slack = jnp.minimum(donor - 1, most - sink)
    shifted = jax.random.randint(jax.random.fold_in(key, 1), (twos,), 0, 1 << 20) % (slack + 1)
    sizes = sizes.at[1:1 + 2 * twos:2].set(donor - shifted).at[2:2 + 2 * twos:2].set(sink + shifted)
    return sizes[jax.random.permutation(jax.random.fold_in(key, 2), number_of)]


def normal_values(key, dims, scale, limit, cuts=(), held_as=jnp.bfloat16):
    values = jax.random.normal(key, dims, jnp.float32) * scale
    if len(cuts) > 0:
        values = levels(key, dims, cuts, -0.22, 0.18) * values
    return jnp.clip(values, min=-limit, max=limit).astype(held_as)


def setup_inputs(seed: int = 0) -> dict:
    key_of = jax.random.split(jax.random.key(seed), 16)
    layer_input = normal_values(key_of[0], (TOKENS, D), 1.0, 6.0, ((0, 16), (1, 2)))
    lengths = jax.vmap(lambda own: ragged_sizes(own, DOCS, LEN, LEN // 2, 2))(jax.random.split(key_of[1], SEQS)).reshape((SEQS, DOCS)).astype(jnp.int32)
    w_qkv = normal_values(key_of[2], (D, 3, D), D ** -0.5, 0.21875, ((0, 4), (2, 2)))
    bias_qv = normal_values(key_of[3], (2, D), 0.5, 3.0, ((1, 8),))
    w_out = normal_values(key_of[4], (D, D), (D // 16) ** -0.5, 0.875, ((0, 8),))
    bias_out = normal_values(key_of[5], (D,), 0.5, 3.0, ((0, 8),))
    gain_attn = jnp.clip(1.0 + 0.15 * jax.random.normal(key_of[6], (D,), jnp.float32), 0.25, 1.75).astype(jnp.bfloat16)
    shift_attn = normal_values(key_of[7], (D,), 0.5, 3.0, ((0, 8),))
    w_in = normal_values(key_of[8], (D, FF), D ** -0.5, 0.21875, ((0, 4), (1, 2)))
    bias_in = normal_values(key_of[9], (FF,), 0.5, 3.0, ((0, 8),))
    w_down = normal_values(key_of[10], (FF, D), FF ** -0.5, 0.109375, ((0, 8),))
    bias_down = normal_values(key_of[11], (D,), 0.5, 3.0, ((0, 8),))
    gain_ffn = jnp.clip(1.0 + 0.15 * jax.random.normal(key_of[12], (D,), jnp.float32), 0.25, 1.75).astype(jnp.bfloat16)
    shift_ffn = normal_values(key_of[13], (D,), 0.5, 3.0, ((0, 8),))
    cotangent = normal_values(key_of[14], (TOKENS, D), 1.0, 6.0, ((0, 16), (1, 2)))
    return {"layer_input": layer_input, "lengths": lengths, "w_qkv": w_qkv, "bias_qv": bias_qv, "w_out": w_out, "bias_out": bias_out, "gain_attn": gain_attn, "shift_attn": shift_attn, "w_in": w_in, "bias_in": bias_in, "w_down": w_down, "bias_down": bias_down, "gain_ffn": gain_ffn, "shift_ffn": shift_ffn, "cotangent": cotangent}


@jax.custom_vjp
def low(v):
    return lax.optimization_barrier(v.astype(jnp.bfloat16)).astype(jnp.float32)

@jax.custom_vjp
def low_back(v):
    return v

def low_keep(v):
    return (low(v), None)

def low_pass(kept, grad):
    return (grad,)

def back_keep(v):
    return (v, None)

def back_low(kept, grad):
    return (low(grad),)
low.defvjp(low_keep, low_pass)
low_back.defvjp(back_keep, back_low)
EPSILON = 1e-12
MASKED = -1e+30
PRECISE = lax.Precision.HIGHEST

def segment_ids(doc_lengths, seq_length):
    doc_ends = jnp.cumsum(doc_lengths)
    places = jnp.arange(seq_length, dtype=jnp.int32)
    return lax.optimization_barrier(jnp.sum((places[:, None] >= doc_ends[None, :]).astype(jnp.int32), axis=1))

def layer_norm(summed, gain_vec, shift_vec):
    center = lax.optimization_barrier(jnp.mean(summed, axis=-1, keepdims=True))
    centered = summed - center
    spread = lax.optimization_barrier(jnp.mean(centered * centered, axis=-1, keepdims=True))
    return centered * lax.rsqrt(spread + EPSILON) * gain_vec + shift_vec

def sequence_layer(params, seq_input, doc_lengths):
    w_qkv, bias_qv, w_out, bias_out, gain_attn, shift_attn, w_in, bias_in, w_down, bias_down, gain_ffn, shift_ffn = params
    qkv_vals = jnp.einsum('td,dke->tke', seq_input, w_qkv, precision=PRECISE)
    bias_rows = jnp.stack([bias_qv[0], jnp.zeros_like(bias_qv[0]), bias_qv[1]])
    qkv_vals = low(low_back(qkv_vals + bias_rows[None]))
    query_vals = qkv_vals[:, 0].reshape(LEN, HEADS, HD)
    key_vals = qkv_vals[:, 1].reshape(LEN, HEADS, HD)
    value_vals = qkv_vals[:, 2].reshape(LEN, HEADS, HD)
    seg_ids = segment_ids(doc_lengths, LEN)
    same_doc = seg_ids[:, None] == seg_ids[None, :]
    scores = jnp.einsum('qhd,khd->hqk', query_vals, key_vals, precision=PRECISE) * HD ** (-0.5)
    scores = low_back(scores)
    scores = jnp.where(same_doc[None], scores, MASKED)
    row_max = lax.optimization_barrier(jnp.max(scores, axis=-1, keepdims=True))
    raised = jnp.exp(scores - row_max)
    attn_weights = low(raised / lax.optimization_barrier(jnp.sum(raised, axis=-1, keepdims=True)))
    attended = jnp.einsum('hqk,khd->qhd', attn_weights, value_vals, precision=PRECISE).reshape(LEN, D)
    attended = low(low_back(attended))
    projected = low_back(jnp.dot(attended, w_out, precision=PRECISE))
    normed = layer_norm(seq_input + projected + bias_out, gain_attn, shift_attn)
    hidden = low_back(jnp.dot(low(normed), w_in, precision=PRECISE) + bias_in)
    activated = low(jax.nn.gelu(hidden, approximate=False))
    ffn_out = low_back(jnp.dot(activated, w_down, precision=PRECISE))
    return layer_norm(normed + ffn_out + bias_down, gain_ffn, shift_ffn)

def whole_layer(lengths):

    def layer_run(layer_input, *params):
        pieces = layer_input.reshape(SEQS, LEN, D)
        seq_layer = jax.checkpoint(sequence_layer)

        def scan_step(running, entries):
            return (running, seq_layer(params, entries[0], entries[1]))
        _, outputs = lax.scan(scan_step, jnp.zeros((), jnp.float32), (pieces, lengths))
        return outputs.reshape(SEQS * LEN, D)
    return layer_run

def reference(layer_input, lengths, w_qkv, bias_qv, w_out, bias_out, gain_attn, shift_attn, w_in, bias_in, w_down, bias_down, gain_ffn, shift_ffn, cotangent):
    floats = [value.astype(jnp.float32) for value in (layer_input, w_qkv, bias_qv, w_out, bias_out, gain_attn, shift_attn, w_in, bias_in, w_down, bias_down, gain_ffn, shift_ffn)]
    result, pullback = jax.vjp(whole_layer(lengths), *floats)
    gradients = pullback(cotangent.astype(jnp.float32))
    return (result.astype(jnp.bfloat16), gradients[0], gradients[1], gradients[2], gradients[3], gradients[4], gradients[5], gradients[6], gradients[7], gradients[8], gradients[9], gradients[10], gradients[11], gradients[12])
```

```python
import functools

import jax
import jax.numpy as jnp
from jax import lax
from jax.experimental import pallas as pl
from jax.experimental.pallas import tpu as pltpu
from jax.sharding import PartitionSpec as P

D = 768
HD = 64
LEN = 2048
WIDE = 384
LANES = 128

EPSILON = 1e-12
MASKED = -1e30
HALF_ROOT = 0.7071067811865476
DENSITY = 0.3989422804014327
BF = jnp.bfloat16
F32 = jnp.float32


def matmul(left_mat, right_mat):
    return jnp.dot(left_mat, right_mat, preferred_element_type=F32)


def left_inner(left_mat, right_mat):
    return lax.dot_general(
        left_mat, right_mat, (((0,), (0,)), ((), ())), preferred_element_type=F32
    )


def right_inner(left_mat, right_mat):
    return lax.dot_general(
        left_mat, right_mat, (((1,), (1,)), ((), ())), preferred_element_type=F32
    )


def swap(value):
    return lax.ppermute(value, "row", [(0, 1), (1, 0)])


def ordered(row, mine, other, axis):
    return jnp.where(
        row == 0,
        jnp.concatenate([mine, other], axis=axis),
        jnp.concatenate([other, mine], axis=axis),
    )


def half_of(value, which, axis):
    size = value.shape[axis] // 2
    return lax.dynamic_slice_in_dim(value, which * size, size, axis)


def to_tokens(value, row):
    return half_of(value, row, 0), swap(half_of(value, 1 - row, 0))


def to_features(value, row):
    other = swap(half_of(value, 1 - row, 1))
    return ordered(row, half_of(value, row, 1), other, 0)


def dp_swap(value, bit):
    count = lax.axis_size("dp")
    return lax.ppermute(value, "dp", [(i, i ^ bit) for i in range(count)])


def col_shift(value, step, reach):
    count = lax.axis_size("col")
    if step > 0:
        pairs = [(i, i + 1) for i in range(count - 1) if i + reach < count]
    else:
        pairs = [(i, i - 1) for i in range(1, count) if i - reach >= 0]
    return lax.ppermute(value, "col", pairs)


def col_gather(piece):
    count = lax.axis_size("col")
    if count > 4:
        return lax.all_gather(piece, "col", axis=0)
    rights, lefts = [piece], [piece]
    for _ in range(count - 1):
        rights.append(col_shift(rights[-1], 1, 1))
        lefts.append(col_shift(lefts[-1], -1, 1))
    slots = jnp.stack(rights[:0:-1] + [piece] + lefts[1:])
    return lax.dynamic_slice_in_dim(slots, count - 1 - lax.axis_index("col"), count, 0)


def dp_gather(first, second):
    first_x = dp_swap(first, 1)
    second_y = dp_swap(second, 2)
    first_pair = dp_swap(jnp.stack([first, first_x]), 2)
    second_pair = dp_swap(jnp.stack([second, second_y]), 1)
    own = lax.axis_index("dp")

    def place(relative):
        stacked = jnp.stack(relative)
        return jnp.stack(
            [lax.dynamic_index_in_dim(stacked, own ^ i, 0, keepdims=False) for i in range(4)]
        )

    return (
        place([first, first_x, first_pair[0], first_pair[1]]),
        place([second, second_pair[0], second_y, second_pair[1]]),
    )


def dp_scatter(first, second):
    own = lax.axis_index("dp")

    def part(value, relative):
        return lax.dynamic_index_in_dim(value, own ^ relative, 1, keepdims=False)

    def run(value, near, far):
        got = dp_swap(jnp.stack([part(value, near), part(value, 3)]), near)
        keep = part(value, 0).astype(F32) + got[0].astype(F32)
        give = (part(value, far).astype(F32) + got[1].astype(F32)).astype(BF)
        return (keep + dp_swap(give, far).astype(F32)).astype(BF)

    return run(first, 1, 2), run(second, 2, 1)


def col_scatter(value):
    count = lax.axis_size("col")
    own = lax.axis_index("col")
    if count > 4:
        return lax.psum_scatter(value, "col", scatter_dimension=0, tiled=False).astype(F32)

    def part(target):
        target = jnp.clip(target, 0, count - 1)
        return lax.dynamic_index_in_dim(value, target, 0, keepdims=False)

    total = part(own).astype(F32)
    for step in (1, -1):
        flow = None
        for reach in range(count - 1, 0, -1):
            term = part(own + step * reach)
            if flow is not None:
                term = (term.astype(F32) + flow.astype(F32)).astype(BF)
            flow = col_shift(term, step, reach)
        total = total + flow.astype(F32)
    return total


def reduce_all(packed):
    count, rows, width = packed.shape
    quarters = packed.reshape(count, 4, rows // 4, width)
    half = count // 2
    low, high = dp_scatter(quarters[:half], quarters[half:])
    piece = col_scatter(jnp.concatenate([low, high], axis=0)).astype(BF)
    cut = rows // 8
    first, second = dp_gather(piece[:cut], piece[cut:])
    return jnp.concatenate([first, second], axis=1).reshape(rows, width).astype(F32)


def stack_heads(value):
    lane = lax.broadcasted_iota(jnp.int32, value.shape, 1)
    zero = jnp.zeros_like(value)
    return jnp.concatenate(
        [jnp.where(lane < HD, value, zero), jnp.where(lane >= HD, value, zero)], axis=0
    )


def join_heads(value, block):
    lane = lax.broadcasted_iota(jnp.int32, (LANES, block), 0)
    return jnp.where(lane < HD, value[:, :block], value[:, block:]).T


def doubled(value):
    return jnp.concatenate([value, value], axis=1)


def mask_bias(key_place, first_key, past_key):
    places = key_place + lax.broadcasted_iota(jnp.int32, (key_place_rows(), first_key.shape[1]), 0)
    inside = (places >= first_key) & (places < past_key)
    return doubled(jnp.where(inside, 0.0, MASKED))


KEY_BLOCK = 256


def key_place_rows():
    return KEY_BLOCK


def copy_blocks(dest, own, others, rows):
    dest[:rows, :] = own[...]
    dest[rows:, :] = others[...]


def forward_kernel(
    blocks, table, q_ref, k_ref, v_ref, ko_ref, vo_ref, span_ref, out_ref, log_ref, keys, values
):
    rows = q_ref.shape[0]
    block = rows // blocks
    copy_blocks(keys, k_ref, ko_ref, rows)
    copy_blocks(values, v_ref, vo_ref, rows)
    slots = keys.shape[0] // KEY_BLOCK
    base = table[2 * blocks]

    for at in range(blocks):
        here = slice(at * block, (at + 1) * block)
        query = stack_heads((q_ref[here, :].astype(F32) * 0.125).astype(BF))
        first_key = span_ref[0:1, here]
        past_key = span_ref[1:2, here]

        def step(place, running):
            peak, total, summed = running
            slot = lax.rem(place - base + slots, slots)
            rows_at = pl.ds(pl.multiple_of(slot * KEY_BLOCK, KEY_BLOCK), KEY_BLOCK)
            scores = right_inner(keys[rows_at, :], query)
            scores = scores + mask_bias(place * KEY_BLOCK, first_key, past_key)
            higher = jnp.maximum(peak, jnp.max(scores, axis=0, keepdims=True))
            raised = jnp.exp(scores - higher)
            fade = jnp.exp(peak - higher)
            total = total * fade + jnp.sum(raised, axis=0, keepdims=True)
            summed = summed * fade + left_inner(values[rows_at, :], raised.astype(BF))
            return (higher, total, summed)

        init = (
            jnp.full((1, 2 * block), MASKED, F32),
            jnp.zeros((1, 2 * block), F32),
            jnp.zeros((LANES, 2 * block), F32),
        )
        peak, total, summed = lax.fori_loop(table[at], table[blocks + at], step, init)
        out_ref[here, :] = join_heads(summed / total, block).astype(BF)
        log_ref[:, at * 2 * block : (at + 1) * 2 * block] = jnp.broadcast_to(
            peak + jnp.log(total), (8, 2 * block)
        )


def backward_kernel(
    blocks,
    table,
    q_ref,
    k_ref,
    v_ref,
    ko_ref,
    vo_ref,
    span_ref,
    out_ref,
    log_ref,
    grad_ref,
    dq_ref,
    dk_ref,
    dv_ref,
    dko_ref,
    dvo_ref,
    keys,
    values,
    key_sum,
    value_sum,
):
    rows = q_ref.shape[0]
    block = rows // blocks
    copy_blocks(keys, k_ref, ko_ref, rows)
    copy_blocks(values, v_ref, vo_ref, rows)
    slots = keys.shape[0] // KEY_BLOCK
    base = table[2 * blocks]
    key_sum[...] = jnp.zeros_like(key_sum)
    value_sum[...] = jnp.zeros_like(value_sum)

    for at in range(blocks):
        here = slice(at * block, (at + 1) * block)
        query = stack_heads((q_ref[here, :].astype(F32) * 0.125).astype(BF))
        grad = stack_heads(grad_ref[here, :])
        along = (grad_ref[here, :].astype(F32) * out_ref[here, :].astype(F32)).T
        dots = jnp.concatenate(
            [
                jnp.sum(along[:HD], axis=0, keepdims=True),
                jnp.sum(along[HD:], axis=0, keepdims=True),
            ],
            axis=1,
        )
        logs = log_ref[0:1, at * 2 * block : (at + 1) * 2 * block]
        first_key = span_ref[0:1, here]
        past_key = span_ref[1:2, here]

        def step(place, summed):
            slot = lax.rem(place - base + slots, slots)
            rows_at = pl.ds(pl.multiple_of(slot * KEY_BLOCK, KEY_BLOCK), KEY_BLOCK)
            key = keys[rows_at, :]
            scores = right_inner(key, query)
            scores = scores + mask_bias(place * KEY_BLOCK, first_key, past_key)
            weights = jnp.exp(scores - logs)
            grad_weights = right_inner(values[rows_at, :], grad)
            value_sum[rows_at, :] += matmul(weights.astype(BF), grad)
            grad_scores = (weights * (grad_weights - dots)).astype(BF)
            key_sum[rows_at, :] += matmul(grad_scores, query)
            return summed + left_inner(key, grad_scores)

        summed = lax.fori_loop(
            table[at], table[blocks + at], step, jnp.zeros((LANES, 2 * block), F32)
        )
        dq_ref[here, :] = (join_heads(summed, block) * 0.125).astype(BF)

    dk_ref[...] = key_sum[:rows, :]
    dv_ref[...] = value_sum[:rows, :]
    dko_ref[...] = key_sum[rows:, :].astype(BF)
    dvo_ref[...] = value_sum[rows:, :].astype(BF)


def attention_specs(rows, others):
    return [
        pl.BlockSpec((rows, LANES), lambda g, t: (0, g)),
        pl.BlockSpec((rows, LANES), lambda g, t: (0, 3 + g)),
        pl.BlockSpec((rows, LANES), lambda g, t: (0, 6 + g)),
        pl.BlockSpec((others, LANES), lambda g, t: (0, g)),
        pl.BlockSpec((others, LANES), lambda g, t: (0, 3 + g)),
        pl.BlockSpec((8, rows), lambda g, t: (0, 0)),
    ]


def attend_forward(table, qkv, kv_others, spans, blocks):
    rows, others = qkv.shape[0], kv_others.shape[0]
    pairs = WIDE // LANES
    return pl.pallas_call(
        functools.partial(forward_kernel, blocks),
        out_shape=(
            jax.ShapeDtypeStruct((rows, WIDE), BF),
            jax.ShapeDtypeStruct((pairs * 8, 2 * rows), F32),
        ),
        grid_spec=pltpu.PrefetchScalarGridSpec(
            num_scalar_prefetch=1,
            grid=(pairs,),
            in_specs=attention_specs(rows, others),
            out_specs=(
                pl.BlockSpec((rows, LANES), lambda g, t: (0, g)),
                pl.BlockSpec((8, 2 * rows), lambda g, t: (g, 0)),
            ),
            scratch_shapes=[pltpu.VMEM((rows + others, LANES), BF)] * 2,
        ),
        cost_estimate=pl.CostEstimate(
            flops=8 * rows * LEN * WIDE, bytes_accessed=8 * rows * WIDE, transcendentals=0
        ),
        name="attend_forward",
    )(table, qkv, qkv, qkv, kv_others, kv_others, spans)


def attend_backward(table, qkv, kv_others, spans, out, logs, grad, blocks):
    rows, others = qkv.shape[0], kv_others.shape[0]
    pairs = WIDE // LANES
    by_pair = pl.BlockSpec((rows, LANES), lambda g, t: (0, g))
    by_pair_others = pl.BlockSpec((others, LANES), lambda g, t: (0, g))
    return pl.pallas_call(
        functools.partial(backward_kernel, blocks),
        out_shape=(
            jax.ShapeDtypeStruct((rows, WIDE), BF),
            jax.ShapeDtypeStruct((rows, WIDE), F32),
            jax.ShapeDtypeStruct((rows, WIDE), F32),
            jax.ShapeDtypeStruct((others, WIDE), BF),
            jax.ShapeDtypeStruct((others, WIDE), BF),
        ),
        grid_spec=pltpu.PrefetchScalarGridSpec(
            num_scalar_prefetch=1,
            grid=(pairs,),
            in_specs=attention_specs(rows, others)
            + [by_pair, pl.BlockSpec((8, 2 * rows), lambda g, t: (g, 0)), by_pair],
            out_specs=(by_pair, by_pair, by_pair, by_pair_others, by_pair_others),
            scratch_shapes=[pltpu.VMEM((rows + others, LANES), BF)] * 2
            + [pltpu.VMEM((rows + others, LANES), F32)] * 2,
        ),
        cost_estimate=pl.CostEstimate(
            flops=20 * rows * LEN * WIDE, bytes_accessed=16 * rows * WIDE, transcendentals=0
        ),
        name="attend_backward",
    )(table, qkv, qkv, qkv, kv_others, kv_others, spans, out, logs, grad)


def norm_forward(summed, gain_vec, shift_vec):
    center = jnp.mean(summed, axis=1, keepdims=True)
    centered = summed - center
    spread = jnp.mean(centered * centered, axis=1, keepdims=True)
    inv_scale = lax.rsqrt(spread + EPSILON)
    normed_hat = centered * inv_scale
    return (normed_hat * gain_vec + shift_vec, normed_hat, inv_scale)


def norm_backward(grad_vals, normed_hat, inv_scale, gain_vec):
    grad_hat = grad_vals * gain_vec
    return inv_scale * (
        grad_hat
        - jnp.mean(grad_hat, axis=1, keepdims=True)
        - normed_hat * jnp.mean(grad_hat * normed_hat, axis=1, keepdims=True)
    )


def gelu_value(hidden):
    return 0.5 * hidden * (1.0 + lax.erf(hidden * HALF_ROOT))


def gelu_slope(hidden):
    return (
        0.5 * (1.0 + lax.erf(hidden * HALF_ROOT))
        + hidden * jnp.exp(-0.5 * hidden * hidden) * DENSITY
    )


def lanes_to_rows(value):
    pieces = value.shape[2] // WIDE
    return jnp.concatenate(
        [value[:, :, i * WIDE : (i + 1) * WIDE] for i in range(pieces)], axis=1
    )


def rows_to_lanes(value, pieces):
    rows = value.shape[-2] // pieces
    return jnp.concatenate(
        [value[..., i * rows : (i + 1) * rows, :] for i in range(pieces)], axis=-1
    )


def dp_part(value, own, axis=0):
    size = value.shape[axis] // 4
    return lax.dynamic_slice_in_dim(value, own * size, size, axis)


def padded_rows(flat, rows):
    count, size = flat.shape
    return jnp.pad(flat, ((0, 0), (0, rows * WIDE - size))).reshape(count, rows, WIDE)


def body(
    layer_input,
    lengths,
    w_qkv,
    bias_qv,
    w_out,
    bias_out,
    gain_attn,
    shift_attn,
    w_in,
    bias_in,
    w_down,
    bias_down,
    gain_ffn,
    shift_ffn,
    cotangent,
):
    col_grid = lax.axis_size("col")
    rows = layer_input.shape[0]
    row = lax.axis_index("row")
    own_dp = lax.axis_index("dp")
    own_col = lax.axis_index("col")
    group = LEN // rows
    start_row = own_col * rows
    block = min(256, rows)
    blocks = rows // block

    qkv_piece = jnp.swapaxes(dp_part(w_qkv, own_dp), 0, 1)
    depth = qkv_piece.shape[1]
    vectors = jnp.concatenate(
        [
            bias_qv.reshape(-1),
            bias_out,
            gain_attn,
            shift_attn,
            bias_down,
            gain_ffn,
            shift_ffn,
            bias_in,
        ]
    )
    share = bias_out.shape[0]
    vector_rows = 16
    first_piece = jnp.concatenate(
        [qkv_piece.reshape(3 * depth, WIDE), padded_rows(vectors[None], vector_rows)[0]], axis=0
    )
    first_cols = col_gather(first_piece)
    vectors_col = first_cols[:, 3 * depth :].reshape(col_grid, vector_rows * WIDE)
    vectors_col = vectors_col[:, : vectors.shape[0]]
    vectors_both = swap(vectors_col)
    cut = 3 * depth // 2
    qkv_low_part, qkv_high_part = dp_gather(
        first_cols[:, :cut], first_cols[:, cut : 3 * depth]
    )
    qkv_parts = jnp.concatenate([qkv_low_part, qkv_high_part], axis=2)
    w_qkv_half = jnp.transpose(
        qkv_parts.reshape(4, col_grid, 3, depth, WIDE), (1, 0, 3, 2, 4)
    ).reshape(D, 3 * WIDE)

    def vector(at, count=1):
        mine = vectors_col[:, at * share : (at + count) * share].reshape(-1)
        other = vectors_both[:, at * share : (at + count) * share].reshape(-1)
        return mine.astype(F32), other.astype(F32)

    def whole_vector(at):
        mine, other = vector(at)
        return ordered(row, mine, other, 0)[None]

    bias_q = vectors_col[:, :share].reshape(-1).astype(F32)
    bias_v = vectors_col[:, share : 2 * share].reshape(-1).astype(F32)
    bias_out_f = whole_vector(2)
    gain_attn_f = whole_vector(3)
    shift_attn_f = whole_vector(4)
    bias_down_f = whole_vector(5)
    gain_ffn_f = whole_vector(6)
    shift_ffn_f = whole_vector(7)
    bias_in_mine, bias_in_other = vector(8, 4)

    input_full = ordered(row, layer_input, swap(layer_input), 1)
    input_tokens = half_of(input_full, row, 0).astype(F32)
    cot_mine, cot_other = to_tokens(cotangent, row)
    grad_out = ordered(row, cot_mine, cot_other, 1).astype(F32)

    bias_rows = jnp.concatenate([bias_q, jnp.zeros_like(bias_q), bias_v])
    qkv_low = (matmul(input_full, w_qkv_half) + bias_rows[None]).astype(BF)

    def group_perm(offset, back):
        pairs = []
        for i in range(col_grid):
            source = i // group * group + (i + offset) % group
            pairs.append((i, source) if back else (source, i))
        return pairs

    kv_local = qkv_low[:, WIDE:]
    kv_others = jnp.concatenate(
        [lax.ppermute(kv_local, "col", group_perm(j, False)) for j in range(1, group)], axis=0
    )

    down_rows = w_down.shape[0] // 4
    down_piece = lanes_to_rows(dp_part(w_down, own_dp)[None])[0]
    in_piece = lanes_to_rows(dp_part(w_in, own_dp)[None])[0]
    out_piece = lanes_to_rows(dp_part(w_out, own_dp)[None])[0]
    later_piece = jnp.concatenate([down_piece, in_piece, out_piece], axis=0)
    later_cols = col_gather(later_piece)
    cut_down = down_piece.shape[0]
    cut_in = cut_down + in_piece.shape[0]
    down_parts, in_parts = dp_gather(later_cols[:, :cut_down], later_cols[:, cut_down:])
    out_parts = in_parts[:, :, cut_in - cut_down :]
    in_parts = in_parts[:, :, : cut_in - cut_down]

    def whole_half(parts, pieces):
        joined = jnp.swapaxes(rows_to_lanes(parts, pieces), 0, 1)
        return joined.reshape(-1, joined.shape[-1])

    w_down_mine = whole_half(down_parts, w_down.shape[1] // WIDE)
    w_in_mine = whole_half(in_parts, w_in.shape[1] // WIDE)
    w_out_mine = whole_half(out_parts, w_out.shape[1] // WIDE)
    w_out_other, w_in_other, w_down_other = swap(w_out_mine), swap(w_in_mine), swap(w_down_mine)

    own_lengths = lax.dynamic_index_in_dim(lengths, start_row // LEN, 0, keepdims=False)
    ends = jnp.cumsum(own_lengths)
    first_place = start_row % LEN
    places = first_place + jnp.arange(rows, dtype=jnp.int32)
    past = places[:, None] >= ends[None, :]
    first_key = jnp.max(jnp.where(past, ends[None, :], 0), axis=1)
    past_key = jnp.min(jnp.where(past, LEN, ends[None, :]), axis=1)
    spans = jnp.pad(jnp.stack([first_key, past_key]), ((0, 6), (0, 0)))
    table = jnp.concatenate(
        [
            first_key[::block] // KEY_BLOCK,
            (past_key[block - 1 :: block] + (KEY_BLOCK - 1)) // KEY_BLOCK,
            (first_place // KEY_BLOCK)[None],
        ]
    ).astype(jnp.int32)

    attended, logs = attend_forward(table, qkv_low, kv_others, spans, blocks)
    att_mine, att_other = to_tokens(attended, row)

    projected = matmul(att_mine, w_out_mine) + matmul(att_other, w_out_other)
    first_sum = input_tokens + projected + bias_out_f
    normed, first_hat, first_scale = norm_forward(first_sum, gain_attn_f, shift_attn_f)
    normed_low = normed.astype(BF)
    hidden_mine = matmul(normed_low, w_in_mine) + bias_in_mine[None]
    hidden_other = matmul(normed_low, w_in_other) + bias_in_other[None]
    act_mine = gelu_value(hidden_mine).astype(BF)
    act_other = gelu_value(hidden_other).astype(BF)
    second_sum = (
        normed
        + matmul(act_mine, w_down_mine)
        + matmul(act_other, w_down_other)
        + bias_down_f
    )
    result, second_hat, second_scale = norm_forward(second_sum, gain_ffn_f, shift_ffn_f)
    result = to_features(result.astype(BF), row)

    grad_gain_ffn = jnp.sum(grad_out * second_hat, axis=0)
    grad_shift_ffn = jnp.sum(grad_out, axis=0)
    grad_second = norm_backward(grad_out, second_hat, second_scale, gain_ffn_f)
    grad_bias_down = jnp.sum(grad_second, axis=0)
    grad_ffn = grad_second.astype(BF)
    grad_hidden_mine = (right_inner(grad_ffn, w_down_mine) * gelu_slope(hidden_mine)).astype(BF)
    grad_hidden_other = (right_inner(grad_ffn, w_down_other) * gelu_slope(hidden_other)).astype(BF)
    grad_normed = (
        grad_second
        + right_inner(grad_hidden_mine, w_in_mine)
        + right_inner(grad_hidden_other, w_in_other)
    )
    grad_gain_attn = jnp.sum(grad_normed * first_hat, axis=0)
    grad_shift_attn = jnp.sum(grad_normed, axis=0)
    grad_first = norm_backward(grad_normed, first_hat, first_scale, gain_attn_f)
    grad_bias_out = jnp.sum(grad_first, axis=0)
    grad_proj = grad_first.astype(BF)
    grad_att_mine = right_inner(grad_proj, w_out_mine).astype(BF)
    grad_att_other = right_inner(grad_proj, w_out_other).astype(BF)
    grad_attended = ordered(row, grad_att_mine, swap(grad_att_other), 0)
    grad_first_features = to_features(grad_first, row)

    def both_tokens(mine, other):
        return (mine + swap(other.astype(BF)).astype(F32)).astype(BF)

    grad_down = both_tokens(left_inner(act_mine, grad_ffn), left_inner(act_other, grad_ffn))
    grad_in = both_tokens(
        left_inner(normed_low, grad_hidden_mine), left_inner(normed_low, grad_hidden_other)
    )
    grad_out_w = both_tokens(left_inner(att_mine, grad_proj), left_inner(att_other, grad_proj))
    by_row = jnp.stack(
        [
            grad_bias_out,
            grad_gain_attn,
            grad_shift_attn,
            grad_bias_down,
            grad_gain_ffn,
            grad_shift_ffn,
        ]
    )
    in_mine = jnp.sum(grad_hidden_mine, axis=0, dtype=F32)
    in_other = jnp.sum(grad_hidden_other, axis=0, dtype=F32)

    def vector_block(six, inner):
        split = jnp.swapaxes(six.reshape(6, col_grid, share), 0, 1).reshape(col_grid, -1)
        return jnp.concatenate([split, inner.reshape(col_grid, -1)], axis=1)

    vec_mine = vector_block(half_of(by_row, row, 1), in_mine)
    vec_other = vector_block(half_of(by_row, 1 - row, 1), in_other)
    vec_sum = (vec_mine + swap(vec_other)).astype(BF)

    down_grad_rows, in_grad_rows, out_grad_rows = 2 * w_down.shape[0], 4 * w_in.shape[0], 2 * w_out.shape[0]
    early_rows = down_grad_rows + in_grad_rows + out_grad_rows
    early_pad = 64 - early_rows % 64 if early_rows % 64 else 64
    early = jnp.concatenate(
        [
            lanes_to_rows(grad_down.reshape(col_grid, -1, D)),
            lanes_to_rows(grad_in.reshape(col_grid, -1, 4 * WIDE)),
            lanes_to_rows(grad_out_w.reshape(col_grid, -1, D)),
            padded_rows(vec_sum, early_pad),
        ],
        axis=1,
    )
    early_total = reduce_all(early)

    grad_query, key_own, value_own, key_others, value_others = attend_backward(
        table, qkv_low, kv_others, spans, attended, logs, grad_attended, blocks
    )
    for j in range(1, group):
        part = slice((j - 1) * rows, j * rows)
        perm = group_perm(j, True)
        key_own = key_own + lax.ppermute(key_others[part], "col", perm).astype(F32)
        value_own = value_own + lax.ppermute(value_others[part], "col", perm).astype(F32)
    grad_qkv = jnp.concatenate([grad_query, key_own.astype(BF), value_own.astype(BF)], axis=1)

    grad_w_qkv = left_inner(input_full, grad_qkv).astype(BF)
    bias_sums = jnp.sum(grad_qkv, axis=0, dtype=F32)
    bias_pair = jnp.stack([bias_sums[:WIDE], bias_sums[2 * WIDE :]])
    bias_pair = jnp.swapaxes(bias_pair.reshape(2, col_grid, share), 0, 1).reshape(col_grid, -1)
    late_rows = 3 * w_qkv.shape[0]
    late_pad = 64 - late_rows % 64 if late_rows % 64 else 64
    late = jnp.concatenate(
        [
            lanes_to_rows(grad_w_qkv.reshape(col_grid, -1, 3 * WIDE)),
            padded_rows(bias_pair.astype(BF), late_pad),
        ],
        axis=1,
    )
    late_total = reduce_all(late)

    partial = right_inner(grad_qkv, w_qkv_half)
    arrived = swap(half_of(partial, 1 - row, 1).astype(BF)).astype(F32)
    grad_input = grad_first_features + half_of(partial, row, 1) + arrived

    grad_down_own = rows_to_lanes(early_total[:down_grad_rows], 2)
    grad_in_own = rows_to_lanes(early_total[down_grad_rows : down_grad_rows + in_grad_rows], 4)
    grad_out_own = rows_to_lanes(early_total[down_grad_rows + in_grad_rows : early_rows], 2)
    vec_own = early_total[early_rows:].reshape(-1)
    vecs = [vec_own[i * share : (i + 1) * share] for i in range(6)]
    bias_in_own = vec_own[6 * share : 10 * share]
    qkv_own = rows_to_lanes(late_total[:late_rows], 3).reshape(w_qkv.shape)
    bias_own = late_total[late_rows:].reshape(-1)[: 2 * share].reshape(2, share)
    return (
        result,
        grad_input,
        qkv_own,
        bias_own,
        grad_out_own,
        vecs[0],
        vecs[1],
        vecs[2],
        grad_in_own,
        bias_in_own,
        grad_down_own,
        vecs[3],
        vecs[4],
        vecs[5],
    )


def solution(mesh):
    both = P(("row", "col"))
    specs = (
        P("col", None, "row"),
        P(None, ("row", "col")),
        P(("row", "col"), None),
        both,
        both,
        both,
        P("col", "row"),
        both,
        P(("row", "col"), None),
        both,
        both,
        both,
    )
    tokens = P(("dp", "col"), "row")
    return jax.shard_map(
        body,
        mesh=mesh,
        in_specs=(tokens, P("dp", None)) + specs + (tokens,),
        out_specs=(tokens, tokens) + specs,
        check_vma=False,
    )
```

```python
import functools

import jax
import jax.numpy as jnp
from jax import lax
from jax.experimental import pallas as pl
from jax.experimental.pallas import tpu as pltpu
from jax.sharding import PartitionSpec as P

D = 768
HD = 64
LEN = 2048
WIDE = 384
LANES = 128
PAIRS = WIDE // LANES

EPSILON = 1e-12
MASKED = -1e30
HALF_ROOT = 0.7071067811865476
DENSITY = 0.3989422804014327
BF = jnp.bfloat16
F32 = jnp.float32


def matmul(left_mat, right_mat):
    return jnp.dot(left_mat, right_mat, preferred_element_type=F32)


def left_inner(left_mat, right_mat):
    return lax.dot_general(
        left_mat, right_mat, (((0,), (0,)), ((), ())), preferred_element_type=F32
    )


def right_inner(left_mat, right_mat):
    return lax.dot_general(
        left_mat, right_mat, (((1,), (1,)), ((), ())), preferred_element_type=F32
    )


def swap(value):
    return lax.ppermute(value, "row", [(0, 1), (1, 0)])


def ordered(row, mine, other, axis):
    return jnp.where(
        row == 0,
        jnp.concatenate([mine, other], axis=axis),
        jnp.concatenate([other, mine], axis=axis),
    )


def half_of(value, which, axis):
    size = value.shape[axis] // 2
    return lax.dynamic_slice_in_dim(value, which * size, size, axis)


def to_tokens(value, row):
    return half_of(value, row, 0), swap(half_of(value, 1 - row, 0))


def to_features(value, row):
    other = swap(half_of(value, 1 - row, 1))
    return ordered(row, half_of(value, row, 1), other, 0)


def xor_swap(value, axis, mask):
    count = lax.axis_size(axis)
    return lax.ppermute(value, axis, [(i, i ^ mask) for i in range(count)])


def picked(parts, axis):
    stacked = jnp.stack(parts)
    own = lax.axis_index(axis)
    return [
        lax.dynamic_index_in_dim(stacked, own ^ i, 0, keepdims=False) for i in range(len(parts))
    ]


def gathered(value, axis):
    count = lax.axis_size(axis)
    if count > 4:
        return lax.all_gather(value, axis, axis=0)
    parts = [value] + [xor_swap(value, axis, k) for k in range(1, count)]
    return jnp.stack(picked(parts, axis))


def scattered(value, axis, dim):
    count = lax.axis_size(axis)
    if count > 4:
        return lax.psum_scatter(value, axis, scatter_dimension=dim, tiled=False).astype(F32)
    own = lax.axis_index(axis)

    def part(k):
        return lax.dynamic_index_in_dim(value, own ^ k, dim, keepdims=False)

    arrived = [xor_swap(part(k), axis, k) for k in range(1, count)]
    total = part(0).astype(F32)
    for one in arrived:
        total = total + one.astype(F32)
    return total


def reduce_all(quarters):
    ours = scattered(quarters, "dp", 1).astype(BF)
    piece = scattered(ours, "col", 0).astype(BF)
    return gathered(piece, "dp").reshape(-1, piece.shape[1]).astype(F32)


def quartered(packed):
    count, rows, width = packed.shape
    return packed.reshape(count, 4, rows // 4, width)


def stack_heads(value):
    lane = lax.broadcasted_iota(jnp.int32, value.shape, 1)
    zero = jnp.zeros_like(value)
    return jnp.concatenate(
        [jnp.where(lane < HD, value, zero), jnp.where(lane >= HD, value, zero)], axis=0
    )


def join_heads(value, block):
    lane = lax.broadcasted_iota(jnp.int32, (LANES, block), 0)
    return jnp.where(lane < HD, value[:, :block], value[:, block:]).T


def doubled(value):
    return jnp.concatenate([value, value], axis=1)


def mask_bias(key_place, first_key, past_key):
    places = key_place + lax.broadcasted_iota(jnp.int32, (key_place_rows(), first_key.shape[1]), 0)
    inside = (places >= first_key) & (places < past_key)
    return doubled(jnp.where(inside, 0.0, MASKED))


KEY_BLOCK = 256


def key_place_rows():
    return KEY_BLOCK


def copy_blocks(dest, own, others, rows):
    dest[:rows, :] = own[...]
    dest[rows:, :] = others[...]


def forward_kernel(
    blocks, table, q_ref, k_ref, v_ref, ko_ref, vo_ref, span_ref, out_ref, log_ref, keys, values
):
    rows = q_ref.shape[0]
    block = rows // blocks
    copy_blocks(keys, k_ref, ko_ref, rows)
    copy_blocks(values, v_ref, vo_ref, rows)
    slots = keys.shape[0] // KEY_BLOCK
    base = table[2 * blocks]

    for at in range(blocks):
        here = slice(at * block, (at + 1) * block)
        query = stack_heads((q_ref[here, :].astype(F32) * 0.125).astype(BF))
        first_key = span_ref[0:1, here]
        past_key = span_ref[1:2, here]

        def step(place, running):
            peak, total, summed = running
            slot = lax.rem(place - base + slots, slots)
            rows_at = pl.ds(pl.multiple_of(slot * KEY_BLOCK, KEY_BLOCK), KEY_BLOCK)
            scores = right_inner(keys[rows_at, :], query)
            scores = scores + mask_bias(place * KEY_BLOCK, first_key, past_key)
            higher = jnp.maximum(peak, jnp.max(scores, axis=0, keepdims=True))
            raised = jnp.exp(scores - higher)
            fade = jnp.exp(peak - higher)
            total = total * fade + jnp.sum(raised, axis=0, keepdims=True)
            summed = summed * fade + left_inner(values[rows_at, :], raised.astype(BF))
            return (higher, total, summed)

        init = (
            jnp.full((1, 2 * block), MASKED, F32),
            jnp.zeros((1, 2 * block), F32),
            jnp.zeros((LANES, 2 * block), F32),
        )
        peak, total, summed = lax.fori_loop(table[at], table[blocks + at], step, init)
        out_ref[here, :] = join_heads(summed / total, block).astype(BF)
        log_ref[:, at * 2 * block : (at + 1) * 2 * block] = jnp.broadcast_to(
            peak + jnp.log(total), (8, 2 * block)
        )


def backward_kernel(
    blocks,
    table,
    q_ref,
    k_ref,
    v_ref,
    ko_ref,
    vo_ref,
    span_ref,
    out_ref,
    log_ref,
    grad_ref,
    dq_ref,
    dk_ref,
    dv_ref,
    others_ref,
    keys,
    values,
    key_sum,
    value_sum,
):
    rows = q_ref.shape[0]
    block = rows // blocks
    copy_blocks(keys, k_ref, ko_ref, rows)
    copy_blocks(values, v_ref, vo_ref, rows)
    slots = keys.shape[0] // KEY_BLOCK
    base = table[2 * blocks]
    key_sum[...] = jnp.zeros_like(key_sum)
    value_sum[...] = jnp.zeros_like(value_sum)

    for at in range(blocks):
        here = slice(at * block, (at + 1) * block)
        query = stack_heads((q_ref[here, :].astype(F32) * 0.125).astype(BF))
        grad = stack_heads(grad_ref[here, :])
        along = (grad_ref[here, :].astype(F32) * out_ref[here, :].astype(F32)).T
        dots = jnp.concatenate(
            [
                jnp.sum(along[:HD], axis=0, keepdims=True),
                jnp.sum(along[HD:], axis=0, keepdims=True),
            ],
            axis=1,
        )
        logs = log_ref[0:1, at * 2 * block : (at + 1) * 2 * block]
        first_key = span_ref[0:1, here]
        past_key = span_ref[1:2, here]

        def step(place, summed):
            slot = lax.rem(place - base + slots, slots)
            rows_at = pl.ds(pl.multiple_of(slot * KEY_BLOCK, KEY_BLOCK), KEY_BLOCK)
            key = keys[rows_at, :]
            scores = right_inner(key, query)
            scores = scores + mask_bias(place * KEY_BLOCK, first_key, past_key)
            weights = jnp.exp(scores - logs)
            grad_weights = right_inner(values[rows_at, :], grad)
            value_sum[rows_at, :] += matmul(weights.astype(BF), grad)
            grad_scores = (weights * (grad_weights - dots)).astype(BF)
            key_sum[rows_at, :] += matmul(grad_scores, query)
            return summed + left_inner(key, grad_scores)

        summed = lax.fori_loop(
            table[at], table[blocks + at], step, jnp.zeros((LANES, 2 * block), F32)
        )
        dq_ref[here, :] = (join_heads(summed, block) * 0.125).astype(BF)

    dk_ref[...] = key_sum[:rows, :]
    dv_ref[...] = value_sum[:rows, :]
    others_ref[:, :LANES] = key_sum[rows:, :].astype(BF)
    others_ref[:, LANES:] = value_sum[rows:, :].astype(BF)


def attention_specs(rows, others, pair):
    return [
        pl.BlockSpec((rows, LANES), lambda g, t: (0, 3 * pair)),
        pl.BlockSpec((rows, LANES), lambda g, t: (0, 3 * pair + 1)),
        pl.BlockSpec((rows, LANES), lambda g, t: (0, 3 * pair + 2)),
        pl.BlockSpec((others, LANES), lambda g, t: (0, 0)),
        pl.BlockSpec((others, LANES), lambda g, t: (0, 1)),
        pl.BlockSpec((8, rows), lambda g, t: (0, 0)),
    ]


def attend_forward(table, qkv, kv_others, spans, blocks, pair):
    rows, others = qkv.shape[0], kv_others.shape[0]
    return pl.pallas_call(
        functools.partial(forward_kernel, blocks),
        out_shape=(
            jax.ShapeDtypeStruct((rows, LANES), BF),
            jax.ShapeDtypeStruct((8, 2 * rows), F32),
        ),
        grid_spec=pltpu.PrefetchScalarGridSpec(
            num_scalar_prefetch=1,
            grid=(1,),
            in_specs=attention_specs(rows, others, pair),
            out_specs=(
                pl.BlockSpec((rows, LANES), lambda g, t: (0, 0)),
                pl.BlockSpec((8, 2 * rows), lambda g, t: (0, 0)),
            ),
            scratch_shapes=[pltpu.VMEM((rows + others, LANES), BF)] * 2,
        ),
        cost_estimate=pl.CostEstimate(
            flops=8 * rows * LEN * LANES, bytes_accessed=8 * rows * LANES, transcendentals=0
        ),
        name="attend_forward",
    )(table, qkv, qkv, qkv, kv_others, kv_others, spans)


def attend_backward(table, qkv, kv_others, spans, out, logs, grad, blocks, pair):
    rows, others = qkv.shape[0], kv_others.shape[0]
    whole = pl.BlockSpec((rows, LANES), lambda g, t: (0, 0))
    mine = pl.BlockSpec((rows, LANES), lambda g, t: (0, pair))
    return pl.pallas_call(
        functools.partial(backward_kernel, blocks),
        out_shape=(
            jax.ShapeDtypeStruct((rows, LANES), BF),
            jax.ShapeDtypeStruct((rows, LANES), F32),
            jax.ShapeDtypeStruct((rows, LANES), F32),
            jax.ShapeDtypeStruct((others, 2 * LANES), BF),
        ),
        grid_spec=pltpu.PrefetchScalarGridSpec(
            num_scalar_prefetch=1,
            grid=(1,),
            in_specs=attention_specs(rows, others, pair)
            + [whole, pl.BlockSpec((8, 2 * rows), lambda g, t: (0, 0)), mine],
            out_specs=(
                whole,
                whole,
                whole,
                pl.BlockSpec((others, 2 * LANES), lambda g, t: (0, 0)),
            ),
            scratch_shapes=[pltpu.VMEM((rows + others, LANES), BF)] * 2
            + [pltpu.VMEM((rows + others, LANES), F32)] * 2,
        ),
        cost_estimate=pl.CostEstimate(
            flops=20 * rows * LEN * LANES, bytes_accessed=16 * rows * LANES, transcendentals=0
        ),
        name="attend_backward",
    )(table, qkv, qkv, qkv, kv_others, kv_others, spans, out, logs, grad)


def norm_forward(summed, gain_vec, shift_vec):
    center = jnp.mean(summed, axis=1, keepdims=True)
    centered = summed - center
    spread = jnp.mean(centered * centered, axis=1, keepdims=True)
    inv_scale = lax.rsqrt(spread + EPSILON)
    normed_hat = centered * inv_scale
    return (normed_hat * gain_vec + shift_vec, normed_hat, inv_scale)


def norm_backward(grad_vals, normed_hat, inv_scale, gain_vec):
    grad_hat = grad_vals * gain_vec
    return inv_scale * (
        grad_hat
        - jnp.mean(grad_hat, axis=1, keepdims=True)
        - normed_hat * jnp.mean(grad_hat * normed_hat, axis=1, keepdims=True)
    )


def gelu_value(hidden):
    return 0.5 * hidden * (1.0 + lax.erf(hidden * HALF_ROOT))


def gelu_slope(hidden):
    return (
        0.5 * (1.0 + lax.erf(hidden * HALF_ROOT))
        + hidden * jnp.exp(-0.5 * hidden * hidden) * DENSITY
    )


def lanes_to_rows(value):
    pieces = value.shape[2] // WIDE
    return jnp.concatenate(
        [value[:, :, i * WIDE : (i + 1) * WIDE] for i in range(pieces)], axis=1
    )


def rows_to_lanes(value, pieces):
    rows = value.shape[-2] // pieces
    return jnp.concatenate(
        [value[..., i * rows : (i + 1) * rows, :] for i in range(pieces)], axis=-1
    )


def dp_part(value, own, axis=0):
    size = value.shape[axis] // 4
    return lax.dynamic_slice_in_dim(value, own * size, size, axis)


def padded_rows(flat, rows):
    count, size = flat.shape
    return jnp.pad(flat, ((0, 0), (0, rows * WIDE - size))).reshape(count, rows, WIDE)


def body(
    layer_input,
    lengths,
    w_qkv,
    bias_qv,
    w_out,
    bias_out,
    gain_attn,
    shift_attn,
    w_in,
    bias_in,
    w_down,
    bias_down,
    gain_ffn,
    shift_ffn,
    cotangent,
):
    col_grid = lax.axis_size("col")
    rows = layer_input.shape[0]
    row = lax.axis_index("row")
    own_dp = lax.axis_index("dp")
    own_col = lax.axis_index("col")
    group = LEN // rows
    start_row = own_col * rows
    block = min(256, rows)
    blocks = rows // block

    qkv_piece = jnp.swapaxes(dp_part(w_qkv, own_dp), 0, 1)
    depth = qkv_piece.shape[1]
    vectors = jnp.concatenate(
        [
            bias_qv.reshape(-1),
            bias_out,
            gain_attn,
            shift_attn,
            bias_down,
            gain_ffn,
            shift_ffn,
            bias_in,
        ]
    )
    share = bias_out.shape[0]
    vector_rows = 16
    first_piece = jnp.concatenate(
        [qkv_piece.reshape(3 * depth, WIDE), padded_rows(vectors[None], vector_rows)[0]], axis=0
    )
    first_cols = gathered(first_piece, "col")
    vectors_col = first_cols[:, 3 * depth :].reshape(col_grid, vector_rows * WIDE)
    vectors_col = vectors_col[:, : vectors.shape[0]]
    vectors_both = swap(vectors_col)
    qkv_parts = gathered(first_cols[:, : 3 * depth], "dp")
    w_qkv_half = jnp.transpose(
        qkv_parts.reshape(4, col_grid, 3, depth, PAIRS, LANES), (1, 0, 3, 4, 2, 5)
    ).reshape(D, 3 * WIDE)

    def vector(at, count=1):
        mine = vectors_col[:, at * share : (at + count) * share].reshape(-1)
        other = vectors_both[:, at * share : (at + count) * share].reshape(-1)
        return mine.astype(F32), other.astype(F32)

    def whole_vector(at):
        mine, other = vector(at)
        return ordered(row, mine, other, 0)[None]

    bias_q = vectors_col[:, :share].reshape(-1).astype(F32)
    bias_v = vectors_col[:, share : 2 * share].reshape(-1).astype(F32)
    bias_out_f = whole_vector(2)
    gain_attn_f = whole_vector(3)
    shift_attn_f = whole_vector(4)
    bias_down_f = whole_vector(5)
    gain_ffn_f = whole_vector(6)
    shift_ffn_f = whole_vector(7)
    bias_in_mine, bias_in_other = vector(8, 4)

    input_full = ordered(row, layer_input, swap(layer_input), 1)
    input_tokens = half_of(input_full, row, 0).astype(F32)
    cot_mine, cot_other = to_tokens(cotangent, row)
    grad_out = ordered(row, cot_mine, cot_other, 1).astype(F32)

    bias_rows = jnp.stack(
        [
            bias_q.reshape(PAIRS, LANES),
            jnp.zeros((PAIRS, LANES), F32),
            bias_v.reshape(PAIRS, LANES),
        ],
        axis=1,
    ).reshape(-1)
    qkv_low = (matmul(input_full, w_qkv_half) + bias_rows[None]).astype(BF)

    def group_perm(offset, back):
        pairs = []
        for i in range(col_grid):
            source = i // group * group + (i + offset) % group
            pairs.append((i, source) if back else (source, i))
        return pairs

    kv_others = []
    for pair in range(PAIRS):
        kv_local = qkv_low[:, (3 * pair + 1) * LANES : (3 * pair + 3) * LANES]
        kv_others.append(
            jnp.concatenate(
                [lax.ppermute(kv_local, "col", group_perm(j, False)) for j in range(1, group)],
                axis=0,
            )
        )

    down_rows = w_down.shape[0] // 4
    down_piece = lanes_to_rows(dp_part(w_down, own_dp)[None])[0]
    in_piece = lanes_to_rows(dp_part(w_in, own_dp)[None])[0]
    out_piece = lanes_to_rows(dp_part(w_out, own_dp)[None])[0]
    later_piece = jnp.concatenate([down_piece, in_piece, out_piece], axis=0)
    later_parts = gathered(gathered(later_piece, "col"), "dp")
    cut_down = down_piece.shape[0]
    cut_in = cut_down + in_piece.shape[0]
    down_parts = later_parts[:, :, :cut_down]
    in_parts = later_parts[:, :, cut_down:cut_in]
    out_parts = later_parts[:, :, cut_in:]

    def whole_half(parts, pieces):
        joined = jnp.swapaxes(rows_to_lanes(parts, pieces), 0, 1)
        return joined.reshape(-1, joined.shape[-1])

    w_down_mine = whole_half(down_parts, w_down.shape[1] // WIDE)
    w_in_mine = whole_half(in_parts, w_in.shape[1] // WIDE)
    w_out_mine = whole_half(out_parts, w_out.shape[1] // WIDE)
    w_out_other, w_in_other, w_down_other = swap(w_out_mine), swap(w_in_mine), swap(w_down_mine)

    own_lengths = lax.dynamic_index_in_dim(lengths, start_row // LEN, 0, keepdims=False)
    ends = jnp.cumsum(own_lengths)
    first_place = start_row % LEN
    places = first_place + jnp.arange(rows, dtype=jnp.int32)
    past = places[:, None] >= ends[None, :]
    first_key = jnp.max(jnp.where(past, ends[None, :], 0), axis=1)
    past_key = jnp.min(jnp.where(past, LEN, ends[None, :]), axis=1)
    spans = jnp.pad(jnp.stack([first_key, past_key]), ((0, 6), (0, 0)))
    table = jnp.concatenate(
        [
            first_key[::block] // KEY_BLOCK,
            (past_key[block - 1 :: block] + (KEY_BLOCK - 1)) // KEY_BLOCK,
            (first_place // KEY_BLOCK)[None],
        ]
    ).astype(jnp.int32)

    attended = [
        attend_forward(table, qkv_low, kv_others[pair], spans, blocks, pair)
        for pair in range(PAIRS)
    ]
    att_mine, att_other = to_tokens(jnp.concatenate([out for out, _ in attended], axis=1), row)

    projected = matmul(att_mine, w_out_mine) + matmul(att_other, w_out_other)
    first_sum = input_tokens + projected + bias_out_f
    normed, first_hat, first_scale = norm_forward(first_sum, gain_attn_f, shift_attn_f)
    normed_low = normed.astype(BF)
    hidden_mine = matmul(normed_low, w_in_mine) + bias_in_mine[None]
    hidden_other = matmul(normed_low, w_in_other) + bias_in_other[None]
    act_mine = gelu_value(hidden_mine).astype(BF)
    act_other = gelu_value(hidden_other).astype(BF)
    second_sum = (
        normed
        + matmul(act_mine, w_down_mine)
        + matmul(act_other, w_down_other)
        + bias_down_f
    )
    result, second_hat, second_scale = norm_forward(second_sum, gain_ffn_f, shift_ffn_f)
    result = to_features(result.astype(BF), row)

    grad_gain_ffn = jnp.sum(grad_out * second_hat, axis=0)
    grad_shift_ffn = jnp.sum(grad_out, axis=0)
    grad_second = norm_backward(grad_out, second_hat, second_scale, gain_ffn_f)
    grad_bias_down = jnp.sum(grad_second, axis=0)
    grad_ffn = grad_second.astype(BF)
    grad_hidden_mine = (right_inner(grad_ffn, w_down_mine) * gelu_slope(hidden_mine)).astype(BF)
    grad_hidden_other = (right_inner(grad_ffn, w_down_other) * gelu_slope(hidden_other)).astype(BF)
    grad_normed = (
        grad_second
        + right_inner(grad_hidden_mine, w_in_mine)
        + right_inner(grad_hidden_other, w_in_other)
    )
    grad_gain_attn = jnp.sum(grad_normed * first_hat, axis=0)
    grad_shift_attn = jnp.sum(grad_normed, axis=0)
    grad_first = norm_backward(grad_normed, first_hat, first_scale, gain_attn_f)
    grad_bias_out = jnp.sum(grad_first, axis=0)
    grad_proj = grad_first.astype(BF)
    grad_att_mine = right_inner(grad_proj, w_out_mine).astype(BF)
    grad_att_other = right_inner(grad_proj, w_out_other).astype(BF)
    grad_attended = ordered(row, grad_att_mine, swap(grad_att_other), 0)
    grad_first_features = to_features(grad_first, row)

    def both_tokens(mine, other):
        return (mine + swap(other.astype(BF)).astype(F32)).astype(BF)

    grad_down = both_tokens(left_inner(act_mine, grad_ffn), left_inner(act_other, grad_ffn))
    grad_in = both_tokens(
        left_inner(normed_low, grad_hidden_mine), left_inner(normed_low, grad_hidden_other)
    )
    grad_out_w = both_tokens(left_inner(att_mine, grad_proj), left_inner(att_other, grad_proj))
    by_row = jnp.stack(
        [
            grad_bias_out,
            grad_gain_attn,
            grad_shift_attn,
            grad_bias_down,
            grad_gain_ffn,
            grad_shift_ffn,
        ]
    )
    in_mine = jnp.sum(grad_hidden_mine, axis=0, dtype=F32)
    in_other = jnp.sum(grad_hidden_other, axis=0, dtype=F32)

    def vector_block(six, inner):
        split = jnp.swapaxes(six.reshape(6, col_grid, share), 0, 1).reshape(col_grid, -1)
        return jnp.concatenate([split, inner.reshape(col_grid, -1)], axis=1)

    vec_mine = vector_block(half_of(by_row, row, 1), in_mine)
    vec_other = vector_block(half_of(by_row, 1 - row, 1), in_other)
    vec_sum = (vec_mine + swap(vec_other)).astype(BF)

    down_grad_rows, in_grad_rows, out_grad_rows = 2 * w_down.shape[0], 4 * w_in.shape[0], 2 * w_out.shape[0]
    early_rows = down_grad_rows + in_grad_rows + out_grad_rows
    early_pad = 64 - early_rows % 64 if early_rows % 64 else 64
    early = jnp.concatenate(
        [
            lanes_to_rows(grad_down.reshape(col_grid, -1, D)),
            lanes_to_rows(grad_in.reshape(col_grid, -1, 4 * WIDE)),
            lanes_to_rows(grad_out_w.reshape(col_grid, -1, D)),
            padded_rows(vec_sum, early_pad),
        ],
        axis=1,
    )
    early, grad_attended = lax.optimization_barrier((quartered(early), grad_attended))
    early_total = reduce_all(early)

    grad_pairs = []
    for pair in range(PAIRS):
        out, logs = attended[pair]
        grad_query, key_own, value_own, others = attend_backward(
            table, qkv_low, kv_others[pair], spans, out, logs, grad_attended, blocks, pair
        )
        for j in range(1, group):
            arrived = lax.ppermute(
                others[(j - 1) * rows : j * rows], "col", group_perm(j, True)
            ).astype(F32)
            key_own = key_own + arrived[:, :LANES]
            value_own = value_own + arrived[:, LANES:]
        grad_pairs += [grad_query, key_own.astype(BF), value_own.astype(BF)]
    grad_qkv = jnp.concatenate(grad_pairs, axis=1)

    grad_w_qkv = left_inner(input_full, grad_qkv).astype(BF)
    bias_sums = jnp.sum(grad_qkv, axis=0, dtype=F32).reshape(PAIRS, 3, LANES)
    bias_pair = jnp.stack([bias_sums[:, 0].reshape(-1), bias_sums[:, 2].reshape(-1)])
    bias_pair = jnp.swapaxes(bias_pair.reshape(2, col_grid, share), 0, 1).reshape(col_grid, -1)
    late_rows = 3 * w_qkv.shape[0]
    late_pad = 64 - late_rows % 64 if late_rows % 64 else 64
    late = jnp.concatenate(
        [
            lanes_to_rows(grad_w_qkv.reshape(col_grid, -1, 3 * WIDE)),
            padded_rows(bias_pair.astype(BF), late_pad),
        ],
        axis=1,
    )
    late_total = reduce_all(quartered(late))

    partial = right_inner(grad_qkv, w_qkv_half)
    arrived = swap(half_of(partial, 1 - row, 1).astype(BF)).astype(F32)
    grad_input = grad_first_features + half_of(partial, row, 1) + arrived

    grad_down_own = rows_to_lanes(early_total[:down_grad_rows], 2)
    grad_in_own = rows_to_lanes(early_total[down_grad_rows : down_grad_rows + in_grad_rows], 4)
    grad_out_own = rows_to_lanes(early_total[down_grad_rows + in_grad_rows : early_rows], 2)
    vec_own = early_total[early_rows:].reshape(-1)
    vecs = [vec_own[i * share : (i + 1) * share] for i in range(6)]
    bias_in_own = vec_own[6 * share : 10 * share]
    qkv_own = late_total[:late_rows].reshape(PAIRS, w_qkv.shape[0], 3, LANES)
    qkv_own = jnp.transpose(qkv_own, (1, 2, 0, 3)).reshape(w_qkv.shape)
    bias_own = late_total[late_rows:].reshape(-1)[: 2 * share].reshape(2, share)
    return (
        result,
        grad_input,
        qkv_own,
        bias_own,
        grad_out_own,
        vecs[0],
        vecs[1],
        vecs[2],
        grad_in_own,
        bias_in_own,
        grad_down_own,
        vecs[3],
        vecs[4],
        vecs[5],
    )


def solution(mesh):
    both = P(("row", "col"))
    specs = (
        P("col", None, "row"),
        P(None, ("row", "col")),
        P(("row", "col"), None),
        both,
        both,
        both,
        P("col", "row"),
        both,
        P(("row", "col"), None),
        both,
        both,
        both,
    )
    tokens = P(("dp", "col"), "row")
    return jax.shard_map(
        body,
        mesh=mesh,
        in_specs=(tokens, P("dp", None)) + specs + (tokens,),
        out_specs=(tokens, tokens) + specs,
        check_vma=False,
    )
```

```python
import functools

import jax
import jax.numpy as jnp
from jax import lax
from jax.experimental import pallas as pl
from jax.experimental.pallas import tpu as pltpu
from jax.sharding import PartitionSpec as P


D = 768
HD = 64
LEN = 2048
WIDE = 384
LANES = 128
PAIRS = WIDE // LANES

EPSILON = 1e-12
MASKED = -1e30
HALF_ROOT = 0.7071067811865476
DENSITY = 0.3989422804014327
BF = jnp.bfloat16
F32 = jnp.float32


def matmul(left_mat, right_mat):
    return jnp.dot(left_mat, right_mat, preferred_element_type=F32)


def left_inner(left_mat, right_mat):
    return lax.dot_general(
        left_mat, right_mat, (((0,), (0,)), ((), ())), preferred_element_type=F32
    )


def right_inner(left_mat, right_mat):
    return lax.dot_general(
        left_mat, right_mat, (((1,), (1,)), ((), ())), preferred_element_type=F32
    )


def swap(value):
    return lax.ppermute(value, "row", [(0, 1), (1, 0)])


def ordered(row, mine, other, axis):
    return jnp.where(
        row == 0,
        jnp.concatenate([mine, other], axis=axis),
        jnp.concatenate([other, mine], axis=axis),
    )


def half_of(value, which, axis):
    size = value.shape[axis] // 2
    return lax.dynamic_slice_in_dim(value, which * size, size, axis)


def to_tokens(value, row):
    return half_of(value, row, 0), swap(half_of(value, 1 - row, 0))


def to_features(value, row):
    other = swap(half_of(value, 1 - row, 1))
    return ordered(row, half_of(value, row, 1), other, 0)


def xor_swap(value, axis, mask):
    count = lax.axis_size(axis)
    return lax.ppermute(value, axis, [(i, i ^ mask) for i in range(count)])


def picked(parts, axis):
    stacked = jnp.stack(parts)
    own = lax.axis_index(axis)
    return [
        lax.dynamic_index_in_dim(stacked, own ^ i, 0, keepdims=False) for i in range(len(parts))
    ]


def gathered(value, axis):
    count = lax.axis_size(axis)
    if count > 4:
        return lax.all_gather(value, axis, axis=0)
    parts = [value] + [xor_swap(value, axis, k) for k in range(1, count)]
    return jnp.stack(picked(parts, axis))


def scattered(value, axis, dim):
    count = lax.axis_size(axis)
    if count > 4:
        return lax.psum_scatter(value, axis, scatter_dimension=dim, tiled=False).astype(F32)
    own = lax.axis_index(axis)

    def part(k):
        return lax.dynamic_index_in_dim(value, own ^ k, dim, keepdims=False)

    arrived = [xor_swap(part(k), axis, k) for k in range(1, count)]
    total = part(0).astype(F32)
    for one in arrived:
        total = total + one.astype(F32)
    return total


def two_level(piece, used):
    arrived = [xor_swap(piece, "col", k) for k in range(1, lax.axis_size("col"))]
    ours = jnp.stack([one[:used] for one in arrived])
    return arrived, [ours] + [xor_swap(ours, "dp", j) for j in range(1, 4)]


def reduce_all(quarters):
    own = lax.axis_index("dp")

    def part(k):
        return lax.dynamic_index_in_dim(quarters, own ^ k, 1, keepdims=False)

    arrived = []
    for k in range(1, 4):
        arrived.append(xor_swap(part(k), "dp", k))
    total = part(0).astype(F32)
    for one in arrived:
        total = total + one.astype(F32)
    piece = scattered(total.astype(BF), "col", 0).astype(BF)
    return [piece] + [xor_swap(piece, "dp", k) for k in range(1, 4)]


def places_of():
    return jnp.stack([lax.axis_index("col"), lax.axis_index("dp")]).astype(jnp.int32)


def at_rows(start, count):
    return pl.ds(pl.multiple_of(start, 16), count)


def local_call(kernel, places, inputs, outs):
    spec = pl.BlockSpec(memory_space=pltpu.VMEM)
    return pl.pallas_call(
        kernel,
        out_shape=outs,
        in_specs=[pl.BlockSpec(memory_space=pltpu.SMEM)] + [spec] * len(inputs),
        out_specs=jax.tree.map(lambda _: spec, outs),
        cost_estimate=pl.CostEstimate(flops=0, bytes_accessed=4 << 20, transcendentals=0),
    )(places, *inputs)


def qkv_kernel(places, own, *refs):
    parts, out = refs[:-1], refs[-1]
    col, dp = places[0], places[1]
    share = own.shape[1]
    depth = share // 4
    for kind in range(3):
        for pair in range(PAIRS):
            lanes = slice((3 * pair + kind) * LANES, (3 * pair + kind + 1) * LANES)
            source = slice(pair * LANES, (pair + 1) * LANES)
            out[at_rows(col * share, share), lanes] = own[kind, :, source]
            for j in range(4):
                for k in range(1, 4):
                    rows = at_rows((col ^ k) * share + (dp ^ j) * depth, depth)
                    out[rows, lanes] = parts[j][
                        k - 1, kind * depth : (kind + 1) * depth, source
                    ]


def later_kernel(places, own_down, own_in, own_out, *refs):
    parts, (down, inner, out) = refs[:-3], refs[-3:]
    col, dp = places[0], places[1]
    wide_rows, deep_rows, out_rows = own_down.shape[0], own_in.shape[0], own_out.shape[0]
    down[at_rows(col * wide_rows, wide_rows), :] = own_down[...]
    inner[at_rows(col * deep_rows, deep_rows), :] = own_in[...]
    out[at_rows(col * out_rows, out_rows), :] = own_out[...]
    for j in range(4):
        there = dp ^ j
        for k in range(1, 4):
            part = parts[j].at[k - 1]
            count, at = wide_rows // 4, 0
            rows = at_rows((col ^ k) * wide_rows + there * count, count)
            for i in range(2):
                down[rows, i * WIDE : (i + 1) * WIDE] = part[at : at + count, :]
                at += count
            count = deep_rows // 4
            rows = at_rows((col ^ k) * deep_rows + there * count, count)
            for i in range(4):
                inner[rows, i * WIDE : (i + 1) * WIDE] = part[at : at + count, :]
                at += count
            count = out_rows // 2
            rows = at_rows((col ^ k) * out_rows + lax.rem(there, 2) * count, count)
            lanes = pl.ds(pl.multiple_of(there // 2 * WIDE, LANES), WIDE)
            out[rows, lanes] = part[at : at + count, :]


def early_out_kernel(places, *refs):
    parts, (down, inner, out) = refs[:-3], refs[-3:]
    dp = places[1]
    for j in range(4):
        there = dp ^ j
        count, at = down.shape[0] // 4, 0
        for i in range(2):
            down[at_rows(there * count, count), i * WIDE : (i + 1) * WIDE] = parts[j][
                at : at + count, :
            ].astype(F32)
            at += count
        count = inner.shape[0] // 4
        for i in range(4):
            inner[at_rows(there * count, count), i * WIDE : (i + 1) * WIDE] = parts[j][
                at : at + count, :
            ].astype(F32)
            at += count
        count = out.shape[0] // 2
        lanes = pl.ds(pl.multiple_of(there // 2 * WIDE, LANES), WIDE)
        out[at_rows(lax.rem(there, 2) * count, count), lanes] = parts[j][
            at : at + count, :
        ].astype(F32)


def late_out_kernel(places, *refs):
    parts, out = refs[:-1], refs[-1]
    dp = places[1]
    count = out.shape[1] // 4
    for j in range(4):
        rows = at_rows((dp ^ j) * count, count)
        for pair in range(PAIRS):
            for kind in range(3):
                out[kind, rows, pair * LANES : (pair + 1) * LANES] = parts[j][
                    pair * count : (pair + 1) * count, kind * LANES : (kind + 1) * LANES
                ].astype(F32)


def quartered_rows(value, count):
    pieces = value.shape[1] // WIDE
    cut = value.reshape(count, 4, -1, value.shape[1])
    return jnp.concatenate(
        [cut[..., i * WIDE : (i + 1) * WIDE] for i in range(pieces)], axis=2
    )


def quartered_halves(value, count):
    cut = value.reshape(count, 2, -1, 2 * WIDE)
    return jnp.concatenate([cut[..., :WIDE], cut[..., WIDE:]], axis=1)


def quartered_vector(flat, rows):
    count, size = flat.shape
    return jnp.pad(flat, ((0, 0), (0, 4 * rows * WIDE - size))).reshape(count, 4, rows, WIDE)


def first_quarter(parts, rows):
    stacked = jnp.stack([one[-rows:] for one in parts])
    return lax.dynamic_index_in_dim(
        stacked, lax.axis_index("dp"), 0, keepdims=False
    ).astype(F32).reshape(-1)


def stack_heads(value):
    lane = lax.broadcasted_iota(jnp.int32, value.shape, 1)
    zero = jnp.zeros_like(value)
    return jnp.concatenate(
        [jnp.where(lane < HD, value, zero), jnp.where(lane >= HD, value, zero)], axis=0
    )


def join_heads(value, block):
    lane = lax.broadcasted_iota(jnp.int32, (LANES, block), 0)
    return jnp.where(lane < HD, value[:, :block], value[:, block:]).T


def doubled(value):
    return jnp.concatenate([value, value], axis=1)


def mask_bias(key_place, first_key, past_key):
    places = key_place + lax.broadcasted_iota(jnp.int32, (key_place_rows(), first_key.shape[1]), 0)
    inside = (places >= first_key) & (places < past_key)
    return doubled(jnp.where(inside, 0.0, MASKED))


KEY_BLOCK = 256


def key_place_rows():
    return KEY_BLOCK


def copy_blocks(dest, own, others, rows):
    dest[:rows, :] = own[...]
    dest[rows:, :] = others[...]


def forward_kernel(
    blocks, table, q_ref, k_ref, v_ref, ko_ref, vo_ref, span_ref, out_ref, log_ref, keys, values
):
    rows = q_ref.shape[0]
    block = rows // blocks
    copy_blocks(keys, k_ref, ko_ref, rows)
    copy_blocks(values, v_ref, vo_ref, rows)
    slots = keys.shape[0] // KEY_BLOCK
    base = table[2 * blocks]

    @pl.loop(0, blocks)
    def _(at):
        here = pl.ds(pl.multiple_of(at * block, block), block)
        wide = pl.ds(pl.multiple_of(at * 2 * block, 2 * block), 2 * block)
        query = stack_heads((q_ref[here, :].astype(F32) * 0.125).astype(BF))
        first_key = span_ref[0:1, here]
        past_key = span_ref[1:2, here]

        def step(place, running):
            peak, total, summed = running
            slot = lax.rem(place - base + slots, slots)
            rows_at = pl.ds(pl.multiple_of(slot * KEY_BLOCK, KEY_BLOCK), KEY_BLOCK)
            scores = right_inner(keys[rows_at, :], query)
            scores = scores + mask_bias(place * KEY_BLOCK, first_key, past_key)
            higher = jnp.maximum(peak, jnp.max(scores, axis=0, keepdims=True))
            raised = jnp.exp(scores - higher)
            fade = jnp.exp(peak - higher)
            total = total * fade + jnp.sum(raised, axis=0, keepdims=True)
            summed = summed * fade + left_inner(values[rows_at, :], raised.astype(BF))
            return (higher, total, summed)

        init = (
            jnp.full((1, 2 * block), MASKED, F32),
            jnp.zeros((1, 2 * block), F32),
            jnp.zeros((LANES, 2 * block), F32),
        )
        peak, total, summed = lax.fori_loop(table[at], table[blocks + at], step, init)
        out_ref[here, :] = join_heads(summed / total, block).astype(BF)
        log_ref[:, wide] = jnp.broadcast_to(
            peak + jnp.log(total), (8, 2 * block)
        )


def backward_kernel(
    blocks,
    table,
    q_ref,
    k_ref,
    v_ref,
    ko_ref,
    vo_ref,
    span_ref,
    out_ref,
    log_ref,
    grad_ref,
    dq_ref,
    dk_ref,
    dv_ref,
    others_ref,
    keys,
    values,
    key_sum,
    value_sum,
):
    rows = q_ref.shape[0]
    block = rows // blocks
    copy_blocks(keys, k_ref, ko_ref, rows)
    copy_blocks(values, v_ref, vo_ref, rows)
    slots = keys.shape[0] // KEY_BLOCK
    base = table[2 * blocks]
    key_sum[...] = jnp.zeros_like(key_sum)
    value_sum[...] = jnp.zeros_like(value_sum)

    @pl.loop(0, blocks)
    def _(at):
        here = pl.ds(pl.multiple_of(at * block, block), block)
        wide = pl.ds(pl.multiple_of(at * 2 * block, 2 * block), 2 * block)
        query = stack_heads((q_ref[here, :].astype(F32) * 0.125).astype(BF))
        grad = stack_heads(grad_ref[here, :])
        along = (grad_ref[here, :].astype(F32) * out_ref[here, :].astype(F32)).T
        dots = jnp.concatenate(
            [
                jnp.sum(along[:HD], axis=0, keepdims=True),
                jnp.sum(along[HD:], axis=0, keepdims=True),
            ],
            axis=1,
        )
        logs = log_ref[0:1, wide]
        first_key = span_ref[0:1, here]
        past_key = span_ref[1:2, here]

        def step(place, summed):
            slot = lax.rem(place - base + slots, slots)
            rows_at = pl.ds(pl.multiple_of(slot * KEY_BLOCK, KEY_BLOCK), KEY_BLOCK)
            key = keys[rows_at, :]
            scores = right_inner(key, query)
            scores = scores + mask_bias(place * KEY_BLOCK, first_key, past_key)
            weights = jnp.exp(scores - logs)
            grad_weights = right_inner(values[rows_at, :], grad)
            value_sum[rows_at, :] += matmul(weights.astype(BF), grad)
            grad_scores = (weights * (grad_weights - dots)).astype(BF)
            key_sum[rows_at, :] += matmul(grad_scores, query)
            return summed + left_inner(key, grad_scores)

        summed = lax.fori_loop(
            table[at], table[blocks + at], step, jnp.zeros((LANES, 2 * block), F32)
        )
        dq_ref[here, :] = (join_heads(summed, block) * 0.125).astype(BF)

    dk_ref[...] = key_sum[:rows, :]
    dv_ref[...] = value_sum[:rows, :]
    others_ref[:, :LANES] = key_sum[rows:, :].astype(BF)
    others_ref[:, LANES:] = value_sum[rows:, :].astype(BF)


def attention_specs(rows, others, pair):
    return [
        pl.BlockSpec((rows, LANES), lambda g, t: (0, 3 * pair)),
        pl.BlockSpec((rows, LANES), lambda g, t: (0, 3 * pair + 1)),
        pl.BlockSpec((rows, LANES), lambda g, t: (0, 3 * pair + 2)),
        pl.BlockSpec((others, LANES), lambda g, t: (0, 0)),
        pl.BlockSpec((others, LANES), lambda g, t: (0, 1)),
        pl.BlockSpec((8, rows), lambda g, t: (0, 0)),
    ]


def attend_forward(table, qkv, kv_others, spans, blocks, pair):
    rows, others = qkv.shape[0], kv_others.shape[0]
    return pl.pallas_call(
        functools.partial(forward_kernel, blocks),
        out_shape=(
            jax.ShapeDtypeStruct((rows, LANES), BF),
            jax.ShapeDtypeStruct((8, 2 * rows), F32),
        ),
        grid_spec=pltpu.PrefetchScalarGridSpec(
            num_scalar_prefetch=1,
            grid=(1,),
            in_specs=attention_specs(rows, others, pair),
            out_specs=(
                pl.BlockSpec((rows, LANES), lambda g, t: (0, 0)),
                pl.BlockSpec((8, 2 * rows), lambda g, t: (0, 0)),
            ),
            scratch_shapes=[pltpu.VMEM((rows + others, LANES), BF)] * 2,
        ),
        cost_estimate=pl.CostEstimate(
            flops=8 * rows * LEN * LANES, bytes_accessed=8 * rows * LANES, transcendentals=0
        ),
        name="attend_forward",
    )(table, qkv, qkv, qkv, kv_others, kv_others, spans)


def attend_backward(table, qkv, kv_others, spans, out, logs, grad, blocks, pair):
    rows, others = qkv.shape[0], kv_others.shape[0]
    whole = pl.BlockSpec((rows, LANES), lambda g, t: (0, 0))
    mine = pl.BlockSpec((rows, LANES), lambda g, t: (0, pair))
    return pl.pallas_call(
        functools.partial(backward_kernel, blocks),
        out_shape=(
            jax.ShapeDtypeStruct((rows, LANES), BF),
            jax.ShapeDtypeStruct((rows, LANES), F32),
            jax.ShapeDtypeStruct((rows, LANES), F32),
            jax.ShapeDtypeStruct((others, 2 * LANES), BF),
        ),
        grid_spec=pltpu.PrefetchScalarGridSpec(
            num_scalar_prefetch=1,
            grid=(1,),
            in_specs=attention_specs(rows, others, pair)
            + [whole, pl.BlockSpec((8, 2 * rows), lambda g, t: (0, 0)), mine],
            out_specs=(
                whole,
                whole,
                whole,
                pl.BlockSpec((others, 2 * LANES), lambda g, t: (0, 0)),
            ),
            scratch_shapes=[pltpu.VMEM((rows + others, LANES), BF)] * 2
            + [pltpu.VMEM((rows + others, LANES), F32)] * 2,
        ),
        cost_estimate=pl.CostEstimate(
            flops=20 * rows * LEN * LANES, bytes_accessed=16 * rows * LANES, transcendentals=0
        ),
        name="attend_backward",
    )(table, qkv, qkv, qkv, kv_others, kv_others, spans, out, logs, grad)


def norm_forward(summed, gain_vec, shift_vec):
    center = jnp.mean(summed, axis=1, keepdims=True)
    centered = summed - center
    spread = jnp.mean(centered * centered, axis=1, keepdims=True)
    inv_scale = lax.rsqrt(spread + EPSILON)
    normed_hat = centered * inv_scale
    return (normed_hat * gain_vec + shift_vec, normed_hat, inv_scale)


def norm_backward(grad_vals, normed_hat, inv_scale, gain_vec):
    grad_hat = grad_vals * gain_vec
    return inv_scale * (
        grad_hat
        - jnp.mean(grad_hat, axis=1, keepdims=True)
        - normed_hat * jnp.mean(grad_hat * normed_hat, axis=1, keepdims=True)
    )


def gelu_value(hidden):
    return 0.5 * hidden * (1.0 + lax.erf(hidden * HALF_ROOT))


def gelu_slope(hidden):
    return (
        0.5 * (1.0 + lax.erf(hidden * HALF_ROOT))
        + hidden * jnp.exp(-0.5 * hidden * hidden) * DENSITY
    )


def lanes_to_rows(value):
    pieces = value.shape[2] // WIDE
    return jnp.concatenate(
        [value[:, :, i * WIDE : (i + 1) * WIDE] for i in range(pieces)], axis=1
    )


def rows_to_lanes(value, pieces):
    rows = value.shape[-2] // pieces
    return jnp.concatenate(
        [value[..., i * rows : (i + 1) * rows, :] for i in range(pieces)], axis=-1
    )


def dp_part(value, own, axis=0):
    size = value.shape[axis] // 4
    return lax.dynamic_slice_in_dim(value, own * size, size, axis)


def padded_rows(flat, rows):
    count, size = flat.shape
    return jnp.pad(flat, ((0, 0), (0, rows * WIDE - size))).reshape(count, rows, WIDE)


def body(
    layer_input,
    lengths,
    w_qkv,
    bias_qv,
    w_out,
    bias_out,
    gain_attn,
    shift_attn,
    w_in,
    bias_in,
    w_down,
    bias_down,
    gain_ffn,
    shift_ffn,
    cotangent,
):
    col_grid = lax.axis_size("col")
    rows = layer_input.shape[0]
    row = lax.axis_index("row")
    own_dp = lax.axis_index("dp")
    own_col = lax.axis_index("col")
    group = LEN // rows
    start_row = own_col * rows
    block = min(256, rows)
    blocks = rows // block

    qkv_piece = jnp.swapaxes(dp_part(w_qkv, own_dp), 0, 1)
    depth = qkv_piece.shape[1]
    vectors = jnp.concatenate(
        [
            bias_qv.reshape(-1),
            bias_out,
            gain_attn,
            shift_attn,
            bias_down,
            gain_ffn,
            shift_ffn,
            bias_in,
        ]
    )
    share = bias_out.shape[0]
    vector_rows = 16
    first_piece = jnp.concatenate(
        [qkv_piece.reshape(3 * depth, WIDE), padded_rows(vectors[None], vector_rows)[0]], axis=0
    )
    places = places_of()
    if col_grid > 4:
        first_cols = gathered(first_piece, "col")
        vectors_col = first_cols[:, 3 * depth :]
        qkv_parts = gathered(first_cols[:, : 3 * depth], "dp")
        w_qkv_half = jnp.transpose(
            qkv_parts.reshape(4, col_grid, 3, depth, PAIRS, LANES), (1, 0, 3, 4, 2, 5)
        ).reshape(D, 3 * WIDE)
    else:
        first_arrived, first_parts = two_level(first_piece, 3 * depth)
        vectors_col = jnp.stack(
            picked([one[3 * depth :] for one in [first_piece] + first_arrived], "col")
        )
        w_qkv_half = local_call(
            qkv_kernel,
            places,
            [jnp.swapaxes(w_qkv, 0, 1)] + first_parts,
            jax.ShapeDtypeStruct((D, 3 * WIDE), BF),
        )
    vectors_col = vectors_col.reshape(col_grid, vector_rows * WIDE)[:, : vectors.shape[0]]
    vectors_both = swap(vectors_col)

    def vector(at, count=1):
        mine = vectors_col[:, at * share : (at + count) * share].reshape(-1)
        other = vectors_both[:, at * share : (at + count) * share].reshape(-1)
        return mine.astype(F32), other.astype(F32)

    def whole_vector(at):
        mine, other = vector(at)
        return ordered(row, mine, other, 0)[None]

    bias_q = vectors_col[:, :share].reshape(-1).astype(F32)
    bias_v = vectors_col[:, share : 2 * share].reshape(-1).astype(F32)
    bias_out_f = whole_vector(2)
    gain_attn_f = whole_vector(3)
    shift_attn_f = whole_vector(4)
    bias_down_f = whole_vector(5)
    gain_ffn_f = whole_vector(6)
    shift_ffn_f = whole_vector(7)
    bias_in_mine, bias_in_other = vector(8, 4)

    input_full = ordered(row, layer_input, swap(layer_input), 1)
    input_tokens = half_of(input_full, row, 0).astype(F32)
    cot_mine, cot_other = to_tokens(cotangent, row)
    grad_out = ordered(row, cot_mine, cot_other, 1).astype(F32)

    bias_rows = jnp.stack(
        [
            bias_q.reshape(PAIRS, LANES),
            jnp.zeros((PAIRS, LANES), F32),
            bias_v.reshape(PAIRS, LANES),
        ],
        axis=1,
    ).reshape(-1)
    qkv_low = (matmul(input_full, w_qkv_half) + bias_rows[None]).astype(BF)

    def group_perm(offset, back):
        pairs = []
        for i in range(col_grid):
            source = i // group * group + (i + offset) % group
            pairs.append((i, source) if back else (source, i))
        return pairs

    kv_others = []
    for pair in range(PAIRS):
        kv_local = qkv_low[:, (3 * pair + 1) * LANES : (3 * pair + 3) * LANES]
        kv_others.append(
            jnp.concatenate(
                [lax.ppermute(kv_local, "col", group_perm(j, False)) for j in range(1, group)],
                axis=0,
            )
        )

    down_piece = lanes_to_rows(dp_part(w_down, own_dp)[None])[0]
    in_piece = lanes_to_rows(dp_part(w_in, own_dp)[None])[0]
    if col_grid > 4:
        out_piece = lanes_to_rows(dp_part(w_out, own_dp)[None])[0]
        later_piece = jnp.concatenate([down_piece, in_piece, out_piece], axis=0)
        later_parts = gathered(gathered(later_piece, "col"), "dp")
        cut_down = down_piece.shape[0]
        cut_in = cut_down + in_piece.shape[0]

        def whole_half(parts, pieces):
            joined = jnp.swapaxes(rows_to_lanes(parts, pieces), 0, 1)
            return joined.reshape(-1, joined.shape[-1])

        w_down_mine = whole_half(later_parts[:, :, :cut_down], 2)
        w_in_mine = whole_half(later_parts[:, :, cut_down:cut_in], 4)
        w_out_mine = whole_half(later_parts[:, :, cut_in:], 2)
    else:
        out_half = w_out.shape[0] // 2
        out_piece = lax.dynamic_slice(
            w_out, (own_dp % 2 * out_half, own_dp // 2 * WIDE), (out_half, WIDE)
        )
        later_piece = jnp.concatenate([down_piece, in_piece, out_piece], axis=0)
        _, later_parts = two_level(later_piece, later_piece.shape[0])
        w_down_mine, w_in_mine, w_out_mine = local_call(
            later_kernel,
            places,
            [w_down, w_in, w_out] + later_parts,
            (
                jax.ShapeDtypeStruct((4 * w_down.shape[0], D), BF),
                jax.ShapeDtypeStruct((4 * w_in.shape[0], w_in.shape[1]), BF),
                jax.ShapeDtypeStruct((4 * w_out.shape[0], D), BF),
            ),
        )
    w_out_other, w_in_other, w_down_other = swap(w_out_mine), swap(w_in_mine), swap(w_down_mine)

    own_lengths = lax.dynamic_index_in_dim(lengths, start_row // LEN, 0, keepdims=False)
    ends = jnp.cumsum(own_lengths)
    first_place = start_row % LEN
    spots = first_place + jnp.arange(rows, dtype=jnp.int32)
    past = spots[:, None] >= ends[None, :]
    first_key = jnp.max(jnp.where(past, ends[None, :], 0), axis=1)
    past_key = jnp.min(jnp.where(past, LEN, ends[None, :]), axis=1)
    spans = jnp.pad(jnp.stack([first_key, past_key]), ((0, 6), (0, 0)))
    table = jnp.concatenate(
        [
            first_key[::block] // KEY_BLOCK,
            (past_key[block - 1 :: block] + (KEY_BLOCK - 1)) // KEY_BLOCK,
            (first_place // KEY_BLOCK)[None],
        ]
    ).astype(jnp.int32)

    attended = [
        attend_forward(table, qkv_low, kv_others[pair], spans, blocks, pair)
        for pair in range(PAIRS)
    ]
    att_mine, att_other = to_tokens(jnp.concatenate([out for out, _ in attended], axis=1), row)

    projected = matmul(att_mine, w_out_mine) + matmul(att_other, w_out_other)
    first_sum = input_tokens + projected + bias_out_f
    normed, first_hat, first_scale = norm_forward(first_sum, gain_attn_f, shift_attn_f)
    normed_low = normed.astype(BF)
    hidden_mine = matmul(normed_low, w_in_mine) + bias_in_mine[None]
    hidden_other = matmul(normed_low, w_in_other) + bias_in_other[None]
    act_mine = gelu_value(hidden_mine).astype(BF)
    act_other = gelu_value(hidden_other).astype(BF)
    second_sum = (
        normed
        + matmul(act_mine, w_down_mine)
        + matmul(act_other, w_down_other)
        + bias_down_f
    )
    result, second_hat, second_scale = norm_forward(second_sum, gain_ffn_f, shift_ffn_f)
    result = to_features(result.astype(BF), row)

    grad_gain_ffn = jnp.sum(grad_out * second_hat, axis=0)
    grad_shift_ffn = jnp.sum(grad_out, axis=0)
    grad_second = norm_backward(grad_out, second_hat, second_scale, gain_ffn_f)
    grad_bias_down = jnp.sum(grad_second, axis=0)
    grad_ffn = grad_second.astype(BF)
    grad_hidden_mine = (right_inner(grad_ffn, w_down_mine) * gelu_slope(hidden_mine)).astype(BF)
    grad_hidden_other = (right_inner(grad_ffn, w_down_other) * gelu_slope(hidden_other)).astype(BF)
    grad_normed = (
        grad_second
        + right_inner(grad_hidden_mine, w_in_mine)
        + right_inner(grad_hidden_other, w_in_other)
    )
    grad_gain_attn = jnp.sum(grad_normed * first_hat, axis=0)
    grad_shift_attn = jnp.sum(grad_normed, axis=0)
    grad_first = norm_backward(grad_normed, first_hat, first_scale, gain_attn_f)
    grad_bias_out = jnp.sum(grad_first, axis=0)
    grad_proj = grad_first.astype(BF)
    grad_att_mine = right_inner(grad_proj, w_out_mine).astype(BF)
    grad_att_other = right_inner(grad_proj, w_out_other).astype(BF)
    grad_attended = ordered(row, grad_att_mine, swap(grad_att_other), 0)
    grad_first_features = to_features(grad_first, row)

    def both_tokens(mine, other):
        return (mine + swap(other.astype(BF)).astype(F32)).astype(BF)

    grad_down = both_tokens(left_inner(act_mine, grad_ffn), left_inner(act_other, grad_ffn))
    grad_in = both_tokens(
        left_inner(normed_low, grad_hidden_mine), left_inner(normed_low, grad_hidden_other)
    )
    grad_out_w = both_tokens(left_inner(att_mine, grad_proj), left_inner(att_other, grad_proj))
    by_row = jnp.stack(
        [
            grad_bias_out,
            grad_gain_attn,
            grad_shift_attn,
            grad_bias_down,
            grad_gain_ffn,
            grad_shift_ffn,
        ]
    )
    in_mine = jnp.sum(grad_hidden_mine, axis=0, dtype=F32)
    in_other = jnp.sum(grad_hidden_other, axis=0, dtype=F32)

    def vector_block(six, inner):
        split = jnp.swapaxes(six.reshape(6, col_grid, share), 0, 1).reshape(col_grid, -1)
        return jnp.concatenate([split, inner.reshape(col_grid, -1)], axis=1)

    vec_mine = vector_block(half_of(by_row, row, 1), in_mine)
    vec_other = vector_block(half_of(by_row, 1 - row, 1), in_other)
    vec_sum = (vec_mine + swap(vec_other)).astype(BF)

    vec_pad = 16
    early = jnp.concatenate(
        [
            quartered_rows(grad_down, col_grid),
            quartered_rows(grad_in, col_grid),
            quartered_halves(grad_out_w, col_grid)
            if col_grid <= 4
            else quartered_rows(grad_out_w, col_grid),
            quartered_vector(vec_sum, vec_pad),
        ],
        axis=2,
    )
    early, grad_attended = lax.optimization_barrier((early, grad_attended))
    early_parts = reduce_all(early)

    grad_pairs = []
    for pair in range(PAIRS):
        out, logs = attended[pair]
        grad_query, key_own, value_own, others = attend_backward(
            table, qkv_low, kv_others[pair], spans, out, logs, grad_attended, blocks, pair
        )
        for j in range(1, group):
            arrived = lax.ppermute(
                others[(j - 1) * rows : j * rows], "col", group_perm(j, True)
            ).astype(F32)
            key_own = key_own + arrived[:, :LANES]
            value_own = value_own + arrived[:, LANES:]
        grad_pairs += [grad_query, key_own.astype(BF), value_own.astype(BF)]
    grad_qkv = jnp.concatenate(grad_pairs, axis=1)

    grad_w_qkv = left_inner(input_full, grad_qkv).astype(BF)
    bias_sums = jnp.sum(grad_qkv, axis=0, dtype=F32).reshape(PAIRS, 3, LANES)
    bias_pair = jnp.stack([bias_sums[:, 0].reshape(-1), bias_sums[:, 2].reshape(-1)])
    bias_pair = jnp.swapaxes(bias_pair.reshape(2, col_grid, share), 0, 1).reshape(col_grid, -1)
    late = jnp.concatenate(
        [
            quartered_rows(grad_w_qkv, col_grid),
            quartered_vector(bias_pair.astype(BF), vec_pad),
        ],
        axis=2,
    )
    late_parts = reduce_all(late)

    partial = right_inner(grad_qkv, w_qkv_half)
    arrived = swap(half_of(partial, 1 - row, 1).astype(BF)).astype(F32)
    grad_input = grad_first_features + half_of(partial, row, 1) + arrived

    if col_grid > 4:
        early_all = jnp.stack(picked(early_parts, "dp")).astype(F32)
        late_all = jnp.stack(picked(late_parts, "dp")).astype(F32)
        cut_down = 2 * w_down.shape[0] // 4
        cut_in = cut_down + w_in.shape[0]
        grad_down_own = rows_to_lanes(early_all[:, :cut_down], 2).reshape(w_down.shape)
        grad_in_own = rows_to_lanes(early_all[:, cut_down:cut_in], 4).reshape(w_in.shape)
        grad_out_own = rows_to_lanes(early_all[:, cut_in:-vec_pad], 2).reshape(w_out.shape)
        qkv_own = late_all[:, :-vec_pad].reshape(4, PAIRS, depth, 3, LANES)
        qkv_own = jnp.transpose(qkv_own, (0, 2, 3, 1, 4)).reshape(w_qkv.shape)
    else:
        grad_down_own, grad_in_own, grad_out_own = local_call(
            early_out_kernel,
            places,
            early_parts,
            tuple(jax.ShapeDtypeStruct(one.shape, F32) for one in (w_down, w_in, w_out)),
        )
        qkv_own = local_call(
            late_out_kernel,
            places,
            late_parts,
            jax.ShapeDtypeStruct((3, w_qkv.shape[0], WIDE), F32),
        )
        qkv_own = jnp.swapaxes(qkv_own, 0, 1)
    vec_own = first_quarter(early_parts, vec_pad)
    vecs = [vec_own[i * share : (i + 1) * share] for i in range(6)]
    bias_in_own = vec_own[6 * share : 10 * share]
    bias_own = first_quarter(late_parts, vec_pad)[: 2 * share].reshape(2, share)
    return (
        result,
        grad_input,
        qkv_own,
        bias_own,
        grad_out_own,
        vecs[0],
        vecs[1],
        vecs[2],
        grad_in_own,
        bias_in_own,
        grad_down_own,
        vecs[3],
        vecs[4],
        vecs[5],
    )


def solution(mesh):
    both = P(("row", "col"))
    specs = (
        P("col", None, "row"),
        P(None, ("row", "col")),
        P(("row", "col"), None),
        both,
        both,
        both,
        P("col", "row"),
        both,
        P(("row", "col"), None),
        both,
        both,
        both,
    )
    tokens = P(("dp", "col"), "row")
    return jax.shard_map(
        body,
        mesh=mesh,
        in_specs=(tokens, P("dp", None)) + specs + (tokens,),
        out_specs=(tokens, tokens) + specs,
        check_vma=False,
    )
```

```python
import functools

import jax
import jax.numpy as jnp
from jax import lax
from jax.experimental import pallas as pl
from jax.experimental.pallas import tpu as pltpu
from jax.sharding import PartitionSpec as P


D = 768
HD = 64
LEN = 2048
WIDE = 384
LANES = 128
PAIRS = WIDE // LANES

EPSILON = 1e-12
MASKED = -1e30
HALF_ROOT = 0.7071067811865476
DENSITY = 0.3989422804014327
BF = jnp.bfloat16
F32 = jnp.float32


def matmul(left_mat, right_mat):
    return jnp.dot(left_mat, right_mat, preferred_element_type=F32)


def left_inner(left_mat, right_mat):
    return lax.dot_general(
        left_mat, right_mat, (((0,), (0,)), ((), ())), preferred_element_type=F32
    )


def right_inner(left_mat, right_mat):
    return lax.dot_general(
        left_mat, right_mat, (((1,), (1,)), ((), ())), preferred_element_type=F32
    )


def swap(value):
    return lax.ppermute(value, "row", [(0, 1), (1, 0)])


def ordered(row, mine, other, axis):
    return jnp.where(
        row == 0,
        jnp.concatenate([mine, other], axis=axis),
        jnp.concatenate([other, mine], axis=axis),
    )


def half_of(value, which, axis):
    size = value.shape[axis] // 2
    return lax.dynamic_slice_in_dim(value, which * size, size, axis)


def to_tokens(value, row):
    return half_of(value, row, 0), swap(half_of(value, 1 - row, 0))


def to_features(value, row):
    other = swap(half_of(value, 1 - row, 1))
    return ordered(row, half_of(value, row, 1), other, 0)


def xor_swap(value, axis, mask):
    count = lax.axis_size(axis)
    return lax.ppermute(value, axis, [(i, i ^ mask) for i in range(count)])


def picked(parts, axis):
    stacked = jnp.stack(parts)
    own = lax.axis_index(axis)
    return [
        lax.dynamic_index_in_dim(stacked, own ^ i, 0, keepdims=False) for i in range(len(parts))
    ]


def gathered(value, axis):
    count = lax.axis_size(axis)
    if count > 4:
        return lax.all_gather(value, axis, axis=0)
    parts = [value] + [xor_swap(value, axis, k) for k in range(1, count)]
    return jnp.stack(picked(parts, axis))


def scattered(value, axis, dim):
    count = lax.axis_size(axis)
    if count > 4:
        return lax.psum_scatter(value, axis, scatter_dimension=dim, tiled=False).astype(F32)
    own = lax.axis_index(axis)

    def part(k):
        return lax.dynamic_index_in_dim(value, own ^ k, dim, keepdims=False)

    arrived = [xor_swap(part(k), axis, k) for k in range(1, count)]
    total = part(0).astype(F32)
    for one in arrived:
        total = total + one.astype(F32)
    return total


def two_level(piece, used):
    arrived = []
    for k in range(1, lax.axis_size("col")):
        arrived.append(xor_swap(piece, "col", k))
    ours = jnp.stack([one[:used] for one in arrived])
    return arrived, [ours] + [xor_swap(ours, "dp", j) for j in range(1, 4)]


def reduce_dp(quarters):
    own = lax.axis_index("dp")

    def part(k):
        return lax.dynamic_index_in_dim(quarters, own ^ k, 1, keepdims=False)

    arrived = []
    for k in range(1, 4):
        arrived.append(xor_swap(part(k), "dp", k))
    total = part(0).astype(F32)
    for one in arrived:
        total = total + one.astype(F32)
    return total.astype(BF)


def reduce_col(ours):
    piece = scattered(ours, "col", 0).astype(BF)
    return [piece] + [xor_swap(piece, "dp", k) for k in range(1, 4)]


def places_of():
    return jnp.stack([lax.axis_index("col"), lax.axis_index("dp")]).astype(jnp.int32)


def at_rows(start, count):
    return pl.ds(pl.multiple_of(start, 16), count)


def local_call(kernel, places, inputs, outs):
    spec = pl.BlockSpec(memory_space=pltpu.VMEM)
    return pl.pallas_call(
        kernel,
        out_shape=outs,
        in_specs=[pl.BlockSpec(memory_space=pltpu.SMEM)] + [spec] * len(inputs),
        out_specs=jax.tree.map(lambda _: spec, outs),
        cost_estimate=pl.CostEstimate(flops=0, bytes_accessed=4 << 20, transcendentals=0),
    )(places, *inputs)


def qkv_kernel(places, own, *refs):
    parts, out = refs[:-1], refs[-1]
    col, dp = places[0], places[1]
    share = own.shape[1]
    depth = share // 4
    for kind in range(3):
        for pair in range(PAIRS):
            lanes = slice((3 * pair + kind) * LANES, (3 * pair + kind + 1) * LANES)
            source = slice(pair * LANES, (pair + 1) * LANES)
            out[at_rows(col * share, share), lanes] = own[kind, :, source]
            for j in range(4):
                for k in range(1, 4):
                    rows = at_rows((col ^ k) * share + (dp ^ j) * depth, depth)
                    out[rows, lanes] = parts[j][
                        k - 1, kind * depth : (kind + 1) * depth, source
                    ]


def later_kernel(places, own_down, own_in, own_out, *refs):
    parts, (down, inner, out) = refs[:-3], refs[-3:]
    col, dp = places[0], places[1]
    wide_rows, deep_rows, out_rows = own_down.shape[0], own_in.shape[0], own_out.shape[0]
    down[at_rows(col * wide_rows, wide_rows), :] = own_down[...]
    inner[at_rows(col * deep_rows, deep_rows), :] = own_in[...]
    out[at_rows(col * out_rows, out_rows), :] = own_out[...]
    for j in range(4):
        there = dp ^ j
        for k in range(1, 4):
            part = parts[j].at[k - 1]
            count, at = wide_rows // 4, 0
            rows = at_rows((col ^ k) * wide_rows + there * count, count)
            for i in range(2):
                down[rows, i * WIDE : (i + 1) * WIDE] = part[at : at + count, :]
                at += count
            count = deep_rows // 4
            rows = at_rows((col ^ k) * deep_rows + there * count, count)
            for i in range(4):
                inner[rows, i * WIDE : (i + 1) * WIDE] = part[at : at + count, :]
                at += count
            count = out_rows // 2
            rows = at_rows((col ^ k) * out_rows + lax.rem(there, 2) * count, count)
            lanes = pl.ds(pl.multiple_of(there // 2 * WIDE, LANES), WIDE)
            out[rows, lanes] = part[at : at + count, :]


def early_out_kernel(places, *refs):
    parts, (down, inner, out) = refs[:-3], refs[-3:]
    dp = places[1]
    for j in range(4):
        there = dp ^ j
        count, at = down.shape[0] // 4, 0
        for i in range(2):
            down[at_rows(there * count, count), i * WIDE : (i + 1) * WIDE] = parts[j][
                at : at + count, :
            ].astype(F32)
            at += count
        count = inner.shape[0] // 4
        for i in range(4):
            inner[at_rows(there * count, count), i * WIDE : (i + 1) * WIDE] = parts[j][
                at : at + count, :
            ].astype(F32)
            at += count
        count = out.shape[0] // 2
        lanes = pl.ds(pl.multiple_of(there // 2 * WIDE, LANES), WIDE)
        out[at_rows(lax.rem(there, 2) * count, count), lanes] = parts[j][
            at : at + count, :
        ].astype(F32)


def late_out_kernel(places, *refs):
    parts, out = refs[:-1], refs[-1]
    dp = places[1]
    count = out.shape[1] // 4
    for j in range(4):
        rows = at_rows((dp ^ j) * count, count)
        for pair in range(PAIRS):
            for kind in range(3):
                out[kind, rows, pair * LANES : (pair + 1) * LANES] = parts[j][
                    pair * count : (pair + 1) * count, kind * LANES : (kind + 1) * LANES
                ].astype(F32)


def quartered_rows(value, count):
    pieces = value.shape[1] // WIDE
    cut = value.reshape(count, 4, -1, value.shape[1])
    return jnp.concatenate(
        [cut[..., i * WIDE : (i + 1) * WIDE] for i in range(pieces)], axis=2
    )


def quartered_halves(value, count):
    cut = value.reshape(count, 2, -1, 2 * WIDE)
    return jnp.concatenate([cut[..., :WIDE], cut[..., WIDE:]], axis=1)


def quartered_vector(flat, rows):
    count, size = flat.shape
    return jnp.pad(flat, ((0, 0), (0, 4 * rows * WIDE - size))).reshape(count, 4, rows, WIDE)


def first_quarter(parts, rows):
    stacked = jnp.stack([one[-rows:] for one in parts])
    return lax.dynamic_index_in_dim(
        stacked, lax.axis_index("dp"), 0, keepdims=False
    ).astype(F32).reshape(-1)


def stack_heads(value):
    lane = lax.broadcasted_iota(jnp.int32, value.shape, 1)
    zero = jnp.zeros_like(value)
    return jnp.concatenate(
        [jnp.where(lane < HD, value, zero), jnp.where(lane >= HD, value, zero)], axis=0
    )


def join_heads(value, block):
    lane = lax.broadcasted_iota(jnp.int32, (LANES, block), 0)
    return jnp.where(lane < HD, value[:, :block], value[:, block:]).T


def doubled(value):
    return jnp.concatenate([value, value], axis=1)


def mask_bias(key_place, first_key, past_key):
    places = key_place + lax.broadcasted_iota(jnp.int32, (key_place_rows(), first_key.shape[1]), 0)
    inside = (places >= first_key) & (places < past_key)
    return doubled(jnp.where(inside, 0.0, MASKED))


KEY_BLOCK = 256


def key_place_rows():
    return KEY_BLOCK


def copy_blocks(dest, own, others, rows):
    dest[:rows, :] = own[...]
    dest[rows:, :] = others[...]


def forward_kernel(
    blocks, table, q_ref, k_ref, v_ref, ko_ref, vo_ref, span_ref, out_ref, log_ref, keys, values
):
    rows = q_ref.shape[0]
    block = rows // blocks
    copy_blocks(keys, k_ref, ko_ref, rows)
    copy_blocks(values, v_ref, vo_ref, rows)
    slots = keys.shape[0] // KEY_BLOCK
    base = table[2 * blocks]

    @pl.loop(0, blocks)
    def _(at):
        here = pl.ds(pl.multiple_of(at * block, block), block)
        wide = pl.ds(pl.multiple_of(at * 2 * block, 2 * block), 2 * block)
        query = stack_heads((q_ref[here, :].astype(F32) * 0.125).astype(BF))
        first_key = span_ref[0:1, here]
        past_key = span_ref[1:2, here]

        def step(place, running):
            peak, total, summed = running
            slot = lax.rem(place - base + slots, slots)
            rows_at = pl.ds(pl.multiple_of(slot * KEY_BLOCK, KEY_BLOCK), KEY_BLOCK)
            scores = right_inner(keys[rows_at, :], query)
            scores = scores + mask_bias(place * KEY_BLOCK, first_key, past_key)
            higher = jnp.maximum(peak, jnp.max(scores, axis=0, keepdims=True))
            raised = jnp.exp(scores - higher)
            fade = jnp.exp(peak - higher)
            total = total * fade + jnp.sum(raised, axis=0, keepdims=True)
            summed = summed * fade + left_inner(values[rows_at, :], raised.astype(BF))
            return (higher, total, summed)

        init = (
            jnp.full((1, 2 * block), MASKED, F32),
            jnp.zeros((1, 2 * block), F32),
            jnp.zeros((LANES, 2 * block), F32),
        )
        peak, total, summed = lax.fori_loop(table[at], table[blocks + at], step, init)
        out_ref[here, :] = join_heads(summed / total, block).astype(BF)
        log_ref[:, wide] = jnp.broadcast_to(
            peak + jnp.log(total), (8, 2 * block)
        )


def backward_kernel(
    blocks,
    table,
    q_ref,
    k_ref,
    v_ref,
    ko_ref,
    vo_ref,
    span_ref,
    out_ref,
    log_ref,
    grad_ref,
    dq_ref,
    dk_ref,
    dv_ref,
    others_ref,
    keys,
    values,
    key_sum,
    value_sum,
):
    rows = q_ref.shape[0]
    block = rows // blocks
    copy_blocks(keys, k_ref, ko_ref, rows)
    copy_blocks(values, v_ref, vo_ref, rows)
    slots = keys.shape[0] // KEY_BLOCK
    base = table[2 * blocks]
    key_sum[...] = jnp.zeros_like(key_sum)
    value_sum[...] = jnp.zeros_like(value_sum)

    @pl.loop(0, blocks)
    def _(at):
        here = pl.ds(pl.multiple_of(at * block, block), block)
        wide = pl.ds(pl.multiple_of(at * 2 * block, 2 * block), 2 * block)
        query = stack_heads((q_ref[here, :].astype(F32) * 0.125).astype(BF))
        grad = stack_heads(grad_ref[here, :])
        along = (grad_ref[here, :].astype(F32) * out_ref[here, :].astype(F32)).T
        dots = jnp.concatenate(
            [
                jnp.sum(along[:HD], axis=0, keepdims=True),
                jnp.sum(along[HD:], axis=0, keepdims=True),
            ],
            axis=1,
        )
        logs = log_ref[0:1, wide]
        first_key = span_ref[0:1, here]
        past_key = span_ref[1:2, here]

        def step(place, summed):
            slot = lax.rem(place - base + slots, slots)
            rows_at = pl.ds(pl.multiple_of(slot * KEY_BLOCK, KEY_BLOCK), KEY_BLOCK)
            key = keys[rows_at, :]
            scores = right_inner(key, query)
            scores = scores + mask_bias(place * KEY_BLOCK, first_key, past_key)
            weights = jnp.exp(scores - logs)
            grad_weights = right_inner(values[rows_at, :], grad)
            value_sum[rows_at, :] += matmul(weights.astype(BF), grad)
            grad_scores = (weights * (grad_weights - dots)).astype(BF)
            key_sum[rows_at, :] += matmul(grad_scores, query)
            return summed + left_inner(key, grad_scores)

        summed = lax.fori_loop(
            table[at], table[blocks + at], step, jnp.zeros((LANES, 2 * block), F32)
        )
        dq_ref[here, :] = (join_heads(summed, block) * 0.125).astype(BF)

    dk_ref[...] = key_sum[:rows, :]
    dv_ref[...] = value_sum[:rows, :]
    others_ref[:, :LANES] = key_sum[rows:, :].astype(BF)
    others_ref[:, LANES:] = value_sum[rows:, :].astype(BF)


def attention_specs(rows, others, pair):
    return [
        pl.BlockSpec((rows, LANES), lambda g, t: (0, 3 * pair)),
        pl.BlockSpec((rows, LANES), lambda g, t: (0, 3 * pair + 1)),
        pl.BlockSpec((rows, LANES), lambda g, t: (0, 3 * pair + 2)),
        pl.BlockSpec((others, LANES), lambda g, t: (0, 0)),
        pl.BlockSpec((others, LANES), lambda g, t: (0, 1)),
        pl.BlockSpec((8, rows), lambda g, t: (0, 0)),
    ]


def attend_forward(table, qkv, kv_others, spans, blocks, pair):
    rows, others = qkv.shape[0], kv_others.shape[0]
    return pl.pallas_call(
        functools.partial(forward_kernel, blocks),
        out_shape=(
            jax.ShapeDtypeStruct((rows, LANES), BF),
            jax.ShapeDtypeStruct((8, 2 * rows), F32),
        ),
        grid_spec=pltpu.PrefetchScalarGridSpec(
            num_scalar_prefetch=1,
            grid=(1,),
            in_specs=attention_specs(rows, others, pair),
            out_specs=(
                pl.BlockSpec((rows, LANES), lambda g, t: (0, 0)),
                pl.BlockSpec((8, 2 * rows), lambda g, t: (0, 0)),
            ),
            scratch_shapes=[pltpu.VMEM((rows + others, LANES), BF)] * 2,
        ),
        cost_estimate=pl.CostEstimate(
            flops=8 * rows * LEN * LANES, bytes_accessed=8 * rows * LANES, transcendentals=0
        ),
        name="attend_forward",
    )(table, qkv, qkv, qkv, kv_others, kv_others, spans)


def attend_backward(table, qkv, kv_others, spans, out, logs, grad, blocks, pair):
    rows, others = qkv.shape[0], kv_others.shape[0]
    whole = pl.BlockSpec((rows, LANES), lambda g, t: (0, 0))
    mine = pl.BlockSpec((rows, LANES), lambda g, t: (0, pair))
    return pl.pallas_call(
        functools.partial(backward_kernel, blocks),
        out_shape=(
            jax.ShapeDtypeStruct((rows, LANES), BF),
            jax.ShapeDtypeStruct((rows, LANES), F32),
            jax.ShapeDtypeStruct((rows, LANES), F32),
            jax.ShapeDtypeStruct((others, 2 * LANES), BF),
        ),
        grid_spec=pltpu.PrefetchScalarGridSpec(
            num_scalar_prefetch=1,
            grid=(1,),
            in_specs=attention_specs(rows, others, pair)
            + [whole, pl.BlockSpec((8, 2 * rows), lambda g, t: (0, 0)), mine],
            out_specs=(
                whole,
                whole,
                whole,
                pl.BlockSpec((others, 2 * LANES), lambda g, t: (0, 0)),
            ),
            scratch_shapes=[pltpu.VMEM((rows + others, LANES), BF)] * 2
            + [pltpu.VMEM((rows + others, LANES), F32)] * 2,
        ),
        cost_estimate=pl.CostEstimate(
            flops=20 * rows * LEN * LANES, bytes_accessed=16 * rows * LANES, transcendentals=0
        ),
        name="attend_backward",
    )(table, qkv, qkv, qkv, kv_others, kv_others, spans, out, logs, grad)


def norm_forward(summed, gain_vec, shift_vec):
    center = jnp.mean(summed, axis=1, keepdims=True)
    centered = summed - center
    spread = jnp.mean(centered * centered, axis=1, keepdims=True)
    inv_scale = lax.rsqrt(spread + EPSILON)
    normed_hat = centered * inv_scale
    return (normed_hat * gain_vec + shift_vec, normed_hat, inv_scale)


def norm_backward(grad_vals, normed_hat, inv_scale, gain_vec):
    grad_hat = grad_vals * gain_vec
    return inv_scale * (
        grad_hat
        - jnp.mean(grad_hat, axis=1, keepdims=True)
        - normed_hat * jnp.mean(grad_hat * normed_hat, axis=1, keepdims=True)
    )


def gelu_value(hidden):
    return 0.5 * hidden * (1.0 + lax.erf(hidden * HALF_ROOT))


def gelu_slope(hidden):
    return (
        0.5 * (1.0 + lax.erf(hidden * HALF_ROOT))
        + hidden * jnp.exp(-0.5 * hidden * hidden) * DENSITY
    )


def lanes_to_rows(value):
    pieces = value.shape[2] // WIDE
    return jnp.concatenate(
        [value[:, :, i * WIDE : (i + 1) * WIDE] for i in range(pieces)], axis=1
    )


def rows_to_lanes(value, pieces):
    rows = value.shape[-2] // pieces
    return jnp.concatenate(
        [value[..., i * rows : (i + 1) * rows, :] for i in range(pieces)], axis=-1
    )


def dp_part(value, own, axis=0):
    size = value.shape[axis] // 4
    return lax.dynamic_slice_in_dim(value, own * size, size, axis)


def padded_rows(flat, rows):
    count, size = flat.shape
    return jnp.pad(flat, ((0, 0), (0, rows * WIDE - size))).reshape(count, rows, WIDE)


def body(
    layer_input,
    lengths,
    w_qkv,
    bias_qv,
    w_out,
    bias_out,
    gain_attn,
    shift_attn,
    w_in,
    bias_in,
    w_down,
    bias_down,
    gain_ffn,
    shift_ffn,
    cotangent,
):
    col_grid = lax.axis_size("col")
    rows = layer_input.shape[0]
    row = lax.axis_index("row")
    own_dp = lax.axis_index("dp")
    own_col = lax.axis_index("col")
    group = LEN // rows
    start_row = own_col * rows
    block = min(256, rows)
    blocks = rows // block

    qkv_piece = jnp.swapaxes(dp_part(w_qkv, own_dp), 0, 1)
    depth = qkv_piece.shape[1]
    vectors = jnp.concatenate(
        [bias_out, gain_attn, shift_attn, bias_down, gain_ffn, shift_ffn, bias_in]
    )
    share = bias_out.shape[0]
    vector_rows = 16
    first_piece = jnp.concatenate(
        [
            qkv_piece.reshape(3 * depth, WIDE),
            jnp.pad(bias_qv, ((0, vector_rows - 2), (0, WIDE - share))),
        ],
        axis=0,
    )
    places = places_of()
    if col_grid > 4:
        first_cols = gathered(first_piece, "col")
        bias_col = first_cols[:, 3 * depth :]
        qkv_parts = gathered(first_cols[:, : 3 * depth], "dp")
        w_qkv_half = jnp.transpose(
            qkv_parts.reshape(4, col_grid, 3, depth, PAIRS, LANES), (1, 0, 3, 4, 2, 5)
        ).reshape(D, 3 * WIDE)
    else:
        first_arrived, first_parts = two_level(first_piece, 3 * depth)
        bias_col = jnp.stack(
            picked([one[3 * depth :] for one in [first_piece] + first_arrived], "col")
        )
        w_qkv_half = local_call(
            qkv_kernel,
            places,
            [jnp.swapaxes(w_qkv, 0, 1)] + first_parts,
            jax.ShapeDtypeStruct((D, 3 * WIDE), BF),
        )
    bias_q = bias_col[:, 0, :share].reshape(-1).astype(F32)
    bias_v = bias_col[:, 1, :share].reshape(-1).astype(F32)

    input_full = ordered(row, layer_input, swap(layer_input), 1)
    input_tokens = half_of(input_full, row, 0).astype(F32)
    cot_mine, cot_other = to_tokens(cotangent, row)
    grad_out = ordered(row, cot_mine, cot_other, 1).astype(F32)

    bias_rows = jnp.stack(
        [
            bias_q.reshape(PAIRS, LANES),
            jnp.zeros((PAIRS, LANES), F32),
            bias_v.reshape(PAIRS, LANES),
        ],
        axis=1,
    ).reshape(-1)
    qkv_low = (matmul(input_full, w_qkv_half) + bias_rows[None]).astype(BF)

    def group_perm(offset, back):
        pairs = []
        for i in range(col_grid):
            source = i // group * group + (i + offset) % group
            pairs.append((i, source) if back else (source, i))
        return pairs

    kv_others = []
    for pair in range(PAIRS):
        kv_local = qkv_low[:, (3 * pair + 1) * LANES : (3 * pair + 3) * LANES]
        arrived = [lax.ppermute(kv_local, "col", group_perm(j, False)) for j in range(1, group)]
        kv_others.append(jnp.concatenate(arrived, axis=0))

    down_piece = lanes_to_rows(dp_part(w_down, own_dp)[None])[0]
    in_piece = lanes_to_rows(dp_part(w_in, own_dp)[None])[0]
    if col_grid > 4:
        out_piece = lanes_to_rows(dp_part(w_out, own_dp)[None])[0]
        later_piece = jnp.concatenate([down_piece, in_piece, out_piece], axis=0)
        later_parts = gathered(gathered(later_piece, "col"), "dp")
        vectors_col = gathered(vectors, "col")
        cut_down = down_piece.shape[0]
        cut_in = cut_down + in_piece.shape[0]

        def whole_half(parts, pieces):
            joined = jnp.swapaxes(rows_to_lanes(parts, pieces), 0, 1)
            return joined.reshape(-1, joined.shape[-1])

        w_down_mine = whole_half(later_parts[:, :, :cut_down], 2)
        w_in_mine = whole_half(later_parts[:, :, cut_down:cut_in], 4)
        w_out_mine = whole_half(later_parts[:, :, cut_in:], 2)
    else:
        out_half = w_out.shape[0] // 2
        out_piece = lax.dynamic_slice(
            w_out, (own_dp % 2 * out_half, own_dp // 2 * WIDE), (out_half, WIDE)
        )
        used = down_piece.shape[0] + in_piece.shape[0] + out_half
        later_piece = jnp.concatenate(
            [down_piece, in_piece, out_piece, padded_rows(vectors[None], vector_rows)[0]], axis=0
        )
        later_arrived, later_parts = two_level(later_piece, used)
        vectors_col = jnp.stack(
            picked([one[used:] for one in [later_piece] + later_arrived], "col")
        )
        vectors_col = vectors_col.reshape(col_grid, -1)[:, : vectors.shape[0]]
        w_down_mine, w_in_mine, w_out_mine = local_call(
            later_kernel,
            places,
            [w_down, w_in, w_out] + later_parts,
            (
                jax.ShapeDtypeStruct((4 * w_down.shape[0], D), BF),
                jax.ShapeDtypeStruct((4 * w_in.shape[0], w_in.shape[1]), BF),
                jax.ShapeDtypeStruct((4 * w_out.shape[0], D), BF),
            ),
        )
    vectors_both = swap(vectors_col)

    def vector(at, count=1):
        mine = vectors_col[:, at * share : (at + count) * share].reshape(-1)
        other = vectors_both[:, at * share : (at + count) * share].reshape(-1)
        return mine.astype(F32), other.astype(F32)

    def whole_vector(at):
        mine, other = vector(at)
        return ordered(row, mine, other, 0)[None]

    bias_out_f = whole_vector(0)
    gain_attn_f = whole_vector(1)
    shift_attn_f = whole_vector(2)
    bias_down_f = whole_vector(3)
    gain_ffn_f = whole_vector(4)
    shift_ffn_f = whole_vector(5)
    bias_in_mine, bias_in_other = vector(6, 4)

    w_out_other, w_in_other, w_down_other = swap(w_out_mine), swap(w_in_mine), swap(w_down_mine)

    own_lengths = lax.dynamic_index_in_dim(lengths, start_row // LEN, 0, keepdims=False)
    ends = jnp.cumsum(own_lengths)
    first_place = start_row % LEN
    spots = first_place + jnp.arange(rows, dtype=jnp.int32)
    past = spots[:, None] >= ends[None, :]
    first_key = jnp.max(jnp.where(past, ends[None, :], 0), axis=1)
    past_key = jnp.min(jnp.where(past, LEN, ends[None, :]), axis=1)
    spans = jnp.pad(jnp.stack([first_key, past_key]), ((0, 6), (0, 0)))
    table = jnp.concatenate(
        [
            first_key[::block] // KEY_BLOCK,
            (past_key[block - 1 :: block] + (KEY_BLOCK - 1)) // KEY_BLOCK,
            (first_place // KEY_BLOCK)[None],
        ]
    ).astype(jnp.int32)

    attended = [
        attend_forward(table, qkv_low, kv_others[pair], spans, blocks, pair)
        for pair in range(PAIRS)
    ]
    att_mine, att_other = to_tokens(jnp.concatenate([out for out, _ in attended], axis=1), row)

    projected = matmul(att_mine, w_out_mine) + matmul(att_other, w_out_other)
    first_sum = input_tokens + projected + bias_out_f
    normed, first_hat, first_scale = norm_forward(first_sum, gain_attn_f, shift_attn_f)
    normed_low = normed.astype(BF)
    hidden_mine = matmul(normed_low, w_in_mine) + bias_in_mine[None]
    hidden_other = matmul(normed_low, w_in_other) + bias_in_other[None]
    act_mine = gelu_value(hidden_mine).astype(BF)
    act_other = gelu_value(hidden_other).astype(BF)
    second_sum = (
        normed
        + matmul(act_mine, w_down_mine)
        + matmul(act_other, w_down_other)
        + bias_down_f
    )
    result, second_hat, second_scale = norm_forward(second_sum, gain_ffn_f, shift_ffn_f)
    result = to_features(result.astype(BF), row)

    grad_gain_ffn = jnp.sum(grad_out * second_hat, axis=0)
    grad_shift_ffn = jnp.sum(grad_out, axis=0)
    grad_second = norm_backward(grad_out, second_hat, second_scale, gain_ffn_f)
    grad_bias_down = jnp.sum(grad_second, axis=0)
    grad_ffn = grad_second.astype(BF)
    grad_hidden_mine = (right_inner(grad_ffn, w_down_mine) * gelu_slope(hidden_mine)).astype(BF)
    grad_hidden_other = (right_inner(grad_ffn, w_down_other) * gelu_slope(hidden_other)).astype(BF)
    grad_normed = (
        grad_second
        + right_inner(grad_hidden_mine, w_in_mine)
        + right_inner(grad_hidden_other, w_in_other)
    )
    grad_gain_attn = jnp.sum(grad_normed * first_hat, axis=0)
    grad_shift_attn = jnp.sum(grad_normed, axis=0)
    grad_first = norm_backward(grad_normed, first_hat, first_scale, gain_attn_f)
    grad_bias_out = jnp.sum(grad_first, axis=0)
    grad_proj = grad_first.astype(BF)
    grad_att_mine = right_inner(grad_proj, w_out_mine).astype(BF)
    grad_att_other = right_inner(grad_proj, w_out_other).astype(BF)
    grad_attended = ordered(row, grad_att_mine, swap(grad_att_other), 0)
    grad_first_features = to_features(grad_first, row)

    def both_tokens(mine, other):
        return (mine + swap(other.astype(BF)).astype(F32)).astype(BF)

    grad_down = both_tokens(left_inner(act_mine, grad_ffn), left_inner(act_other, grad_ffn))
    grad_in = both_tokens(
        left_inner(normed_low, grad_hidden_mine), left_inner(normed_low, grad_hidden_other)
    )
    grad_out_w = both_tokens(left_inner(att_mine, grad_proj), left_inner(att_other, grad_proj))
    by_row = jnp.stack(
        [
            grad_bias_out,
            grad_gain_attn,
            grad_shift_attn,
            grad_bias_down,
            grad_gain_ffn,
            grad_shift_ffn,
        ]
    )
    in_mine = jnp.sum(grad_hidden_mine, axis=0, dtype=F32)
    in_other = jnp.sum(grad_hidden_other, axis=0, dtype=F32)

    def vector_block(six, inner):
        split = jnp.swapaxes(six.reshape(6, col_grid, share), 0, 1).reshape(col_grid, -1)
        return jnp.concatenate([split, inner.reshape(col_grid, -1)], axis=1)

    vec_mine = vector_block(half_of(by_row, row, 1), in_mine)
    vec_other = vector_block(half_of(by_row, 1 - row, 1), in_other)
    vec_sum = (vec_mine + swap(vec_other)).astype(BF)

    vec_pad = 16
    early = jnp.concatenate(
        [
            quartered_rows(grad_down, col_grid),
            quartered_rows(grad_in, col_grid),
            quartered_halves(grad_out_w, col_grid)
            if col_grid <= 4
            else quartered_rows(grad_out_w, col_grid),
            quartered_vector(vec_sum, vec_pad),
        ],
        axis=2,
    )
    early, grad_attended = lax.optimization_barrier((early, grad_attended))
    early_dp = reduce_dp(early)

    grad_pairs = []
    for pair in range(PAIRS):
        out, logs = attended[pair]
        grad_query, key_own, value_own, others = attend_backward(
            table, qkv_low, kv_others[pair], spans, out, logs, grad_attended, blocks, pair
        )
        for j in range(1, group):
            arrived = lax.ppermute(
                others[(j - 1) * rows : j * rows], "col", group_perm(j, True)
            ).astype(F32)
            key_own = key_own + arrived[:, :LANES]
            value_own = value_own + arrived[:, LANES:]
        grad_pairs += [grad_query, key_own.astype(BF), value_own.astype(BF)]
    grad_qkv = jnp.concatenate(grad_pairs, axis=1)

    grad_w_qkv = left_inner(input_full, grad_qkv).astype(BF)
    bias_sums = jnp.sum(grad_qkv, axis=0, dtype=F32).reshape(PAIRS, 3, LANES)
    bias_pair = jnp.stack([bias_sums[:, 0].reshape(-1), bias_sums[:, 2].reshape(-1)])
    bias_pair = jnp.swapaxes(bias_pair.reshape(2, col_grid, share), 0, 1).reshape(col_grid, -1)
    late = jnp.concatenate(
        [
            quartered_rows(grad_w_qkv, col_grid),
            quartered_vector(bias_pair.astype(BF), vec_pad),
        ],
        axis=2,
    )
    late, early_dp = lax.optimization_barrier((late, early_dp))
    early_parts = reduce_col(early_dp)
    late_parts = reduce_col(reduce_dp(late))

    partial = right_inner(grad_qkv, w_qkv_half)
    arrived = swap(half_of(partial, 1 - row, 1).astype(BF)).astype(F32)
    grad_input = grad_first_features + half_of(partial, row, 1) + arrived

    if col_grid > 4:
        early_all = jnp.stack(picked(early_parts, "dp")).astype(F32)
        late_all = jnp.stack(picked(late_parts, "dp")).astype(F32)
        cut_down = 2 * w_down.shape[0] // 4
        cut_in = cut_down + w_in.shape[0]
        grad_down_own = rows_to_lanes(early_all[:, :cut_down], 2).reshape(w_down.shape)
        grad_in_own = rows_to_lanes(early_all[:, cut_down:cut_in], 4).reshape(w_in.shape)
        grad_out_own = rows_to_lanes(early_all[:, cut_in:-vec_pad], 2).reshape(w_out.shape)
        qkv_own = late_all[:, :-vec_pad].reshape(4, PAIRS, depth, 3, LANES)
        qkv_own = jnp.transpose(qkv_own, (0, 2, 3, 1, 4)).reshape(w_qkv.shape)
    else:
        grad_down_own, grad_in_own, grad_out_own = local_call(
            early_out_kernel,
            places,
            early_parts,
            tuple(jax.ShapeDtypeStruct(one.shape, F32) for one in (w_down, w_in, w_out)),
        )
        qkv_own = local_call(
            late_out_kernel,
            places,
            late_parts,
            jax.ShapeDtypeStruct((3, w_qkv.shape[0], WIDE), F32),
        )
        qkv_own = jnp.swapaxes(qkv_own, 0, 1)
    vec_own = first_quarter(early_parts, vec_pad)
    vecs = [vec_own[i * share : (i + 1) * share] for i in range(6)]
    bias_in_own = vec_own[6 * share : 10 * share]
    bias_own = first_quarter(late_parts, vec_pad)[: 2 * share].reshape(2, share)
    return (
        result,
        grad_input,
        qkv_own,
        bias_own,
        grad_out_own,
        vecs[0],
        vecs[1],
        vecs[2],
        grad_in_own,
        bias_in_own,
        grad_down_own,
        vecs[3],
        vecs[4],
        vecs[5],
    )


def solution(mesh):
    both = P(("row", "col"))
    specs = (
        P("col", None, "row"),
        P(None, ("row", "col")),
        P(("row", "col"), None),
        both,
        both,
        both,
        P("col", "row"),
        both,
        P(("row", "col"), None),
        both,
        both,
        both,
    )
    tokens = P(("dp", "col"), "row")
    return jax.shard_map(
        body,
        mesh=mesh,
        in_specs=(tokens, P("dp", None)) + specs + (tokens,),
        out_specs=(tokens, tokens) + specs,
        check_vma=False,
    )
```

```python
import functools

import jax
import jax.numpy as jnp
from jax import lax
from jax.experimental import pallas as pl
from jax.experimental.pallas import tpu as pltpu
from jax.sharding import PartitionSpec as P


D = 768
HD = 64
LEN = 2048
WIDE = 384
LANES = 128
PAIRS = WIDE // LANES

EPSILON = 1e-12
MASKED = -1e30
HALF_ROOT = 0.7071067811865476
DENSITY = 0.3989422804014327
BF = jnp.bfloat16
F32 = jnp.float32


def matmul(left_mat, right_mat):
    return jnp.dot(left_mat, right_mat, preferred_element_type=F32)


def left_inner(left_mat, right_mat):
    return lax.dot_general(
        left_mat, right_mat, (((0,), (0,)), ((), ())), preferred_element_type=F32
    )


def right_inner(left_mat, right_mat):
    return lax.dot_general(
        left_mat, right_mat, (((1,), (1,)), ((), ())), preferred_element_type=F32
    )


def swap(value):
    return lax.ppermute(value, "row", [(0, 1), (1, 0)])


def ordered(row, mine, other, axis):
    return jnp.where(
        row == 0,
        jnp.concatenate([mine, other], axis=axis),
        jnp.concatenate([other, mine], axis=axis),
    )


def half_of(value, which, axis):
    size = value.shape[axis] // 2
    return lax.dynamic_slice_in_dim(value, which * size, size, axis)


def to_tokens(value, row):
    return half_of(value, row, 0), swap(half_of(value, 1 - row, 0))


def to_features(value, row):
    other = swap(half_of(value, 1 - row, 1))
    return ordered(row, half_of(value, row, 1), other, 0)


def xor_swap(value, axis, mask):
    count = lax.axis_size(axis)
    return lax.ppermute(value, axis, [(i, i ^ mask) for i in range(count)])


def picked(parts, axis):
    stacked = jnp.stack(parts)
    own = lax.axis_index(axis)
    return [
        lax.dynamic_index_in_dim(stacked, own ^ i, 0, keepdims=False) for i in range(len(parts))
    ]


def gathered(value, axis):
    count = lax.axis_size(axis)
    if count > 4:
        return lax.all_gather(value, axis, axis=0)
    parts = [value] + [xor_swap(value, axis, k) for k in range(1, count)]
    return jnp.stack(picked(parts, axis))


def two_level(piece, used):
    arrived = []
    for k in range(1, lax.axis_size("col")):
        arrived.append(xor_swap(piece, "col", k))
    ours = jnp.stack([one[:used] for one in arrived])
    return arrived, [ours] + [xor_swap(ours, "dp", j) for j in range(1, 4)]


def reduce_dp(quarters):
    own = lax.axis_index("dp")

    def part(k):
        return lax.dynamic_index_in_dim(quarters, own ^ k, 1, keepdims=False)

    arrived = []
    for k in range(1, 4):
        arrived.append(xor_swap(part(k), "dp", k))
    total = part(0).astype(F32)
    for one in arrived:
        total = total + one.astype(F32)
    return total.astype(BF)


def reduce_col(ours):
    count = lax.axis_size("col")
    if count > 4:
        return lax.psum_scatter(ours, "col", scatter_dimension=0, tiled=False)
    own = lax.axis_index("col")

    def part(k):
        return lax.dynamic_index_in_dim(ours, own ^ k, 0, keepdims=False)

    arrived = []
    for k in range(1, count):
        arrived.append(xor_swap(part(k), "col", k))
    total = part(0).astype(F32)
    for one in arrived:
        total = total + one.astype(F32)
    return total.astype(BF)


def spread_dp(piece):
    parts = [piece]
    for k in range(1, 4):
        parts.append(xor_swap(piece, "dp", k))
    return parts


def places_of():
    return jnp.stack([lax.axis_index("col"), lax.axis_index("dp")]).astype(jnp.int32)


def at_rows(start, count):
    return pl.ds(pl.multiple_of(start, 16), count)


def local_call(kernel, places, inputs, outs):
    spec = pl.BlockSpec(memory_space=pltpu.VMEM)
    return pl.pallas_call(
        kernel,
        out_shape=outs,
        in_specs=[pl.BlockSpec(memory_space=pltpu.SMEM)] + [spec] * len(inputs),
        out_specs=jax.tree.map(lambda _: spec, outs),
        cost_estimate=pl.CostEstimate(flops=0, bytes_accessed=4 << 20, transcendentals=0),
    )(places, *inputs)


def qkv_kernel(places, own, *refs):
    parts, out = refs[:-1], refs[-1]
    col, dp = places[0], places[1]
    share = own.shape[1]
    depth = share // 4
    for kind in range(3):
        for pair in range(PAIRS):
            lanes = slice((3 * pair + kind) * LANES, (3 * pair + kind + 1) * LANES)
            source = slice(pair * LANES, (pair + 1) * LANES)
            out[at_rows(col * share, share), lanes] = own[kind, :, source]
            for j in range(4):
                for k in range(1, 4):
                    rows = at_rows((col ^ k) * share + (dp ^ j) * depth, depth)
                    out[rows, lanes] = parts[j][
                        k - 1, kind * depth : (kind + 1) * depth, source
                    ]


def later_kernel(places, own_down, own_in, own_out, *refs):
    parts, (down, inner, out) = refs[:-3], refs[-3:]
    col, dp = places[0], places[1]
    wide_rows, deep_rows, out_rows = own_down.shape[0], own_in.shape[0], own_out.shape[0]
    down[at_rows(col * wide_rows, wide_rows), :] = own_down[...]
    inner[at_rows(col * deep_rows, deep_rows), :] = own_in[...]
    out[at_rows(col * out_rows, out_rows), :] = own_out[...]
    for j in range(4):
        there = dp ^ j
        for k in range(1, 4):
            part = parts[j].at[k - 1]
            count, at = wide_rows // 4, 0
            rows = at_rows((col ^ k) * wide_rows + there * count, count)
            for i in range(2):
                down[rows, i * WIDE : (i + 1) * WIDE] = part[at : at + count, :]
                at += count
            count = deep_rows // 4
            rows = at_rows((col ^ k) * deep_rows + there * count, count)
            for i in range(4):
                inner[rows, i * WIDE : (i + 1) * WIDE] = part[at : at + count, :]
                at += count
            count = out_rows // 2
            rows = at_rows((col ^ k) * out_rows + lax.rem(there, 2) * count, count)
            lanes = pl.ds(pl.multiple_of(there // 2 * WIDE, LANES), WIDE)
            out[rows, lanes] = part[at : at + count, :]


def down_out_kernel(places, *refs):
    parts, down = refs[:-1], refs[-1]
    dp = places[1]
    count = down.shape[0] // 4
    for j in range(4):
        for i in range(2):
            down[at_rows((dp ^ j) * count, count), i * WIDE : (i + 1) * WIDE] = parts[j][
                i * count : (i + 1) * count, :
            ].astype(F32)


def in_out_kernel(places, *refs):
    parts, (inner, out) = refs[:-2], refs[-2:]
    dp = places[1]
    for j in range(4):
        there = dp ^ j
        count, at = inner.shape[0] // 4, 0
        for i in range(4):
            inner[at_rows(there * count, count), i * WIDE : (i + 1) * WIDE] = parts[j][
                at : at + count, :
            ].astype(F32)
            at += count
        count = out.shape[0] // 2
        lanes = pl.ds(pl.multiple_of(there // 2 * WIDE, LANES), WIDE)
        out[at_rows(lax.rem(there, 2) * count, count), lanes] = parts[j][
            at : at + count, :
        ].astype(F32)


def qkv_out_kernel(first_row, places, *refs):
    parts, last_parts, out = refs[:4], refs[4:8], refs[8]
    dp = places[1]
    count = out.shape[1] // 4
    for j in range(4):
        rows = at_rows((dp ^ j) * count, count)
        for pair in range(PAIRS):
            source = last_parts[j] if pair == PAIRS - 1 else parts[j]
            start = 0 if pair == PAIRS - 1 else first_row + pair * count
            for kind in range(3):
                out[kind, rows, pair * LANES : (pair + 1) * LANES] = source[
                    start : start + count, kind * LANES : (kind + 1) * LANES
                ].astype(F32)


def quartered_rows(value, count):
    pieces = value.shape[1] // WIDE
    cut = value.reshape(count, 4, -1, value.shape[1])
    return jnp.concatenate(
        [cut[..., i * WIDE : (i + 1) * WIDE] for i in range(pieces)], axis=2
    )


def quartered_halves(value, count):
    cut = value.reshape(count, 2, -1, 2 * WIDE)
    return jnp.concatenate([cut[..., :WIDE], cut[..., WIDE:]], axis=1)


def quartered_vector(flat, rows):
    count, size = flat.shape
    return jnp.pad(flat, ((0, 0), (0, 4 * rows * WIDE - size))).reshape(count, 4, rows, WIDE)


def first_quarter(parts, start, rows):
    stacked = jnp.stack([one[start : start + rows] for one in parts])
    return lax.dynamic_index_in_dim(
        stacked, lax.axis_index("dp"), 0, keepdims=False
    ).astype(F32).reshape(-1)


def stack_heads(value):
    lane = lax.broadcasted_iota(jnp.int32, value.shape, 1)
    zero = jnp.zeros_like(value)
    return jnp.concatenate(
        [jnp.where(lane < HD, value, zero), jnp.where(lane >= HD, value, zero)], axis=0
    )


def join_heads(value, block):
    lane = lax.broadcasted_iota(jnp.int32, (LANES, block), 0)
    return jnp.where(lane < HD, value[:, :block], value[:, block:]).T


def doubled(value):
    return jnp.concatenate([value, value], axis=1)


def mask_bias(key_place, first_key, past_key):
    places = key_place + lax.broadcasted_iota(jnp.int32, (key_place_rows(), first_key.shape[1]), 0)
    inside = (places >= first_key) & (places < past_key)
    return doubled(jnp.where(inside, 0.0, MASKED))


KEY_BLOCK = 256


def key_place_rows():
    return KEY_BLOCK


def copy_blocks(dest, own, others, rows):
    dest[:rows, :] = own[...]
    dest[rows:, :] = others[...]


def forward_kernel(
    blocks, table, q_ref, k_ref, v_ref, ko_ref, vo_ref, span_ref, out_ref, log_ref, keys, values
):
    rows = q_ref.shape[0]
    block = rows // blocks
    copy_blocks(keys, k_ref, ko_ref, rows)
    copy_blocks(values, v_ref, vo_ref, rows)
    slots = keys.shape[0] // KEY_BLOCK
    base = table[2 * blocks]

    @pl.loop(0, blocks)
    def _(at):
        here = pl.ds(pl.multiple_of(at * block, block), block)
        wide = pl.ds(pl.multiple_of(at * 2 * block, 2 * block), 2 * block)
        query = stack_heads((q_ref[here, :].astype(F32) * 0.125).astype(BF))
        first_key = span_ref[0:1, here]
        past_key = span_ref[1:2, here]

        def step(place, running):
            peak, total, summed = running
            slot = lax.rem(place - base + slots, slots)
            rows_at = pl.ds(pl.multiple_of(slot * KEY_BLOCK, KEY_BLOCK), KEY_BLOCK)
            scores = right_inner(keys[rows_at, :], query)
            scores = scores + mask_bias(place * KEY_BLOCK, first_key, past_key)
            higher = jnp.maximum(peak, jnp.max(scores, axis=0, keepdims=True))
            raised = jnp.exp(scores - higher)
            fade = jnp.exp(peak - higher)
            total = total * fade + jnp.sum(raised, axis=0, keepdims=True)
            summed = summed * fade + left_inner(values[rows_at, :], raised.astype(BF))
            return (higher, total, summed)

        init = (
            jnp.full((1, 2 * block), MASKED, F32),
            jnp.zeros((1, 2 * block), F32),
            jnp.zeros((LANES, 2 * block), F32),
        )
        peak, total, summed = lax.fori_loop(table[at], table[blocks + at], step, init)
        out_ref[here, :] = join_heads(summed / total, block).astype(BF)
        log_ref[:, wide] = jnp.broadcast_to(
            peak + jnp.log(total), (8, 2 * block)
        )


def backward_kernel(
    blocks,
    table,
    q_ref,
    k_ref,
    v_ref,
    ko_ref,
    vo_ref,
    span_ref,
    out_ref,
    log_ref,
    grad_ref,
    dq_ref,
    dk_ref,
    dv_ref,
    others_ref,
    keys,
    values,
    key_sum,
    value_sum,
):
    rows = q_ref.shape[0]
    block = rows // blocks
    copy_blocks(keys, k_ref, ko_ref, rows)
    copy_blocks(values, v_ref, vo_ref, rows)
    slots = keys.shape[0] // KEY_BLOCK
    base = table[2 * blocks]
    key_sum[...] = jnp.zeros_like(key_sum)
    value_sum[...] = jnp.zeros_like(value_sum)

    @pl.loop(0, blocks)
    def _(at):
        here = pl.ds(pl.multiple_of(at * block, block), block)
        wide = pl.ds(pl.multiple_of(at * 2 * block, 2 * block), 2 * block)
        query = stack_heads((q_ref[here, :].astype(F32) * 0.125).astype(BF))
        grad = stack_heads(grad_ref[here, :])
        along = (grad_ref[here, :].astype(F32) * out_ref[here, :].astype(F32)).T
        dots = jnp.concatenate(
            [
                jnp.sum(along[:HD], axis=0, keepdims=True),
                jnp.sum(along[HD:], axis=0, keepdims=True),
            ],
            axis=1,
        )
        logs = log_ref[0:1, wide]
        first_key = span_ref[0:1, here]
        past_key = span_ref[1:2, here]

        def step(place, summed):
            slot = lax.rem(place - base + slots, slots)
            rows_at = pl.ds(pl.multiple_of(slot * KEY_BLOCK, KEY_BLOCK), KEY_BLOCK)
            key = keys[rows_at, :]
            scores = right_inner(key, query)
            scores = scores + mask_bias(place * KEY_BLOCK, first_key, past_key)
            weights = jnp.exp(scores - logs)
            grad_weights = right_inner(values[rows_at, :], grad)
            value_sum[rows_at, :] += matmul(weights.astype(BF), grad)
            grad_scores = (weights * (grad_weights - dots)).astype(BF)
            key_sum[rows_at, :] += matmul(grad_scores, query)
            return summed + left_inner(key, grad_scores)

        summed = lax.fori_loop(
            table[at], table[blocks + at], step, jnp.zeros((LANES, 2 * block), F32)
        )
        dq_ref[here, :] = (join_heads(summed, block) * 0.125).astype(BF)

    dk_ref[...] = key_sum[:rows, :]
    dv_ref[...] = value_sum[:rows, :]
    others_ref[:, :LANES] = key_sum[rows:, :].astype(BF)
    others_ref[:, LANES:] = value_sum[rows:, :].astype(BF)


def attention_specs(rows, others, pair):
    return [
        pl.BlockSpec((rows, LANES), lambda g, t: (0, 3 * pair)),
        pl.BlockSpec((rows, LANES), lambda g, t: (0, 3 * pair + 1)),
        pl.BlockSpec((rows, LANES), lambda g, t: (0, 3 * pair + 2)),
        pl.BlockSpec((others, LANES), lambda g, t: (0, 0)),
        pl.BlockSpec((others, LANES), lambda g, t: (0, 1)),
        pl.BlockSpec((8, rows), lambda g, t: (0, 0)),
    ]


def attend_forward(table, qkv, kv_others, spans, blocks, pair):
    rows, others = qkv.shape[0], kv_others.shape[0]
    return pl.pallas_call(
        functools.partial(forward_kernel, blocks),
        out_shape=(
            jax.ShapeDtypeStruct((rows, LANES), BF),
            jax.ShapeDtypeStruct((8, 2 * rows), F32),
        ),
        grid_spec=pltpu.PrefetchScalarGridSpec(
            num_scalar_prefetch=1,
            grid=(1,),
            in_specs=attention_specs(rows, others, pair),
            out_specs=(
                pl.BlockSpec((rows, LANES), lambda g, t: (0, 0)),
                pl.BlockSpec((8, 2 * rows), lambda g, t: (0, 0)),
            ),
            scratch_shapes=[pltpu.VMEM((rows + others, LANES), BF)] * 2,
        ),
        cost_estimate=pl.CostEstimate(
            flops=8 * rows * LEN * LANES, bytes_accessed=8 * rows * LANES, transcendentals=0
        ),
        name="attend_forward",
    )(table, qkv, qkv, qkv, kv_others, kv_others, spans)


def attend_backward(table, qkv, kv_others, spans, out, logs, grad, blocks, pair):
    rows, others = qkv.shape[0], kv_others.shape[0]
    whole = pl.BlockSpec((rows, LANES), lambda g, t: (0, 0))
    mine = pl.BlockSpec((rows, LANES), lambda g, t: (0, pair))
    return pl.pallas_call(
        functools.partial(backward_kernel, blocks),
        out_shape=(
            jax.ShapeDtypeStruct((rows, LANES), BF),
            jax.ShapeDtypeStruct((rows, LANES), F32),
            jax.ShapeDtypeStruct((rows, LANES), F32),
            jax.ShapeDtypeStruct((others, 2 * LANES), BF),
        ),
        grid_spec=pltpu.PrefetchScalarGridSpec(
            num_scalar_prefetch=1,
            grid=(1,),
            in_specs=attention_specs(rows, others, pair)
            + [whole, pl.BlockSpec((8, 2 * rows), lambda g, t: (0, 0)), mine],
            out_specs=(
                whole,
                whole,
                whole,
                pl.BlockSpec((others, 2 * LANES), lambda g, t: (0, 0)),
            ),
            scratch_shapes=[pltpu.VMEM((rows + others, LANES), BF)] * 2
            + [pltpu.VMEM((rows + others, LANES), F32)] * 2,
        ),
        cost_estimate=pl.CostEstimate(
            flops=20 * rows * LEN * LANES, bytes_accessed=16 * rows * LANES, transcendentals=0
        ),
        name="attend_backward",
    )(table, qkv, qkv, qkv, kv_others, kv_others, spans, out, logs, grad)


def norm_forward(summed, gain_vec, shift_vec):
    center = jnp.mean(summed, axis=1, keepdims=True)
    centered = summed - center
    spread = jnp.mean(centered * centered, axis=1, keepdims=True)
    inv_scale = lax.rsqrt(spread + EPSILON)
    normed_hat = centered * inv_scale
    return (normed_hat * gain_vec + shift_vec, normed_hat, inv_scale)


def norm_backward(grad_vals, normed_hat, inv_scale, gain_vec):
    grad_hat = grad_vals * gain_vec
    return inv_scale * (
        grad_hat
        - jnp.mean(grad_hat, axis=1, keepdims=True)
        - normed_hat * jnp.mean(grad_hat * normed_hat, axis=1, keepdims=True)
    )


def gelu_value(hidden):
    return 0.5 * hidden * (1.0 + lax.erf(hidden * HALF_ROOT))


def gelu_slope(hidden):
    return (
        0.5 * (1.0 + lax.erf(hidden * HALF_ROOT))
        + hidden * jnp.exp(-0.5 * hidden * hidden) * DENSITY
    )


def lanes_to_rows(value):
    pieces = value.shape[2] // WIDE
    return jnp.concatenate(
        [value[:, :, i * WIDE : (i + 1) * WIDE] for i in range(pieces)], axis=1
    )


def rows_to_lanes(value, pieces):
    rows = value.shape[-2] // pieces
    return jnp.concatenate(
        [value[..., i * rows : (i + 1) * rows, :] for i in range(pieces)], axis=-1
    )


def dp_part(value, own, axis=0):
    size = value.shape[axis] // 4
    return lax.dynamic_slice_in_dim(value, own * size, size, axis)


def padded_rows(flat, rows):
    count, size = flat.shape
    return jnp.pad(flat, ((0, 0), (0, rows * WIDE - size))).reshape(count, rows, WIDE)


def body(
    layer_input,
    lengths,
    w_qkv,
    bias_qv,
    w_out,
    bias_out,
    gain_attn,
    shift_attn,
    w_in,
    bias_in,
    w_down,
    bias_down,
    gain_ffn,
    shift_ffn,
    cotangent,
):
    col_grid = lax.axis_size("col")
    rows = layer_input.shape[0]
    row = lax.axis_index("row")
    own_dp = lax.axis_index("dp")
    own_col = lax.axis_index("col")
    group = LEN // rows
    start_row = own_col * rows
    block = min(256, rows)
    blocks = rows // block

    qkv_piece = jnp.swapaxes(dp_part(w_qkv, own_dp), 0, 1)
    depth = qkv_piece.shape[1]
    vectors = jnp.concatenate(
        [bias_out, gain_attn, shift_attn, bias_down, gain_ffn, shift_ffn, bias_in]
    )
    share = bias_out.shape[0]
    vector_rows = 16
    first_piece = jnp.concatenate(
        [
            qkv_piece.reshape(3 * depth, WIDE),
            jnp.pad(bias_qv, ((0, vector_rows - 2), (0, WIDE - share))),
        ],
        axis=0,
    )
    places = places_of()
    if col_grid > 4:
        first_cols = gathered(first_piece, "col")
        bias_col = first_cols[:, 3 * depth :]
        qkv_parts = gathered(first_cols[:, : 3 * depth], "dp")
        w_qkv_half = jnp.transpose(
            qkv_parts.reshape(4, col_grid, 3, depth, PAIRS, LANES), (1, 0, 3, 4, 2, 5)
        ).reshape(D, 3 * WIDE)
    else:
        first_arrived, first_parts = two_level(first_piece, 3 * depth)
        bias_col = jnp.stack(
            picked([one[3 * depth :] for one in [first_piece] + first_arrived], "col")
        )
        w_qkv_half = local_call(
            qkv_kernel,
            places,
            [jnp.swapaxes(w_qkv, 0, 1)] + first_parts,
            jax.ShapeDtypeStruct((D, 3 * WIDE), BF),
        )
    bias_q = bias_col[:, 0, :share].reshape(-1).astype(F32)
    bias_v = bias_col[:, 1, :share].reshape(-1).astype(F32)

    input_full = ordered(row, layer_input, swap(layer_input), 1)
    input_tokens = half_of(input_full, row, 0).astype(F32)
    cot_mine, cot_other = to_tokens(cotangent, row)
    grad_out = ordered(row, cot_mine, cot_other, 1).astype(F32)

    bias_rows = jnp.stack(
        [
            bias_q.reshape(PAIRS, LANES),
            jnp.zeros((PAIRS, LANES), F32),
            bias_v.reshape(PAIRS, LANES),
        ],
        axis=1,
    ).reshape(-1)
    qkv_low = (matmul(input_full, w_qkv_half) + bias_rows[None]).astype(BF)

    def group_perm(offset, back):
        pairs = []
        for i in range(col_grid):
            source = i // group * group + (i + offset) % group
            pairs.append((i, source) if back else (source, i))
        return pairs

    kv_others = []
    for pair in range(PAIRS):
        kv_local = qkv_low[:, (3 * pair + 1) * LANES : (3 * pair + 3) * LANES]
        arrived = [lax.ppermute(kv_local, "col", group_perm(j, False)) for j in range(1, group)]
        kv_others.append(jnp.concatenate(arrived, axis=0))

    down_piece = lanes_to_rows(dp_part(w_down, own_dp)[None])[0]
    in_piece = lanes_to_rows(dp_part(w_in, own_dp)[None])[0]
    if col_grid > 4:
        out_piece = lanes_to_rows(dp_part(w_out, own_dp)[None])[0]
        later_piece = jnp.concatenate([down_piece, in_piece, out_piece], axis=0)
        later_parts = gathered(gathered(later_piece, "col"), "dp")
        vectors_col = gathered(vectors, "col")
        cut_down = down_piece.shape[0]
        cut_in = cut_down + in_piece.shape[0]

        def whole_half(parts, pieces):
            joined = jnp.swapaxes(rows_to_lanes(parts, pieces), 0, 1)
            return joined.reshape(-1, joined.shape[-1])

        w_down_mine = whole_half(later_parts[:, :, :cut_down], 2)
        w_in_mine = whole_half(later_parts[:, :, cut_down:cut_in], 4)
        w_out_mine = whole_half(later_parts[:, :, cut_in:], 2)
    else:
        out_half = w_out.shape[0] // 2
        out_piece = lax.dynamic_slice(
            w_out, (own_dp % 2 * out_half, own_dp // 2 * WIDE), (out_half, WIDE)
        )
        used = down_piece.shape[0] + in_piece.shape[0] + out_half
        later_piece = jnp.concatenate(
            [down_piece, in_piece, out_piece, padded_rows(vectors[None], vector_rows)[0]], axis=0
        )
        later_arrived, later_parts = two_level(later_piece, used)
        vectors_col = jnp.stack(
            picked([one[used:] for one in [later_piece] + later_arrived], "col")
        )
        vectors_col = vectors_col.reshape(col_grid, -1)[:, : vectors.shape[0]]
        w_down_mine, w_in_mine, w_out_mine = local_call(
            later_kernel,
            places,
            [w_down, w_in, w_out] + later_parts,
            (
                jax.ShapeDtypeStruct((4 * w_down.shape[0], D), BF),
                jax.ShapeDtypeStruct((4 * w_in.shape[0], w_in.shape[1]), BF),
                jax.ShapeDtypeStruct((4 * w_out.shape[0], D), BF),
            ),
        )
    vectors_both = swap(vectors_col)

    def vector(at, count=1):
        mine = vectors_col[:, at * share : (at + count) * share].reshape(-1)
        other = vectors_both[:, at * share : (at + count) * share].reshape(-1)
        return mine.astype(F32), other.astype(F32)

    def whole_vector(at):
        mine, other = vector(at)
        return ordered(row, mine, other, 0)[None]

    bias_out_f = whole_vector(0)
    gain_attn_f = whole_vector(1)
    shift_attn_f = whole_vector(2)
    bias_down_f = whole_vector(3)
    gain_ffn_f = whole_vector(4)
    shift_ffn_f = whole_vector(5)
    bias_in_mine, bias_in_other = vector(6, 4)

    w_out_other, w_in_other, w_down_other = swap(w_out_mine), swap(w_in_mine), swap(w_down_mine)

    own_lengths = lax.dynamic_index_in_dim(lengths, start_row // LEN, 0, keepdims=False)
    ends = jnp.cumsum(own_lengths)
    first_place = start_row % LEN
    spots = first_place + jnp.arange(rows, dtype=jnp.int32)
    past = spots[:, None] >= ends[None, :]
    first_key = jnp.max(jnp.where(past, ends[None, :], 0), axis=1)
    past_key = jnp.min(jnp.where(past, LEN, ends[None, :]), axis=1)
    spans = jnp.pad(jnp.stack([first_key, past_key]), ((0, 6), (0, 0)))
    table = jnp.concatenate(
        [
            first_key[::block] // KEY_BLOCK,
            (past_key[block - 1 :: block] + (KEY_BLOCK - 1)) // KEY_BLOCK,
            (first_place // KEY_BLOCK)[None],
        ]
    ).astype(jnp.int32)

    attended = [
        attend_forward(table, qkv_low, kv_others[pair], spans, blocks, pair)
        for pair in range(PAIRS)
    ]
    att_mine, att_other = to_tokens(jnp.concatenate([out for out, _ in attended], axis=1), row)

    projected = matmul(att_mine, w_out_mine) + matmul(att_other, w_out_other)
    first_sum = input_tokens + projected + bias_out_f
    normed, first_hat, first_scale = norm_forward(first_sum, gain_attn_f, shift_attn_f)
    normed_low = normed.astype(BF)
    hidden_mine = matmul(normed_low, w_in_mine) + bias_in_mine[None]
    hidden_other = matmul(normed_low, w_in_other) + bias_in_other[None]
    act_mine = gelu_value(hidden_mine).astype(BF)
    act_other = gelu_value(hidden_other).astype(BF)
    second_sum = (
        normed
        + matmul(act_mine, w_down_mine)
        + matmul(act_other, w_down_other)
        + bias_down_f
    )
    result, second_hat, second_scale = norm_forward(second_sum, gain_ffn_f, shift_ffn_f)
    result = to_features(result.astype(BF), row)

    grad_gain_ffn = jnp.sum(grad_out * second_hat, axis=0)
    grad_shift_ffn = jnp.sum(grad_out, axis=0)
    grad_second = norm_backward(grad_out, second_hat, second_scale, gain_ffn_f)
    grad_bias_down = jnp.sum(grad_second, axis=0)
    grad_ffn = grad_second.astype(BF)
    grad_hidden_mine = (right_inner(grad_ffn, w_down_mine) * gelu_slope(hidden_mine)).astype(BF)
    grad_hidden_other = (right_inner(grad_ffn, w_down_other) * gelu_slope(hidden_other)).astype(BF)
    grad_normed = (
        grad_second
        + right_inner(grad_hidden_mine, w_in_mine)
        + right_inner(grad_hidden_other, w_in_other)
    )
    grad_gain_attn = jnp.sum(grad_normed * first_hat, axis=0)
    grad_shift_attn = jnp.sum(grad_normed, axis=0)
    grad_first = norm_backward(grad_normed, first_hat, first_scale, gain_attn_f)
    grad_bias_out = jnp.sum(grad_first, axis=0)
    grad_proj = grad_first.astype(BF)
    grad_att_mine = right_inner(grad_proj, w_out_mine).astype(BF)
    grad_att_other = right_inner(grad_proj, w_out_other).astype(BF)
    grad_attended = ordered(row, grad_att_mine, swap(grad_att_other), 0)
    grad_first_features = to_features(grad_first, row)

    def both_tokens(mine, other):
        return (mine + swap(other.astype(BF)).astype(F32)).astype(BF)

    grad_down = both_tokens(left_inner(act_mine, grad_ffn), left_inner(act_other, grad_ffn))
    down_dp = reduce_dp(quartered_rows(grad_down, col_grid))
    grad_in_mine = left_inner(normed_low, grad_hidden_mine)
    grad_in_other = left_inner(normed_low, grad_hidden_other).astype(BF)
    grad_in = both_tokens(grad_in_mine, grad_in_other)
    grad_out_w = both_tokens(left_inner(att_mine, grad_proj), left_inner(att_other, grad_proj))
    by_row = jnp.stack(
        [
            grad_bias_out,
            grad_gain_attn,
            grad_shift_attn,
            grad_bias_down,
            grad_gain_ffn,
            grad_shift_ffn,
        ]
    )
    in_mine = jnp.sum(grad_hidden_mine, axis=0, dtype=F32)
    in_other = jnp.sum(grad_hidden_other, axis=0, dtype=F32)

    def vector_block(six, inner):
        split = jnp.swapaxes(six.reshape(6, col_grid, share), 0, 1).reshape(col_grid, -1)
        return jnp.concatenate([split, inner.reshape(col_grid, -1)], axis=1)

    vec_mine = vector_block(half_of(by_row, row, 1), in_mine)
    vec_other = vector_block(half_of(by_row, 1 - row, 1), in_other)
    vec_sum = (vec_mine + swap(vec_other)).astype(BF)

    vec_pad = 16
    early = jnp.concatenate(
        [
            quartered_rows(grad_in, col_grid),
            quartered_halves(grad_out_w, col_grid)
            if col_grid <= 4
            else quartered_rows(grad_out_w, col_grid),
            quartered_vector(vec_sum, vec_pad),
        ],
        axis=2,
    )
    early, grad_attended = lax.optimization_barrier((early, grad_attended))
    early_dp = reduce_dp(early)
    down_parts = spread_dp(reduce_col(down_dp))

    grad_pairs, grad_w_pairs, bias_sums = [], [], []
    for pair in range(PAIRS):
        out, logs = attended[pair]
        grad_query, key_own, value_own, others = attend_backward(
            table, qkv_low, kv_others[pair], spans, out, logs, grad_attended, blocks, pair
        )
        for j in range(1, group):
            arrived = lax.ppermute(
                others[(j - 1) * rows : j * rows], "col", group_perm(j, True)
            ).astype(F32)
            key_own = key_own + arrived[:, :LANES]
            value_own = value_own + arrived[:, LANES:]
        grad_pair = jnp.concatenate(
            [grad_query, key_own.astype(BF), value_own.astype(BF)], axis=1
        )
        grad_pairs.append(grad_pair)
        grad_w_pairs.append(left_inner(input_full, grad_pair).astype(BF))
        bias_sums.append(jnp.sum(grad_pair, axis=0, dtype=F32))
    grad_qkv = jnp.concatenate(grad_pairs, axis=1)

    bias_pair = jnp.stack(
        [
            jnp.concatenate([one[:LANES] for one in bias_sums]),
            jnp.concatenate([one[2 * LANES :] for one in bias_sums]),
        ]
    )
    bias_pair = jnp.swapaxes(bias_pair.reshape(2, col_grid, share), 0, 1).reshape(col_grid, -1)
    pairs_dp = reduce_dp(
        jnp.concatenate([quartered_rows(one, col_grid) for one in grad_w_pairs[:-1]], axis=2),
    )
    early_piece = reduce_col(jnp.concatenate([early_dp, pairs_dp], axis=1))
    early_parts = spread_dp(early_piece)
    late = jnp.concatenate(
        [
            quartered_rows(grad_w_pairs[-1], col_grid),
            quartered_vector(bias_pair.astype(BF), vec_pad),
        ],
        axis=2,
    )
    late_parts = spread_dp(reduce_col(reduce_dp(late)))

    partial = right_inner(grad_qkv, w_qkv_half)
    arrived = swap(half_of(partial, 1 - row, 1).astype(BF)).astype(F32)
    grad_input = grad_first_features + half_of(partial, row, 1) + arrived

    cut_in = w_in.shape[0]
    cut_out = cut_in + w_out.shape[0] // 2
    cut_vec = cut_out + vec_pad
    if col_grid > 4:
        down_all = jnp.stack(picked(down_parts, "dp")).astype(F32)
        early_all = jnp.stack(picked(early_parts, "dp")).astype(F32)
        late_all = jnp.stack(picked(late_parts, "dp")).astype(F32)
        grad_down_own = rows_to_lanes(down_all, 2).reshape(w_down.shape)
        grad_in_own = rows_to_lanes(early_all[:, :cut_in], 4).reshape(w_in.shape)
        grad_out_own = rows_to_lanes(early_all[:, cut_in:cut_out], 2).reshape(w_out.shape)
        qkv_own = jnp.concatenate([early_all[:, cut_vec:], late_all[:, :-vec_pad]], axis=1)
        qkv_own = qkv_own.reshape(4, PAIRS, depth, 3, LANES)
        qkv_own = jnp.transpose(qkv_own, (0, 2, 3, 1, 4)).reshape(w_qkv.shape)
    else:
        grad_down_own = local_call(
            down_out_kernel, places, down_parts, jax.ShapeDtypeStruct(w_down.shape, F32)
        )
        grad_in_own, grad_out_own = local_call(
            in_out_kernel,
            places,
            early_parts,
            tuple(jax.ShapeDtypeStruct(one.shape, F32) for one in (w_in, w_out)),
        )
        qkv_own = local_call(
            functools.partial(qkv_out_kernel, cut_vec),
            places,
            early_parts + late_parts,
            jax.ShapeDtypeStruct((3, w_qkv.shape[0], WIDE), F32),
        )
        qkv_own = jnp.swapaxes(qkv_own, 0, 1)
    vec_own = first_quarter(early_parts, cut_out, vec_pad)
    vecs = [vec_own[i * share : (i + 1) * share] for i in range(6)]
    bias_in_own = vec_own[6 * share : 10 * share]
    bias_own = first_quarter(late_parts, depth, vec_pad)[: 2 * share].reshape(2, share)
    return (
        result,
        grad_input,
        qkv_own,
        bias_own,
        grad_out_own,
        vecs[0],
        vecs[1],
        vecs[2],
        grad_in_own,
        bias_in_own,
        grad_down_own,
        vecs[3],
        vecs[4],
        vecs[5],
    )


def solution(mesh):
    both = P(("row", "col"))
    specs = (
        P("col", None, "row"),
        P(None, ("row", "col")),
        P(("row", "col"), None),
        both,
        both,
        both,
        P("col", "row"),
        both,
        P(("row", "col"), None),
        both,
        both,
        both,
    )
    tokens = P(("dp", "col"), "row")
    return jax.shard_map(
        body,
        mesh=mesh,
        in_specs=(tokens, P("dp", None)) + specs + (tokens,),
        out_specs=(tokens, tokens) + specs,
        check_vma=False,
    )
```

```python
import functools

import jax
import jax.numpy as jnp
from jax import lax
from jax.experimental import pallas as pl
from jax.experimental.pallas import tpu as pltpu
from jax.sharding import PartitionSpec as P


D = 768
HD = 64
LEN = 2048
WIDE = 384
LANES = 128
PAIRS = WIDE // LANES

EPSILON = 1e-12
MASKED = -1e30
HALF_ROOT = 0.7071067811865476
DENSITY = 0.3989422804014327
BF = jnp.bfloat16
F32 = jnp.float32


def matmul(left_mat, right_mat):
    return jnp.dot(left_mat, right_mat, preferred_element_type=F32)


def left_inner(left_mat, right_mat):
    return lax.dot_general(
        left_mat, right_mat, (((0,), (0,)), ((), ())), preferred_element_type=F32
    )


def right_inner(left_mat, right_mat):
    return lax.dot_general(
        left_mat, right_mat, (((1,), (1,)), ((), ())), preferred_element_type=F32
    )


def swap(value):
    return lax.ppermute(value, "row", [(0, 1), (1, 0)])


def ordered(row, mine, other, axis):
    return jnp.where(
        row == 0,
        jnp.concatenate([mine, other], axis=axis),
        jnp.concatenate([other, mine], axis=axis),
    )


def half_of(value, which, axis):
    size = value.shape[axis] // 2
    return lax.dynamic_slice_in_dim(value, which * size, size, axis)


def to_tokens(value, row):
    return half_of(value, row, 0), swap(half_of(value, 1 - row, 0))


def to_features(value, row):
    other = swap(half_of(value, 1 - row, 1))
    return ordered(row, half_of(value, row, 1), other, 0)


def xor_swap(value, axis, mask):
    count = lax.axis_size(axis)
    return lax.ppermute(value, axis, [(i, i ^ mask) for i in range(count)])


def picked(parts, axis):
    stacked = jnp.stack(parts)
    own = lax.axis_index(axis)
    return [
        lax.dynamic_index_in_dim(stacked, own ^ i, 0, keepdims=False) for i in range(len(parts))
    ]


def gathered(value, axis):
    count = lax.axis_size(axis)
    if count > 4:
        return lax.all_gather(value, axis, axis=0)
    parts = [value] + [xor_swap(value, axis, k) for k in range(1, count)]
    return jnp.stack(picked(parts, axis))


def two_level(piece, used):
    arrived = []
    for k in range(1, lax.axis_size("col")):
        arrived.append(xor_swap(piece, "col", k))
    ours = jnp.stack([one[:used] for one in arrived])
    return arrived, [ours] + [xor_swap(ours, "dp", j) for j in range(1, 4)]


def reduce_dp(quarters):
    own = lax.axis_index("dp")

    def part(k):
        return lax.dynamic_index_in_dim(quarters, own ^ k, 1, keepdims=False)

    arrived = []
    for k in range(1, 4):
        arrived.append(xor_swap(part(k), "dp", k))
    total = part(0).astype(F32)
    for one in arrived:
        total = total + one.astype(F32)
    return total.astype(BF)


def reduce_col(ours):
    count = lax.axis_size("col")
    if count > 4:
        return lax.psum_scatter(ours, "col", scatter_dimension=0, tiled=False)
    own = lax.axis_index("col")

    def part(k):
        return lax.dynamic_index_in_dim(ours, own ^ k, 0, keepdims=False)

    arrived = []
    for k in range(1, count):
        arrived.append(xor_swap(part(k), "col", k))
    total = part(0).astype(F32)
    for one in arrived:
        total = total + one.astype(F32)
    return total.astype(BF)


def spread_dp(piece):
    parts = [piece]
    for k in range(1, 4):
        parts.append(xor_swap(piece, "dp", k))
    return parts


def places_of():
    return jnp.stack([lax.axis_index("col"), lax.axis_index("dp")]).astype(jnp.int32)


def at_rows(start, count):
    return pl.ds(pl.multiple_of(start, 16), count)


def local_call(kernel, places, inputs, outs):
    spec = pl.BlockSpec(memory_space=pltpu.VMEM)
    return pl.pallas_call(
        kernel,
        out_shape=outs,
        in_specs=[pl.BlockSpec(memory_space=pltpu.SMEM)] + [spec] * len(inputs),
        out_specs=jax.tree.map(lambda _: spec, outs),
        cost_estimate=pl.CostEstimate(flops=0, bytes_accessed=4 << 20, transcendentals=0),
    )(places, *inputs)


def qkv_kernel(places, own, *refs):
    parts, out = refs[:-1], refs[-1]
    col, dp = places[0], places[1]
    share = own.shape[1]
    depth = share // 4
    for kind in range(3):
        for pair in range(PAIRS):
            lanes = slice((3 * pair + kind) * LANES, (3 * pair + kind + 1) * LANES)
            source = slice(pair * LANES, (pair + 1) * LANES)
            out[at_rows(col * share, share), lanes] = own[kind, :, source]
            for j in range(4):
                for k in range(1, 4):
                    rows = at_rows((col ^ k) * share + (dp ^ j) * depth, depth)
                    out[rows, lanes] = parts[j][
                        k - 1, kind * depth : (kind + 1) * depth, source
                    ]


def later_kernel(places, own_down, own_in, own_out, *refs):
    parts, (down, inner, out) = refs[:-3], refs[-3:]
    col, dp = places[0], places[1]
    wide_rows, deep_rows, out_rows = own_down.shape[0], own_in.shape[0], own_out.shape[0]
    down[at_rows(col * wide_rows, wide_rows), :] = own_down[...]
    inner[at_rows(col * deep_rows, deep_rows), :] = own_in[...]
    out[at_rows(col * out_rows, out_rows), :] = own_out[...]
    for j in range(4):
        there = dp ^ j
        for k in range(1, 4):
            part = parts[j].at[k - 1]
            count, at = wide_rows // 4, 0
            rows = at_rows((col ^ k) * wide_rows + there * count, count)
            for i in range(2):
                down[rows, i * WIDE : (i + 1) * WIDE] = part[at : at + count, :]
                at += count
            count = deep_rows // 4
            rows = at_rows((col ^ k) * deep_rows + there * count, count)
            for i in range(4):
                inner[rows, i * WIDE : (i + 1) * WIDE] = part[at : at + count, :]
                at += count
            count = out_rows // 2
            rows = at_rows((col ^ k) * out_rows + lax.rem(there, 2) * count, count)
            lanes = pl.ds(pl.multiple_of(there // 2 * WIDE, LANES), WIDE)
            out[rows, lanes] = part[at : at + count, :]


def down_out_kernel(places, *refs):
    parts, down = refs[:-1], refs[-1]
    dp = places[1]
    count = down.shape[0] // 4
    for j in range(4):
        for i in range(2):
            down[at_rows((dp ^ j) * count, count), i * WIDE : (i + 1) * WIDE] = parts[j][
                i * count : (i + 1) * count, :
            ].astype(F32)


def in_out_kernel(places, *refs):
    parts, (inner, out) = refs[:-2], refs[-2:]
    dp = places[1]
    for j in range(4):
        there = dp ^ j
        count, at = inner.shape[0] // 4, 0
        for i in range(4):
            inner[at_rows(there * count, count), i * WIDE : (i + 1) * WIDE] = parts[j][
                at : at + count, :
            ].astype(F32)
            at += count
        count = out.shape[0] // 2
        lanes = pl.ds(pl.multiple_of(there // 2 * WIDE, LANES), WIDE)
        out[at_rows(lax.rem(there, 2) * count, count), lanes] = parts[j][
            at : at + count, :
        ].astype(F32)


def qkv_out_kernel(first_row, places, *refs):
    parts, last_parts, out = refs[:4], refs[4:8], refs[8]
    dp = places[1]
    count = out.shape[1] // 4
    for j in range(4):
        rows = at_rows((dp ^ j) * count, count)
        for pair in range(PAIRS):
            source = last_parts[j] if pair == PAIRS - 1 else parts[j]
            start = 0 if pair == PAIRS - 1 else first_row + pair * count
            for kind in range(3):
                out[kind, rows, pair * LANES : (pair + 1) * LANES] = source[
                    start : start + count, kind * LANES : (kind + 1) * LANES
                ].astype(F32)


def quartered_rows(value, count):
    pieces = value.shape[1] // WIDE
    cut = value.reshape(count, 4, -1, value.shape[1])
    return jnp.concatenate(
        [cut[..., i * WIDE : (i + 1) * WIDE] for i in range(pieces)], axis=2
    )


def quartered_halves(value, count):
    cut = value.reshape(count, 2, -1, 2 * WIDE)
    return jnp.concatenate([cut[..., :WIDE], cut[..., WIDE:]], axis=1)


def quartered_vector(flat, rows):
    count, size = flat.shape
    return jnp.pad(flat, ((0, 0), (0, 4 * rows * WIDE - size))).reshape(count, 4, rows, WIDE)


def first_quarter(parts, start, rows):
    stacked = jnp.stack([one[start : start + rows] for one in parts])
    return lax.dynamic_index_in_dim(
        stacked, lax.axis_index("dp"), 0, keepdims=False
    ).astype(F32).reshape(-1)


def stack_heads(value):
    lane = lax.broadcasted_iota(jnp.int32, value.shape, 1)
    zero = jnp.zeros_like(value)
    return jnp.concatenate(
        [jnp.where(lane < HD, value, zero), jnp.where(lane >= HD, value, zero)], axis=0
    )


def join_heads(value, block):
    lane = lax.broadcasted_iota(jnp.int32, (LANES, block), 0)
    return jnp.where(lane < HD, value[:, :block], value[:, block:]).T


def doubled(value):
    return jnp.concatenate([value, value], axis=1)


def mask_bias(key_place, first_key, past_key):
    places = key_place + lax.broadcasted_iota(jnp.int32, (key_place_rows(), first_key.shape[1]), 0)
    inside = (places >= first_key) & (places < past_key)
    return doubled(jnp.where(inside, 0.0, MASKED))


KEY_BLOCK = 256


def key_place_rows():
    return KEY_BLOCK


def copy_blocks(dest, own, others, rows):
    dest[:rows, :] = own[...]
    dest[rows:, :] = others[...]


def forward_kernel(
    blocks, table, q_ref, k_ref, v_ref, ko_ref, vo_ref, span_ref, out_ref, log_ref, keys, values
):
    rows = q_ref.shape[0]
    block = rows // blocks
    copy_blocks(keys, k_ref, ko_ref, rows)
    copy_blocks(values, v_ref, vo_ref, rows)
    slots = keys.shape[0] // KEY_BLOCK
    base = table[2 * blocks]

    @pl.loop(0, blocks)
    def _(at):
        here = pl.ds(pl.multiple_of(at * block, block), block)
        wide = pl.ds(pl.multiple_of(at * 2 * block, 2 * block), 2 * block)
        query = stack_heads((q_ref[here, :].astype(F32) * 0.125).astype(BF))
        first_key = span_ref[0:1, here]
        past_key = span_ref[1:2, here]

        def step(place, running):
            peak, total, summed = running
            slot = lax.rem(place - base + slots, slots)
            rows_at = pl.ds(pl.multiple_of(slot * KEY_BLOCK, KEY_BLOCK), KEY_BLOCK)
            scores = right_inner(keys[rows_at, :], query)
            scores = scores + mask_bias(place * KEY_BLOCK, first_key, past_key)
            higher = jnp.maximum(peak, jnp.max(scores, axis=0, keepdims=True))
            raised = jnp.exp(scores - higher)
            fade = jnp.exp(peak - higher)
            total = total * fade + jnp.sum(raised, axis=0, keepdims=True)
            summed = summed * fade + left_inner(values[rows_at, :], raised.astype(BF))
            return (higher, total, summed)

        init = (
            jnp.full((1, 2 * block), MASKED, F32),
            jnp.zeros((1, 2 * block), F32),
            jnp.zeros((LANES, 2 * block), F32),
        )
        peak, total, summed = lax.fori_loop(table[at], table[blocks + at], step, init)
        out_ref[here, :] = join_heads(summed / total, block).astype(BF)
        log_ref[:, wide] = jnp.broadcast_to(
            peak + jnp.log(total), (8, 2 * block)
        )


def backward_block(blocks, rows, at, refs, key_at, spans_of_keys, before):
    q_ref, span_ref, out_ref, log_ref, grad_ref, keys, values, key_sum, value_sum = refs
    block = rows // blocks
    here = pl.ds(pl.multiple_of(at * block, block), block)
    wide = pl.ds(pl.multiple_of(at * 2 * block, 2 * block), 2 * block)
    query = stack_heads((q_ref[here, :].astype(F32) * 0.125).astype(BF))
    grad = stack_heads(grad_ref[here, :])
    along = (grad_ref[here, :].astype(F32) * out_ref[here, :].astype(F32)).T
    dots = jnp.concatenate(
        [
            jnp.sum(along[:HD], axis=0, keepdims=True),
            jnp.sum(along[HD:], axis=0, keepdims=True),
        ],
        axis=1,
    )
    logs = log_ref[0:1, wide]
    first_key = span_ref[0:1, here]
    past_key = span_ref[1:2, here]

    def step(place, summed):
        rows_at = pl.ds(pl.multiple_of(key_at(place) * KEY_BLOCK, KEY_BLOCK), KEY_BLOCK)
        key = keys[rows_at, :]
        scores = right_inner(key, query)
        scores = scores + mask_bias(place * KEY_BLOCK, first_key, past_key)
        weights = jnp.exp(scores - logs)
        grad_weights = right_inner(values[rows_at, :], grad)
        value_sum[rows_at, :] += matmul(weights.astype(BF), grad)
        grad_scores = (weights * (grad_weights - dots)).astype(BF)
        key_sum[rows_at, :] += matmul(grad_scores, query)
        return summed + left_inner(key, grad_scores)

    for low, high in spans_of_keys:
        before = lax.fori_loop(low, high, step, before)
    return here, before


def backward_others_kernel(
    blocks,
    table,
    q_ref,
    ko_ref,
    vo_ref,
    span_ref,
    out_ref,
    log_ref,
    grad_ref,
    dq_ref,
    others_ref,
    key_sum,
    value_sum,
):
    rows = q_ref.shape[0]
    block = rows // blocks
    own = rows // KEY_BLOCK
    slots = own + ko_ref.shape[0] // KEY_BLOCK
    base = table[2 * blocks]
    key_sum[...] = jnp.zeros_like(key_sum)
    value_sum[...] = jnp.zeros_like(value_sum)
    refs = (q_ref, span_ref, out_ref, log_ref, grad_ref, ko_ref, vo_ref, key_sum, value_sum)

    def key_at(place):
        return lax.rem(place - base + slots, slots) - own

    @pl.loop(0, blocks)
    def _(at):
        low, high = table[at], table[blocks + at]
        ranges = ((low, jnp.minimum(high, base)), (jnp.maximum(low, base + own), high))
        here, summed = backward_block(
            blocks, rows, at, refs, key_at, ranges, jnp.zeros((LANES, 2 * block), F32)
        )
        dq_ref[here, :] = join_heads(summed, block)

    others_ref[:, :LANES] = key_sum[...].astype(BF)
    others_ref[:, LANES:] = value_sum[...].astype(BF)


def backward_own_kernel(
    blocks,
    table,
    q_ref,
    k_ref,
    v_ref,
    span_ref,
    out_ref,
    log_ref,
    grad_ref,
    part_ref,
    dq_ref,
    dk_ref,
    dv_ref,
):
    rows = q_ref.shape[0]
    block = rows // blocks
    own = rows // KEY_BLOCK
    base = table[2 * blocks]
    dk_ref[...] = jnp.zeros_like(dk_ref)
    dv_ref[...] = jnp.zeros_like(dv_ref)
    refs = (q_ref, span_ref, out_ref, log_ref, grad_ref, k_ref, v_ref, dk_ref, dv_ref)

    @pl.loop(0, blocks)
    def _(at):
        low, high = table[at], table[blocks + at]
        ranges = ((jnp.maximum(low, base), jnp.minimum(high, base + own)),)
        here, summed = backward_block(
            blocks,
            rows,
            at,
            refs,
            lambda place: place - base,
            ranges,
            jnp.zeros((LANES, 2 * block), F32),
        )
        dq_ref[here, :] = ((part_ref[here, :] + join_heads(summed, block)) * 0.125).astype(BF)


def attention_specs(rows, others, pair):
    return [
        pl.BlockSpec((rows, LANES), lambda g, t: (0, 3 * pair)),
        pl.BlockSpec((rows, LANES), lambda g, t: (0, 3 * pair + 1)),
        pl.BlockSpec((rows, LANES), lambda g, t: (0, 3 * pair + 2)),
        pl.BlockSpec((others, LANES), lambda g, t: (0, 0)),
        pl.BlockSpec((others, LANES), lambda g, t: (0, 1)),
        pl.BlockSpec((8, rows), lambda g, t: (0, 0)),
    ]


def attend_forward(table, qkv, kv_others, spans, blocks, pair):
    rows, others = qkv.shape[0], kv_others.shape[0]
    return pl.pallas_call(
        functools.partial(forward_kernel, blocks),
        out_shape=(
            jax.ShapeDtypeStruct((rows, LANES), BF),
            jax.ShapeDtypeStruct((8, 2 * rows), F32),
        ),
        grid_spec=pltpu.PrefetchScalarGridSpec(
            num_scalar_prefetch=1,
            grid=(1,),
            in_specs=attention_specs(rows, others, pair),
            out_specs=(
                pl.BlockSpec((rows, LANES), lambda g, t: (0, 0)),
                pl.BlockSpec((8, 2 * rows), lambda g, t: (0, 0)),
            ),
            scratch_shapes=[pltpu.VMEM((rows + others, LANES), BF)] * 2,
        ),
        cost_estimate=pl.CostEstimate(
            flops=8 * rows * LEN * LANES, bytes_accessed=8 * rows * LANES, transcendentals=0
        ),
        name="attend_forward",
    )(table, qkv, qkv, qkv, kv_others, kv_others, spans)


def backward_call(kernel, table, inputs, in_specs, outs, out_specs, scratch, rows):
    return pl.pallas_call(
        kernel,
        out_shape=outs,
        grid_spec=pltpu.PrefetchScalarGridSpec(
            num_scalar_prefetch=1,
            grid=(1,),
            in_specs=in_specs,
            out_specs=out_specs,
            scratch_shapes=scratch,
        ),
        cost_estimate=pl.CostEstimate(
            flops=10 * rows * LEN * LANES, bytes_accessed=16 * rows * LANES, transcendentals=0
        ),
    )(table, *inputs)


def attend_backward_others(table, qkv, kv_others, spans, out, logs, grad, blocks, pair):
    rows, others = qkv.shape[0], kv_others.shape[0]
    specs = attention_specs(rows, others, pair)
    whole = pl.BlockSpec((rows, LANES), lambda g, t: (0, 0))
    mine = pl.BlockSpec((rows, LANES), lambda g, t: (0, pair))
    logs_spec = pl.BlockSpec((8, 2 * rows), lambda g, t: (0, 0))
    return backward_call(
        functools.partial(backward_others_kernel, blocks),
        table,
        (qkv, kv_others, kv_others, spans, out, logs, grad),
        [specs[0]] + specs[3:] + [whole, logs_spec, mine],
        (
            jax.ShapeDtypeStruct((rows, LANES), F32),
            jax.ShapeDtypeStruct((others, 2 * LANES), BF),
        ),
        (whole, pl.BlockSpec((others, 2 * LANES), lambda g, t: (0, 0))),
        [pltpu.VMEM((others, LANES), F32)] * 2,
        rows,
    )


def attend_backward_own(table, qkv, spans, out, logs, grad, part, blocks, pair):
    rows = qkv.shape[0]
    specs = attention_specs(rows, rows, pair)
    whole = pl.BlockSpec((rows, LANES), lambda g, t: (0, 0))
    mine = pl.BlockSpec((rows, LANES), lambda g, t: (0, pair))
    logs_spec = pl.BlockSpec((8, 2 * rows), lambda g, t: (0, 0))
    return backward_call(
        functools.partial(backward_own_kernel, blocks),
        table,
        (qkv, qkv, qkv, spans, out, logs, grad, part),
        specs[:3] + [specs[5], whole, logs_spec, mine, whole],
        (
            jax.ShapeDtypeStruct((rows, LANES), BF),
            jax.ShapeDtypeStruct((rows, LANES), F32),
            jax.ShapeDtypeStruct((rows, LANES), F32),
        ),
        (whole, whole, whole),
        [],
        rows,
    )


def norm_forward(summed, gain_vec, shift_vec):
    center = jnp.mean(summed, axis=1, keepdims=True)
    centered = summed - center
    spread = jnp.mean(centered * centered, axis=1, keepdims=True)
    inv_scale = lax.rsqrt(spread + EPSILON)
    normed_hat = centered * inv_scale
    return (normed_hat * gain_vec + shift_vec, normed_hat, inv_scale)


def norm_backward(grad_vals, normed_hat, inv_scale, gain_vec):
    grad_hat = grad_vals * gain_vec
    return inv_scale * (
        grad_hat
        - jnp.mean(grad_hat, axis=1, keepdims=True)
        - normed_hat * jnp.mean(grad_hat * normed_hat, axis=1, keepdims=True)
    )


def gelu_value(hidden):
    return 0.5 * hidden * (1.0 + lax.erf(hidden * HALF_ROOT))


def gelu_slope(hidden):
    return (
        0.5 * (1.0 + lax.erf(hidden * HALF_ROOT))
        + hidden * jnp.exp(-0.5 * hidden * hidden) * DENSITY
    )


def lanes_to_rows(value):
    pieces = value.shape[2] // WIDE
    return jnp.concatenate(
        [value[:, :, i * WIDE : (i + 1) * WIDE] for i in range(pieces)], axis=1
    )


def rows_to_lanes(value, pieces):
    rows = value.shape[-2] // pieces
    return jnp.concatenate(
        [value[..., i * rows : (i + 1) * rows, :] for i in range(pieces)], axis=-1
    )


def dp_part(value, own, axis=0):
    size = value.shape[axis] // 4
    return lax.dynamic_slice_in_dim(value, own * size, size, axis)


def padded_rows(flat, rows):
    count, size = flat.shape
    return jnp.pad(flat, ((0, 0), (0, rows * WIDE - size))).reshape(count, rows, WIDE)


def body(
    layer_input,
    lengths,
    w_qkv,
    bias_qv,
    w_out,
    bias_out,
    gain_attn,
    shift_attn,
    w_in,
    bias_in,
    w_down,
    bias_down,
    gain_ffn,
    shift_ffn,
    cotangent,
):
    col_grid = lax.axis_size("col")
    rows = layer_input.shape[0]
    row = lax.axis_index("row")
    own_dp = lax.axis_index("dp")
    own_col = lax.axis_index("col")
    group = LEN // rows
    start_row = own_col * rows
    block = min(256, rows)
    blocks = rows // block

    qkv_piece = jnp.swapaxes(dp_part(w_qkv, own_dp), 0, 1)
    depth = qkv_piece.shape[1]
    vectors = jnp.concatenate(
        [bias_out, gain_attn, shift_attn, bias_down, gain_ffn, shift_ffn, bias_in]
    )
    share = bias_out.shape[0]
    vector_rows = 16
    first_piece = jnp.concatenate(
        [
            qkv_piece.reshape(3 * depth, WIDE),
            jnp.pad(bias_qv, ((0, vector_rows - 2), (0, WIDE - share))),
        ],
        axis=0,
    )
    places = places_of()
    if col_grid > 4:
        first_cols = gathered(first_piece, "col")
        bias_col = first_cols[:, 3 * depth :]
        qkv_parts = gathered(first_cols[:, : 3 * depth], "dp")
        w_qkv_half = jnp.transpose(
            qkv_parts.reshape(4, col_grid, 3, depth, PAIRS, LANES), (1, 0, 3, 4, 2, 5)
        ).reshape(D, 3 * WIDE)
    else:
        first_arrived, first_parts = two_level(first_piece, 3 * depth)
        bias_col = jnp.stack(
            picked([one[3 * depth :] for one in [first_piece] + first_arrived], "col")
        )
        w_qkv_half = local_call(
            qkv_kernel,
            places,
            [jnp.swapaxes(w_qkv, 0, 1)] + first_parts,
            jax.ShapeDtypeStruct((D, 3 * WIDE), BF),
        )
    bias_q = bias_col[:, 0, :share].reshape(-1).astype(F32)
    bias_v = bias_col[:, 1, :share].reshape(-1).astype(F32)

    input_full = ordered(row, layer_input, swap(layer_input), 1)
    input_tokens = half_of(input_full, row, 0).astype(F32)
    cot_mine, cot_other = to_tokens(cotangent, row)
    grad_out = ordered(row, cot_mine, cot_other, 1).astype(F32)

    bias_rows = jnp.stack(
        [
            bias_q.reshape(PAIRS, LANES),
            jnp.zeros((PAIRS, LANES), F32),
            bias_v.reshape(PAIRS, LANES),
        ],
        axis=1,
    ).reshape(-1)
    qkv_low = (matmul(input_full, w_qkv_half) + bias_rows[None]).astype(BF)

    def group_perm(offset, back):
        pairs = []
        for i in range(col_grid):
            source = i // group * group + (i + offset) % group
            pairs.append((i, source) if back else (source, i))
        return pairs

    kv_others = []
    for pair in range(PAIRS):
        kv_local = qkv_low[:, (3 * pair + 1) * LANES : (3 * pair + 3) * LANES]
        arrived = [lax.ppermute(kv_local, "col", group_perm(j, False)) for j in range(1, group)]
        kv_others.append(jnp.concatenate(arrived, axis=0))

    down_piece = lanes_to_rows(dp_part(w_down, own_dp)[None])[0]
    in_piece = lanes_to_rows(dp_part(w_in, own_dp)[None])[0]
    if col_grid > 4:
        out_piece = lanes_to_rows(dp_part(w_out, own_dp)[None])[0]
        later_piece = jnp.concatenate([down_piece, in_piece, out_piece], axis=0)
        later_parts = gathered(gathered(later_piece, "col"), "dp")
        vectors_col = gathered(vectors, "col")
        cut_down = down_piece.shape[0]
        cut_in = cut_down + in_piece.shape[0]

        def whole_half(parts, pieces):
            joined = jnp.swapaxes(rows_to_lanes(parts, pieces), 0, 1)
            return joined.reshape(-1, joined.shape[-1])

        w_down_mine = whole_half(later_parts[:, :, :cut_down], 2)
        w_in_mine = whole_half(later_parts[:, :, cut_down:cut_in], 4)
        w_out_mine = whole_half(later_parts[:, :, cut_in:], 2)
    else:
        out_half = w_out.shape[0] // 2
        out_piece = lax.dynamic_slice(
            w_out, (own_dp % 2 * out_half, own_dp // 2 * WIDE), (out_half, WIDE)
        )
        used = down_piece.shape[0] + in_piece.shape[0] + out_half
        later_piece = jnp.concatenate(
            [down_piece, in_piece, out_piece, padded_rows(vectors[None], vector_rows)[0]], axis=0
        )
        later_arrived, later_parts = two_level(later_piece, used)
        vectors_col = jnp.stack(
            picked([one[used:] for one in [later_piece] + later_arrived], "col")
        )
        vectors_col = vectors_col.reshape(col_grid, -1)[:, : vectors.shape[0]]
        w_down_mine, w_in_mine, w_out_mine = local_call(
            later_kernel,
            places,
            [w_down, w_in, w_out] + later_parts,
            (
                jax.ShapeDtypeStruct((4 * w_down.shape[0], D), BF),
                jax.ShapeDtypeStruct((4 * w_in.shape[0], w_in.shape[1]), BF),
                jax.ShapeDtypeStruct((4 * w_out.shape[0], D), BF),
            ),
        )
    vectors_both = swap(vectors_col)

    def vector(at, count=1):
        mine = vectors_col[:, at * share : (at + count) * share].reshape(-1)
        other = vectors_both[:, at * share : (at + count) * share].reshape(-1)
        return mine.astype(F32), other.astype(F32)

    def whole_vector(at):
        mine, other = vector(at)
        return ordered(row, mine, other, 0)[None]

    bias_out_f = whole_vector(0)
    gain_attn_f = whole_vector(1)
    shift_attn_f = whole_vector(2)
    bias_down_f = whole_vector(3)
    gain_ffn_f = whole_vector(4)
    shift_ffn_f = whole_vector(5)
    bias_in_mine, bias_in_other = vector(6, 4)

    w_out_other, w_in_other, w_down_other = swap(w_out_mine), swap(w_in_mine), swap(w_down_mine)

    own_lengths = lax.dynamic_index_in_dim(lengths, start_row // LEN, 0, keepdims=False)
    ends = jnp.cumsum(own_lengths)
    first_place = start_row % LEN
    spots = first_place + jnp.arange(rows, dtype=jnp.int32)
    past = spots[:, None] >= ends[None, :]
    first_key = jnp.max(jnp.where(past, ends[None, :], 0), axis=1)
    past_key = jnp.min(jnp.where(past, LEN, ends[None, :]), axis=1)
    spans = jnp.pad(jnp.stack([first_key, past_key]), ((0, 6), (0, 0)))
    table = jnp.concatenate(
        [
            first_key[::block] // KEY_BLOCK,
            (past_key[block - 1 :: block] + (KEY_BLOCK - 1)) // KEY_BLOCK,
            (first_place // KEY_BLOCK)[None],
        ]
    ).astype(jnp.int32)

    attended = [
        attend_forward(table, qkv_low, kv_others[pair], spans, blocks, pair)
        for pair in range(PAIRS)
    ]
    att_mine, att_other = to_tokens(jnp.concatenate([out for out, _ in attended], axis=1), row)

    projected = matmul(att_mine, w_out_mine) + matmul(att_other, w_out_other)
    first_sum = input_tokens + projected + bias_out_f
    normed, first_hat, first_scale = norm_forward(first_sum, gain_attn_f, shift_attn_f)
    normed_low = normed.astype(BF)
    hidden_mine = matmul(normed_low, w_in_mine) + bias_in_mine[None]
    hidden_other = matmul(normed_low, w_in_other) + bias_in_other[None]
    act_mine = gelu_value(hidden_mine).astype(BF)
    act_other = gelu_value(hidden_other).astype(BF)
    second_sum = (
        normed
        + matmul(act_mine, w_down_mine)
        + matmul(act_other, w_down_other)
        + bias_down_f
    )
    result, second_hat, second_scale = norm_forward(second_sum, gain_ffn_f, shift_ffn_f)
    result = to_features(result.astype(BF), row)

    grad_gain_ffn = jnp.sum(grad_out * second_hat, axis=0)
    grad_shift_ffn = jnp.sum(grad_out, axis=0)
    grad_second = norm_backward(grad_out, second_hat, second_scale, gain_ffn_f)
    grad_bias_down = jnp.sum(grad_second, axis=0)
    grad_ffn = grad_second.astype(BF)
    grad_hidden_mine = (right_inner(grad_ffn, w_down_mine) * gelu_slope(hidden_mine)).astype(BF)
    grad_hidden_other = (right_inner(grad_ffn, w_down_other) * gelu_slope(hidden_other)).astype(BF)
    grad_normed = (
        grad_second
        + right_inner(grad_hidden_mine, w_in_mine)
        + right_inner(grad_hidden_other, w_in_other)
    )
    grad_gain_attn = jnp.sum(grad_normed * first_hat, axis=0)
    grad_shift_attn = jnp.sum(grad_normed, axis=0)
    grad_first = norm_backward(grad_normed, first_hat, first_scale, gain_attn_f)
    grad_bias_out = jnp.sum(grad_first, axis=0)
    grad_proj = grad_first.astype(BF)
    grad_att_mine = right_inner(grad_proj, w_out_mine).astype(BF)
    grad_att_other = right_inner(grad_proj, w_out_other).astype(BF)
    grad_attended = ordered(row, grad_att_mine, swap(grad_att_other), 0)
    grad_first_features = to_features(grad_first, row)

    def both_tokens(mine, other):
        return (mine + swap(other.astype(BF)).astype(F32)).astype(BF)

    grad_down = both_tokens(left_inner(act_mine, grad_ffn), left_inner(act_other, grad_ffn))
    down_dp = reduce_dp(quartered_rows(grad_down, col_grid))
    grad_in_mine = left_inner(normed_low, grad_hidden_mine)
    grad_in_other = left_inner(normed_low, grad_hidden_other).astype(BF)
    grad_in = both_tokens(grad_in_mine, grad_in_other)
    grad_out_w = both_tokens(left_inner(att_mine, grad_proj), left_inner(att_other, grad_proj))
    by_row = jnp.stack(
        [
            grad_bias_out,
            grad_gain_attn,
            grad_shift_attn,
            grad_bias_down,
            grad_gain_ffn,
            grad_shift_ffn,
        ]
    )
    in_mine = jnp.sum(grad_hidden_mine, axis=0, dtype=F32)
    in_other = jnp.sum(grad_hidden_other, axis=0, dtype=F32)

    def vector_block(six, inner):
        split = jnp.swapaxes(six.reshape(6, col_grid, share), 0, 1).reshape(col_grid, -1)
        return jnp.concatenate([split, inner.reshape(col_grid, -1)], axis=1)

    vec_mine = vector_block(half_of(by_row, row, 1), in_mine)
    vec_other = vector_block(half_of(by_row, 1 - row, 1), in_other)
    vec_sum = (vec_mine + swap(vec_other)).astype(BF)

    vec_pad = 16
    early = jnp.concatenate(
        [
            quartered_rows(grad_in, col_grid),
            quartered_halves(grad_out_w, col_grid)
            if col_grid <= 4
            else quartered_rows(grad_out_w, col_grid),
            quartered_vector(vec_sum, vec_pad),
        ],
        axis=2,
    )
    early, grad_attended = lax.optimization_barrier((early, grad_attended))
    early_dp = reduce_dp(early)
    down_parts = spread_dp(reduce_col(down_dp))

    first_pass = []
    for pair in range(PAIRS):
        out, logs = attended[pair]
        first_pass.append(
            attend_backward_others(
                table, qkv_low, kv_others[pair], spans, out, logs, grad_attended, blocks, pair
            )
        )
    query_parts = lax.optimization_barrier(tuple(part for part, _ in first_pass))
    grad_pairs, grad_w_pairs, bias_sums = [], [], []
    for pair in range(PAIRS):
        out, logs = attended[pair]
        others = first_pass[pair][1]
        grad_query, key_own, value_own = attend_backward_own(
            table, qkv_low, spans, out, logs, grad_attended, query_parts[pair], blocks, pair
        )
        for j in range(1, group):
            arrived = lax.ppermute(
                others[(j - 1) * rows : j * rows], "col", group_perm(j, True)
            ).astype(F32)
            key_own = key_own + arrived[:, :LANES]
            value_own = value_own + arrived[:, LANES:]
        grad_pair = jnp.concatenate(
            [grad_query, key_own.astype(BF), value_own.astype(BF)], axis=1
        )
        grad_pairs.append(grad_pair)
        grad_w_pairs.append(left_inner(input_full, grad_pair).astype(BF))
        bias_sums.append(jnp.sum(grad_pair, axis=0, dtype=F32))
    grad_qkv = jnp.concatenate(grad_pairs, axis=1)

    bias_pair = jnp.stack(
        [
            jnp.concatenate([one[:LANES] for one in bias_sums]),
            jnp.concatenate([one[2 * LANES :] for one in bias_sums]),
        ]
    )
    bias_pair = jnp.swapaxes(bias_pair.reshape(2, col_grid, share), 0, 1).reshape(col_grid, -1)
    pairs_dp = reduce_dp(
        jnp.concatenate([quartered_rows(one, col_grid) for one in grad_w_pairs[:-1]], axis=2),
    )
    early_piece = reduce_col(jnp.concatenate([early_dp, pairs_dp], axis=1))
    early_parts = spread_dp(early_piece)
    late = jnp.concatenate(
        [
            quartered_rows(grad_w_pairs[-1], col_grid),
            quartered_vector(bias_pair.astype(BF), vec_pad),
        ],
        axis=2,
    )
    late_parts = spread_dp(reduce_col(reduce_dp(late)))

    partial = right_inner(grad_qkv, w_qkv_half)
    arrived = swap(half_of(partial, 1 - row, 1).astype(BF)).astype(F32)
    grad_input = grad_first_features + half_of(partial, row, 1) + arrived

    cut_in = w_in.shape[0]
    cut_out = cut_in + w_out.shape[0] // 2
    cut_vec = cut_out + vec_pad
    if col_grid > 4:
        down_all = jnp.stack(picked(down_parts, "dp")).astype(F32)
        early_all = jnp.stack(picked(early_parts, "dp")).astype(F32)
        late_all = jnp.stack(picked(late_parts, "dp")).astype(F32)
        grad_down_own = rows_to_lanes(down_all, 2).reshape(w_down.shape)
        grad_in_own = rows_to_lanes(early_all[:, :cut_in], 4).reshape(w_in.shape)
        grad_out_own = rows_to_lanes(early_all[:, cut_in:cut_out], 2).reshape(w_out.shape)
        qkv_own = jnp.concatenate([early_all[:, cut_vec:], late_all[:, :-vec_pad]], axis=1)
        qkv_own = qkv_own.reshape(4, PAIRS, depth, 3, LANES)
        qkv_own = jnp.transpose(qkv_own, (0, 2, 3, 1, 4)).reshape(w_qkv.shape)
    else:
        grad_down_own = local_call(
            down_out_kernel, places, down_parts, jax.ShapeDtypeStruct(w_down.shape, F32)
        )
        grad_in_own, grad_out_own = local_call(
            in_out_kernel,
            places,
            early_parts,
            tuple(jax.ShapeDtypeStruct(one.shape, F32) for one in (w_in, w_out)),
        )
        qkv_own = local_call(
            functools.partial(qkv_out_kernel, cut_vec),
            places,
            early_parts + late_parts,
            jax.ShapeDtypeStruct((3, w_qkv.shape[0], WIDE), F32),
        )
        qkv_own = jnp.swapaxes(qkv_own, 0, 1)
    vec_own = first_quarter(early_parts, cut_out, vec_pad)
    vecs = [vec_own[i * share : (i + 1) * share] for i in range(6)]
    bias_in_own = vec_own[6 * share : 10 * share]
    bias_own = first_quarter(late_parts, depth, vec_pad)[: 2 * share].reshape(2, share)
    return (
        result,
        grad_input,
        qkv_own,
        bias_own,
        grad_out_own,
        vecs[0],
        vecs[1],
        vecs[2],
        grad_in_own,
        bias_in_own,
        grad_down_own,
        vecs[3],
        vecs[4],
        vecs[5],
    )


def solution(mesh):
    both = P(("row", "col"))
    specs = (
        P("col", None, "row"),
        P(None, ("row", "col")),
        P(("row", "col"), None),
        both,
        both,
        both,
        P("col", "row"),
        both,
        P(("row", "col"), None),
        both,
        both,
        both,
    )
    tokens = P(("dp", "col"), "row")
    return jax.shard_map(
        body,
        mesh=mesh,
        in_specs=(tokens, P("dp", None)) + specs + (tokens,),
        out_specs=(tokens, tokens) + specs,
        check_vma=False,
    )
```

```python
import functools

import jax
import jax.numpy as jnp
from jax import lax
from jax.experimental import pallas as pl
from jax.experimental.pallas import tpu as pltpu
from jax.sharding import PartitionSpec as P


D = 768
HD = 64
LEN = 2048
WIDE = 384
LANES = 128
PAIRS = WIDE // LANES

EPSILON = 1e-12
MASKED = -1e30
HALF_ROOT = 0.7071067811865476
DENSITY = 0.3989422804014327
BF = jnp.bfloat16
F32 = jnp.float32


def matmul(left_mat, right_mat):
    return jnp.dot(left_mat, right_mat, preferred_element_type=F32)


def left_inner(left_mat, right_mat):
    return lax.dot_general(
        left_mat, right_mat, (((0,), (0,)), ((), ())), preferred_element_type=F32
    )


def right_inner(left_mat, right_mat):
    return lax.dot_general(
        left_mat, right_mat, (((1,), (1,)), ((), ())), preferred_element_type=F32
    )


def swap(value):
    return lax.ppermute(value, "row", [(0, 1), (1, 0)])


def ordered(row, mine, other, axis):
    return jnp.where(
        row == 0,
        jnp.concatenate([mine, other], axis=axis),
        jnp.concatenate([other, mine], axis=axis),
    )


def half_of(value, which, axis):
    size = value.shape[axis] // 2
    return lax.dynamic_slice_in_dim(value, which * size, size, axis)


def to_tokens(value, row):
    return half_of(value, row, 0), swap(half_of(value, 1 - row, 0))


def to_features(value, row):
    other = swap(half_of(value, 1 - row, 1))
    return ordered(row, half_of(value, row, 1), other, 0)


def xor_swap(value, axis, mask):
    count = lax.axis_size(axis)
    return lax.ppermute(value, axis, [(i, i ^ mask) for i in range(count)])


def picked(parts, axis):
    stacked = jnp.stack(parts)
    own = lax.axis_index(axis)
    return [
        lax.dynamic_index_in_dim(stacked, own ^ i, 0, keepdims=False) for i in range(len(parts))
    ]


def gathered(value, axis):
    count = lax.axis_size(axis)
    if count > 4:
        return lax.all_gather(value, axis, axis=0)
    parts = [value] + [xor_swap(value, axis, k) for k in range(1, count)]
    return jnp.stack(picked(parts, axis))


def two_level(piece, used):
    arrived = []
    for k in range(1, lax.axis_size("col")):
        arrived.append(xor_swap(piece, "col", k))
    ours = jnp.stack([one[:used] for one in arrived])
    return arrived, [ours] + [xor_swap(ours, "dp", j) for j in range(1, 4)]


def reduce_dp(quarters):
    own = lax.axis_index("dp")

    def part(k):
        return lax.dynamic_index_in_dim(quarters, own ^ k, 1, keepdims=False)

    arrived = []
    for k in range(1, 4):
        arrived.append(xor_swap(part(k), "dp", k))
    total = part(0).astype(F32)
    for one in arrived:
        total = total + one.astype(F32)
    return total.astype(BF)


def reduce_col(ours):
    count = lax.axis_size("col")
    if count > 4:
        return lax.psum_scatter(ours, "col", scatter_dimension=0, tiled=False)
    own = lax.axis_index("col")

    def part(k):
        return lax.dynamic_index_in_dim(ours, own ^ k, 0, keepdims=False)

    arrived = []
    for k in range(1, count):
        arrived.append(xor_swap(part(k), "col", k))
    total = part(0).astype(F32)
    for one in arrived:
        total = total + one.astype(F32)
    return total.astype(BF)


def spread_dp(piece):
    parts = [piece]
    for k in range(1, 4):
        parts.append(xor_swap(piece, "dp", k))
    return parts


def places_of():
    return jnp.stack([lax.axis_index("col"), lax.axis_index("dp")]).astype(jnp.int32)


def at_rows(start, count):
    return pl.ds(pl.multiple_of(start, 16), count)


def local_call(kernel, places, inputs, outs):
    spec = pl.BlockSpec(memory_space=pltpu.VMEM)
    return pl.pallas_call(
        kernel,
        out_shape=outs,
        in_specs=[pl.BlockSpec(memory_space=pltpu.SMEM)] + [spec] * len(inputs),
        out_specs=jax.tree.map(lambda _: spec, outs),
        cost_estimate=pl.CostEstimate(flops=0, bytes_accessed=4 << 20, transcendentals=0),
    )(places, *inputs)


def qkv_kernel(places, own, *refs):
    parts, out = refs[:-1], refs[-1]
    col, dp = places[0], places[1]
    share = own.shape[1]
    depth = share // 4
    for kind in range(3):
        for pair in range(PAIRS):
            lanes = slice((3 * pair + kind) * LANES, (3 * pair + kind + 1) * LANES)
            source = slice(pair * LANES, (pair + 1) * LANES)
            out[at_rows(col * share, share), lanes] = own[kind, :, source]
            for j in range(4):
                for k in range(1, 4):
                    rows = at_rows((col ^ k) * share + (dp ^ j) * depth, depth)
                    out[rows, lanes] = parts[j][
                        k - 1, kind * depth : (kind + 1) * depth, source
                    ]


def later_kernel(places, own_down, own_in, own_out, *refs):
    parts, (down, inner, out) = refs[:-3], refs[-3:]
    col, dp = places[0], places[1]
    wide_rows, deep_rows, out_rows = own_down.shape[0], own_in.shape[0], own_out.shape[0]
    down[at_rows(col * wide_rows, wide_rows), :] = own_down[...]
    inner[at_rows(col * deep_rows, deep_rows), :] = own_in[...]
    out[at_rows(col * out_rows, out_rows), :] = own_out[...]
    for j in range(4):
        there = dp ^ j
        for k in range(1, 4):
            part = parts[j].at[k - 1]
            count, at = wide_rows // 4, 0
            rows = at_rows((col ^ k) * wide_rows + there * count, count)
            for i in range(2):
                down[rows, i * WIDE : (i + 1) * WIDE] = part[at : at + count, :]
                at += count
            count = deep_rows // 4
            rows = at_rows((col ^ k) * deep_rows + there * count, count)
            for i in range(4):
                inner[rows, i * WIDE : (i + 1) * WIDE] = part[at : at + count, :]
                at += count
            count = out_rows // 2
            rows = at_rows((col ^ k) * out_rows + lax.rem(there, 2) * count, count)
            lanes = pl.ds(pl.multiple_of(there // 2 * WIDE, LANES), WIDE)
            out[rows, lanes] = part[at : at + count, :]


def down_out_kernel(places, *refs):
    parts, down = refs[:-1], refs[-1]
    dp = places[1]
    count = down.shape[0] // 4
    for j in range(4):
        for i in range(2):
            down[at_rows((dp ^ j) * count, count), i * WIDE : (i + 1) * WIDE] = parts[j][
                i * count : (i + 1) * count, :
            ].astype(F32)


def in_out_kernel(places, *refs):
    parts, (inner, out) = refs[:-2], refs[-2:]
    dp = places[1]
    for j in range(4):
        there = dp ^ j
        count, at = inner.shape[0] // 4, 0
        for i in range(4):
            inner[at_rows(there * count, count), i * WIDE : (i + 1) * WIDE] = parts[j][
                at : at + count, :
            ].astype(F32)
            at += count
        count = out.shape[0] // 2
        lanes = pl.ds(pl.multiple_of(there // 2 * WIDE, LANES), WIDE)
        out[at_rows(lax.rem(there, 2) * count, count), lanes] = parts[j][
            at : at + count, :
        ].astype(F32)


def qkv_out_kernel(places, *refs):
    parts, out = refs[:-1], refs[-1]
    dp = places[1]
    count = out.shape[1] // 4
    for j in range(4):
        rows = at_rows((dp ^ j) * count, count)
        for pair in range(PAIRS):
            for kind in range(3):
                out[kind, rows, pair * LANES : (pair + 1) * LANES] = parts[j][
                    pair * count : (pair + 1) * count, kind * LANES : (kind + 1) * LANES
                ].astype(F32)


def quartered_rows(value, count):
    pieces = value.shape[1] // WIDE
    cut = value.reshape(count, 4, -1, value.shape[1])
    return jnp.concatenate(
        [cut[..., i * WIDE : (i + 1) * WIDE] for i in range(pieces)], axis=2
    )


def quartered_halves(value, count):
    cut = value.reshape(count, 2, -1, 2 * WIDE)
    return jnp.concatenate([cut[..., :WIDE], cut[..., WIDE:]], axis=1)


def quartered_vector(flat, rows):
    count, size = flat.shape
    return jnp.pad(flat, ((0, 0), (0, 4 * rows * WIDE - size))).reshape(count, 4, rows, WIDE)


def first_quarter(parts, start, rows):
    stacked = jnp.stack([one[start : start + rows] for one in parts])
    return lax.dynamic_index_in_dim(
        stacked, lax.axis_index("dp"), 0, keepdims=False
    ).astype(F32).reshape(-1)


def stack_heads(value):
    lane = lax.broadcasted_iota(jnp.int32, value.shape, 1)
    zero = jnp.zeros_like(value)
    return jnp.concatenate(
        [jnp.where(lane < HD, value, zero), jnp.where(lane >= HD, value, zero)], axis=0
    )


def join_heads(value, block):
    lane = lax.broadcasted_iota(jnp.int32, (LANES, block), 0)
    return jnp.where(lane < HD, value[:, :block], value[:, block:]).T


def doubled(value):
    return jnp.concatenate([value, value], axis=1)


def mask_bias(key_place, first_key, past_key):
    places = key_place + lax.broadcasted_iota(jnp.int32, (key_place_rows(), first_key.shape[1]), 0)
    inside = (places >= first_key) & (places < past_key)
    return doubled(jnp.where(inside, 0.0, MASKED))


KEY_BLOCK = 256


def key_place_rows():
    return KEY_BLOCK


def copy_blocks(dest, own, others, rows):
    dest[:rows, :] = own[...]
    dest[rows:, :] = others[...]


def forward_kernel(
    blocks, table, q_ref, k_ref, v_ref, ko_ref, vo_ref, span_ref, out_ref, log_ref, keys, values
):
    rows = q_ref.shape[0]
    block = rows // blocks
    copy_blocks(keys, k_ref, ko_ref, rows)
    copy_blocks(values, v_ref, vo_ref, rows)
    slots = keys.shape[0] // KEY_BLOCK
    base = table[2 * blocks]

    @pl.loop(0, blocks)
    def _(at):
        here = pl.ds(pl.multiple_of(at * block, block), block)
        wide = pl.ds(pl.multiple_of(at * 2 * block, 2 * block), 2 * block)
        query = stack_heads((q_ref[here, :].astype(F32) * 0.125).astype(BF))
        first_key = span_ref[0:1, here]
        past_key = span_ref[1:2, here]

        def step(place, running):
            peak, total, summed = running
            slot = lax.rem(place - base + slots, slots)
            rows_at = pl.ds(pl.multiple_of(slot * KEY_BLOCK, KEY_BLOCK), KEY_BLOCK)
            scores = right_inner(keys[rows_at, :], query)
            scores = scores + mask_bias(place * KEY_BLOCK, first_key, past_key)
            higher = jnp.maximum(peak, jnp.max(scores, axis=0, keepdims=True))
            raised = jnp.exp(scores - higher)
            fade = jnp.exp(peak - higher)
            total = total * fade + jnp.sum(raised, axis=0, keepdims=True)
            summed = summed * fade + left_inner(values[rows_at, :], raised.astype(BF))
            return (higher, total, summed)

        init = (
            jnp.full((1, 2 * block), MASKED, F32),
            jnp.zeros((1, 2 * block), F32),
            jnp.zeros((LANES, 2 * block), F32),
        )
        peak, total, summed = lax.fori_loop(table[at], table[blocks + at], step, init)
        out_ref[here, :] = join_heads(summed / total, block).astype(BF)
        log_ref[:, wide] = jnp.broadcast_to(
            peak + jnp.log(total), (8, 2 * block)
        )


def backward_block(blocks, rows, at, refs, key_at, spans_of_keys, before):
    q_ref, span_ref, out_ref, log_ref, grad_ref, keys, values, key_sum, value_sum = refs
    block = rows // blocks
    here = pl.ds(pl.multiple_of(at * block, block), block)
    wide = pl.ds(pl.multiple_of(at * 2 * block, 2 * block), 2 * block)
    query = stack_heads((q_ref[here, :].astype(F32) * 0.125).astype(BF))
    grad = stack_heads(grad_ref[here, :])
    along = (grad_ref[here, :].astype(F32) * out_ref[here, :].astype(F32)).T
    dots = jnp.concatenate(
        [
            jnp.sum(along[:HD], axis=0, keepdims=True),
            jnp.sum(along[HD:], axis=0, keepdims=True),
        ],
        axis=1,
    )
    logs = log_ref[0:1, wide]
    first_key = span_ref[0:1, here]
    past_key = span_ref[1:2, here]

    def step(place, summed):
        rows_at = pl.ds(pl.multiple_of(key_at(place) * KEY_BLOCK, KEY_BLOCK), KEY_BLOCK)
        key = keys[rows_at, :]
        scores = right_inner(key, query)
        scores = scores + mask_bias(place * KEY_BLOCK, first_key, past_key)
        weights = jnp.exp(scores - logs)
        grad_weights = right_inner(values[rows_at, :], grad)
        value_sum[rows_at, :] += matmul(weights.astype(BF), grad)
        grad_scores = (weights * (grad_weights - dots)).astype(BF)
        key_sum[rows_at, :] += matmul(grad_scores, query)
        return summed + left_inner(key, grad_scores)

    for low, high in spans_of_keys:
        before = lax.fori_loop(low, high, step, before)
    return here, before


def backward_others_kernel(
    blocks,
    table,
    q_ref,
    ko_ref,
    vo_ref,
    span_ref,
    out_ref,
    log_ref,
    grad_ref,
    dq_ref,
    others_ref,
    key_sum,
    value_sum,
):
    rows = q_ref.shape[0]
    block = rows // blocks
    own = rows // KEY_BLOCK
    slots = own + ko_ref.shape[0] // KEY_BLOCK
    base = table[2 * blocks]
    key_sum[...] = jnp.zeros_like(key_sum)
    value_sum[...] = jnp.zeros_like(value_sum)
    refs = (q_ref, span_ref, out_ref, log_ref, grad_ref, ko_ref, vo_ref, key_sum, value_sum)

    def key_at(place):
        return lax.rem(place - base + slots, slots) - own

    @pl.loop(0, blocks)
    def _(at):
        low, high = table[at], table[blocks + at]
        ranges = ((low, jnp.minimum(high, base)), (jnp.maximum(low, base + own), high))
        here, summed = backward_block(
            blocks, rows, at, refs, key_at, ranges, jnp.zeros((LANES, 2 * block), F32)
        )
        dq_ref[here, :] = join_heads(summed, block)

    others_ref[:, :LANES] = key_sum[...].astype(BF)
    others_ref[:, LANES:] = value_sum[...].astype(BF)


def backward_own_kernel(
    blocks,
    table,
    q_ref,
    k_ref,
    v_ref,
    span_ref,
    out_ref,
    log_ref,
    grad_ref,
    part_ref,
    dq_ref,
    dk_ref,
    dv_ref,
):
    rows = q_ref.shape[0]
    block = rows // blocks
    own = rows // KEY_BLOCK
    base = table[2 * blocks]
    dk_ref[...] = jnp.zeros_like(dk_ref)
    dv_ref[...] = jnp.zeros_like(dv_ref)
    refs = (q_ref, span_ref, out_ref, log_ref, grad_ref, k_ref, v_ref, dk_ref, dv_ref)

    @pl.loop(0, blocks)
    def _(at):
        low, high = table[at], table[blocks + at]
        ranges = ((jnp.maximum(low, base), jnp.minimum(high, base + own)),)
        here, summed = backward_block(
            blocks,
            rows,
            at,
            refs,
            lambda place: place - base,
            ranges,
            jnp.zeros((LANES, 2 * block), F32),
        )
        dq_ref[here, :] = ((part_ref[here, :] + join_heads(summed, block)) * 0.125).astype(BF)


def attention_specs(rows, others, pair):
    return [
        pl.BlockSpec((rows, LANES), lambda g, t: (0, 3 * pair)),
        pl.BlockSpec((rows, LANES), lambda g, t: (0, 3 * pair + 1)),
        pl.BlockSpec((rows, LANES), lambda g, t: (0, 3 * pair + 2)),
        pl.BlockSpec((others, LANES), lambda g, t: (0, 0)),
        pl.BlockSpec((others, LANES), lambda g, t: (0, 1)),
        pl.BlockSpec((8, rows), lambda g, t: (0, 0)),
    ]


def attend_forward(table, qkv, kv_others, spans, blocks, pair):
    rows, others = qkv.shape[0], kv_others.shape[0]
    return pl.pallas_call(
        functools.partial(forward_kernel, blocks),
        out_shape=(
            jax.ShapeDtypeStruct((rows, LANES), BF),
            jax.ShapeDtypeStruct((8, 2 * rows), F32),
        ),
        grid_spec=pltpu.PrefetchScalarGridSpec(
            num_scalar_prefetch=1,
            grid=(1,),
            in_specs=attention_specs(rows, others, pair),
            out_specs=(
                pl.BlockSpec((rows, LANES), lambda g, t: (0, 0)),
                pl.BlockSpec((8, 2 * rows), lambda g, t: (0, 0)),
            ),
            scratch_shapes=[pltpu.VMEM((rows + others, LANES), BF)] * 2,
        ),
        cost_estimate=pl.CostEstimate(
            flops=8 * rows * LEN * LANES, bytes_accessed=8 * rows * LANES, transcendentals=0
        ),
        name="attend_forward",
    )(table, qkv, qkv, qkv, kv_others, kv_others, spans)


def backward_call(kernel, table, inputs, in_specs, outs, out_specs, scratch, rows):
    return pl.pallas_call(
        kernel,
        out_shape=outs,
        grid_spec=pltpu.PrefetchScalarGridSpec(
            num_scalar_prefetch=1,
            grid=(1,),
            in_specs=in_specs,
            out_specs=out_specs,
            scratch_shapes=scratch,
        ),
        cost_estimate=pl.CostEstimate(
            flops=10 * rows * LEN * LANES, bytes_accessed=16 * rows * LANES, transcendentals=0
        ),
    )(table, *inputs)


def finish_kernel(dq_ref, dk_ref, dv_ref, *refs):
    arrived, (grad_ref, sum_ref) = refs[:-2], refs[-2:]
    key, value = dk_ref[...], dv_ref[...]
    for one in arrived:
        key = key + one[:, :LANES].astype(F32)
        value = value + one[:, LANES:].astype(F32)
    for i, part in enumerate((dq_ref[...], key.astype(BF), value.astype(BF))):
        lanes = slice(i * LANES, (i + 1) * LANES)
        grad_ref[:, lanes] = part
        total = jnp.sum(part.astype(F32), axis=0, keepdims=True)
        sum_ref[:, lanes] = jnp.broadcast_to(total, (8, LANES))


def finish_pair(grad_query, key_own, value_own, arrived):
    rows = grad_query.shape[0]
    spec = pl.BlockSpec(memory_space=pltpu.VMEM)
    grad_pair, sums = pl.pallas_call(
        finish_kernel,
        out_shape=(
            jax.ShapeDtypeStruct((rows, 3 * LANES), BF),
            jax.ShapeDtypeStruct((8, 3 * LANES), F32),
        ),
        in_specs=[spec] * (3 + len(arrived)),
        out_specs=(spec, spec),
        cost_estimate=pl.CostEstimate(flops=0, bytes_accessed=3 << 20, transcendentals=0),
        name="finish_pair",
    )(grad_query, key_own, value_own, *arrived)
    return grad_pair, sums[0]


def attend_backward_others(table, qkv, kv_others, spans, out, logs, grad, blocks, pair):
    rows, others = qkv.shape[0], kv_others.shape[0]
    specs = attention_specs(rows, others, pair)
    whole = pl.BlockSpec((rows, LANES), lambda g, t: (0, 0))
    mine = pl.BlockSpec((rows, LANES), lambda g, t: (0, pair))
    logs_spec = pl.BlockSpec((8, 2 * rows), lambda g, t: (0, 0))
    return backward_call(
        functools.partial(backward_others_kernel, blocks),
        table,
        (qkv, kv_others, kv_others, spans, out, logs, grad),
        [specs[0]] + specs[3:] + [whole, logs_spec, mine],
        (
            jax.ShapeDtypeStruct((rows, LANES), F32),
            jax.ShapeDtypeStruct((others, 2 * LANES), BF),
        ),
        (whole, pl.BlockSpec((others, 2 * LANES), lambda g, t: (0, 0))),
        [pltpu.VMEM((others, LANES), F32)] * 2,
        rows,
    )


def attend_backward_own(table, qkv, spans, out, logs, grad, part, blocks, pair):
    rows = qkv.shape[0]
    specs = attention_specs(rows, rows, pair)
    whole = pl.BlockSpec((rows, LANES), lambda g, t: (0, 0))
    mine = pl.BlockSpec((rows, LANES), lambda g, t: (0, pair))
    logs_spec = pl.BlockSpec((8, 2 * rows), lambda g, t: (0, 0))
    return backward_call(
        functools.partial(backward_own_kernel, blocks),
        table,
        (qkv, qkv, qkv, spans, out, logs, grad, part),
        specs[:3] + [specs[5], whole, logs_spec, mine, whole],
        (
            jax.ShapeDtypeStruct((rows, LANES), BF),
            jax.ShapeDtypeStruct((rows, LANES), F32),
            jax.ShapeDtypeStruct((rows, LANES), F32),
        ),
        (whole, whole, whole),
        [],
        rows,
    )


def norm_forward(summed, gain_vec, shift_vec):
    center = jnp.mean(summed, axis=1, keepdims=True)
    centered = summed - center
    spread = jnp.mean(centered * centered, axis=1, keepdims=True)
    inv_scale = lax.rsqrt(spread + EPSILON)
    normed_hat = centered * inv_scale
    return (normed_hat * gain_vec + shift_vec, normed_hat, inv_scale)


def norm_backward(grad_vals, normed_hat, inv_scale, gain_vec):
    grad_hat = grad_vals * gain_vec
    return inv_scale * (
        grad_hat
        - jnp.mean(grad_hat, axis=1, keepdims=True)
        - normed_hat * jnp.mean(grad_hat * normed_hat, axis=1, keepdims=True)
    )


def gelu_value(hidden):
    return 0.5 * hidden * (1.0 + lax.erf(hidden * HALF_ROOT))


def gelu_slope(hidden):
    return (
        0.5 * (1.0 + lax.erf(hidden * HALF_ROOT))
        + hidden * jnp.exp(-0.5 * hidden * hidden) * DENSITY
    )


def lanes_to_rows(value):
    pieces = value.shape[2] // WIDE
    return jnp.concatenate(
        [value[:, :, i * WIDE : (i + 1) * WIDE] for i in range(pieces)], axis=1
    )


def rows_to_lanes(value, pieces):
    rows = value.shape[-2] // pieces
    return jnp.concatenate(
        [value[..., i * rows : (i + 1) * rows, :] for i in range(pieces)], axis=-1
    )


def dp_part(value, own, axis=0):
    size = value.shape[axis] // 4
    return lax.dynamic_slice_in_dim(value, own * size, size, axis)


def padded_rows(flat, rows):
    count, size = flat.shape
    return jnp.pad(flat, ((0, 0), (0, rows * WIDE - size))).reshape(count, rows, WIDE)


def body(
    layer_input,
    lengths,
    w_qkv,
    bias_qv,
    w_out,
    bias_out,
    gain_attn,
    shift_attn,
    w_in,
    bias_in,
    w_down,
    bias_down,
    gain_ffn,
    shift_ffn,
    cotangent,
):
    col_grid = lax.axis_size("col")
    rows = layer_input.shape[0]
    row = lax.axis_index("row")
    own_dp = lax.axis_index("dp")
    own_col = lax.axis_index("col")
    group = LEN // rows
    start_row = own_col * rows
    block = min(256, rows)
    blocks = rows // block

    qkv_piece = jnp.swapaxes(dp_part(w_qkv, own_dp), 0, 1)
    depth = qkv_piece.shape[1]
    vectors = jnp.concatenate(
        [bias_out, gain_attn, shift_attn, bias_down, gain_ffn, shift_ffn, bias_in]
    )
    share = bias_out.shape[0]
    vector_rows = 16
    first_piece = jnp.concatenate(
        [
            qkv_piece.reshape(3 * depth, WIDE),
            jnp.pad(bias_qv, ((0, vector_rows - 2), (0, WIDE - share))),
        ],
        axis=0,
    )
    places = places_of()
    if col_grid > 4:
        first_cols = gathered(first_piece, "col")
        bias_col = first_cols[:, 3 * depth :]
        qkv_parts = gathered(first_cols[:, : 3 * depth], "dp")
        w_qkv_half = jnp.transpose(
            qkv_parts.reshape(4, col_grid, 3, depth, PAIRS, LANES), (1, 0, 3, 4, 2, 5)
        ).reshape(D, 3 * WIDE)
    else:
        first_arrived, first_parts = two_level(first_piece, 3 * depth)
        bias_col = jnp.stack(
            picked([one[3 * depth :] for one in [first_piece] + first_arrived], "col")
        )
        w_qkv_half = local_call(
            qkv_kernel,
            places,
            [jnp.swapaxes(w_qkv, 0, 1)] + first_parts,
            jax.ShapeDtypeStruct((D, 3 * WIDE), BF),
        )
    bias_q = bias_col[:, 0, :share].reshape(-1).astype(F32)
    bias_v = bias_col[:, 1, :share].reshape(-1).astype(F32)

    input_full = ordered(row, layer_input, swap(layer_input), 1)
    input_tokens = half_of(input_full, row, 0).astype(F32)
    cot_mine, cot_other = to_tokens(cotangent, row)
    grad_out = ordered(row, cot_mine, cot_other, 1).astype(F32)

    bias_rows = jnp.stack(
        [
            bias_q.reshape(PAIRS, LANES),
            jnp.zeros((PAIRS, LANES), F32),
            bias_v.reshape(PAIRS, LANES),
        ],
        axis=1,
    ).reshape(-1)
    qkv_low = (matmul(input_full, w_qkv_half) + bias_rows[None]).astype(BF)

    def group_perm(offset, back):
        pairs = []
        for i in range(col_grid):
            source = i // group * group + (i + offset) % group
            pairs.append((i, source) if back else (source, i))
        return pairs

    kv_others = []
    for pair in range(PAIRS):
        kv_local = qkv_low[:, (3 * pair + 1) * LANES : (3 * pair + 3) * LANES]
        arrived = [lax.ppermute(kv_local, "col", group_perm(j, False)) for j in range(1, group)]
        kv_others.append(jnp.concatenate(arrived, axis=0))

    down_piece = lanes_to_rows(dp_part(w_down, own_dp)[None])[0]
    in_piece = lanes_to_rows(dp_part(w_in, own_dp)[None])[0]
    if col_grid > 4:
        out_piece = lanes_to_rows(dp_part(w_out, own_dp)[None])[0]
        later_piece = jnp.concatenate([down_piece, in_piece, out_piece], axis=0)
        later_parts = gathered(gathered(later_piece, "col"), "dp")
        vectors_col = gathered(vectors, "col")
        cut_down = down_piece.shape[0]
        cut_in = cut_down + in_piece.shape[0]

        def whole_half(parts, pieces):
            joined = jnp.swapaxes(rows_to_lanes(parts, pieces), 0, 1)
            return joined.reshape(-1, joined.shape[-1])

        w_down_mine = whole_half(later_parts[:, :, :cut_down], 2)
        w_in_mine = whole_half(later_parts[:, :, cut_down:cut_in], 4)
        w_out_mine = whole_half(later_parts[:, :, cut_in:], 2)
    else:
        out_half = w_out.shape[0] // 2
        out_piece = lax.dynamic_slice(
            w_out, (own_dp % 2 * out_half, own_dp // 2 * WIDE), (out_half, WIDE)
        )
        used = down_piece.shape[0] + in_piece.shape[0] + out_half
        later_piece = jnp.concatenate(
            [down_piece, in_piece, out_piece, padded_rows(vectors[None], vector_rows)[0]], axis=0
        )
        later_arrived, later_parts = two_level(later_piece, used)
        vectors_col = jnp.stack(
            picked([one[used:] for one in [later_piece] + later_arrived], "col")
        )
        vectors_col = vectors_col.reshape(col_grid, -1)[:, : vectors.shape[0]]
        w_down_mine, w_in_mine, w_out_mine = local_call(
            later_kernel,
            places,
            [w_down, w_in, w_out] + later_parts,
            (
                jax.ShapeDtypeStruct((4 * w_down.shape[0], D), BF),
                jax.ShapeDtypeStruct((4 * w_in.shape[0], w_in.shape[1]), BF),
                jax.ShapeDtypeStruct((4 * w_out.shape[0], D), BF),
            ),
        )
    vectors_both = swap(vectors_col)

    def vector(at, count=1):
        mine = vectors_col[:, at * share : (at + count) * share].reshape(-1)
        other = vectors_both[:, at * share : (at + count) * share].reshape(-1)
        return mine.astype(F32), other.astype(F32)

    def whole_vector(at):
        mine, other = vector(at)
        return ordered(row, mine, other, 0)[None]

    bias_out_f = whole_vector(0)
    gain_attn_f = whole_vector(1)
    shift_attn_f = whole_vector(2)
    bias_down_f = whole_vector(3)
    gain_ffn_f = whole_vector(4)
    shift_ffn_f = whole_vector(5)
    bias_in_mine, bias_in_other = vector(6, 4)

    w_out_other, w_in_other, w_down_other = swap(w_out_mine), swap(w_in_mine), swap(w_down_mine)

    own_lengths = lax.dynamic_index_in_dim(lengths, start_row // LEN, 0, keepdims=False)
    ends = jnp.cumsum(own_lengths)
    first_place = start_row % LEN
    spots = first_place + jnp.arange(rows, dtype=jnp.int32)
    past = spots[:, None] >= ends[None, :]
    first_key = jnp.max(jnp.where(past, ends[None, :], 0), axis=1)
    past_key = jnp.min(jnp.where(past, LEN, ends[None, :]), axis=1)
    spans = jnp.pad(jnp.stack([first_key, past_key]), ((0, 6), (0, 0)))
    table = jnp.concatenate(
        [
            first_key[::block] // KEY_BLOCK,
            (past_key[block - 1 :: block] + (KEY_BLOCK - 1)) // KEY_BLOCK,
            (first_place // KEY_BLOCK)[None],
        ]
    ).astype(jnp.int32)

    attended = [
        attend_forward(table, qkv_low, kv_others[pair], spans, blocks, pair)
        for pair in range(PAIRS)
    ]
    att_mine, att_other = to_tokens(jnp.concatenate([out for out, _ in attended], axis=1), row)

    projected = matmul(att_mine, w_out_mine) + matmul(att_other, w_out_other)
    first_sum = input_tokens + projected + bias_out_f
    normed, first_hat, first_scale = norm_forward(first_sum, gain_attn_f, shift_attn_f)
    normed_low = normed.astype(BF)
    hidden_mine = matmul(normed_low, w_in_mine) + bias_in_mine[None]
    hidden_other = matmul(normed_low, w_in_other) + bias_in_other[None]
    act_mine = gelu_value(hidden_mine).astype(BF)
    act_other = gelu_value(hidden_other).astype(BF)
    second_sum = (
        normed
        + matmul(act_mine, w_down_mine)
        + matmul(act_other, w_down_other)
        + bias_down_f
    )
    result, second_hat, second_scale = norm_forward(second_sum, gain_ffn_f, shift_ffn_f)
    result = to_features(result.astype(BF), row)

    grad_gain_ffn = jnp.sum(grad_out * second_hat, axis=0)
    grad_shift_ffn = jnp.sum(grad_out, axis=0)
    grad_second = norm_backward(grad_out, second_hat, second_scale, gain_ffn_f)
    grad_bias_down = jnp.sum(grad_second, axis=0)
    grad_ffn = grad_second.astype(BF)
    grad_hidden_mine = (right_inner(grad_ffn, w_down_mine) * gelu_slope(hidden_mine)).astype(BF)
    grad_hidden_other = (right_inner(grad_ffn, w_down_other) * gelu_slope(hidden_other)).astype(BF)
    grad_normed = (
        grad_second
        + right_inner(grad_hidden_mine, w_in_mine)
        + right_inner(grad_hidden_other, w_in_other)
    )
    grad_gain_attn = jnp.sum(grad_normed * first_hat, axis=0)
    grad_shift_attn = jnp.sum(grad_normed, axis=0)
    grad_first = norm_backward(grad_normed, first_hat, first_scale, gain_attn_f)
    grad_bias_out = jnp.sum(grad_first, axis=0)
    grad_proj = grad_first.astype(BF)
    grad_att_mine = right_inner(grad_proj, w_out_mine).astype(BF)
    grad_att_other = right_inner(grad_proj, w_out_other).astype(BF)
    grad_attended = ordered(row, grad_att_mine, swap(grad_att_other), 0)
    grad_first_features = to_features(grad_first, row)

    def both_tokens(mine, other):
        return (mine + swap(other.astype(BF)).astype(F32)).astype(BF)

    grad_down = both_tokens(left_inner(act_mine, grad_ffn), left_inner(act_other, grad_ffn))
    down_dp = reduce_dp(quartered_rows(grad_down, col_grid))
    grad_in_mine = left_inner(normed_low, grad_hidden_mine)
    grad_in_other = left_inner(normed_low, grad_hidden_other).astype(BF)
    grad_in = both_tokens(grad_in_mine, grad_in_other)
    grad_out_w = both_tokens(left_inner(att_mine, grad_proj), left_inner(att_other, grad_proj))
    by_row = jnp.stack(
        [
            grad_bias_out,
            grad_gain_attn,
            grad_shift_attn,
            grad_bias_down,
            grad_gain_ffn,
            grad_shift_ffn,
        ]
    )
    in_mine = jnp.sum(grad_hidden_mine, axis=0, dtype=F32)
    in_other = jnp.sum(grad_hidden_other, axis=0, dtype=F32)

    def vector_block(six, inner):
        split = jnp.swapaxes(six.reshape(6, col_grid, share), 0, 1).reshape(col_grid, -1)
        return jnp.concatenate([split, inner.reshape(col_grid, -1)], axis=1)

    vec_mine = vector_block(half_of(by_row, row, 1), in_mine)
    vec_other = vector_block(half_of(by_row, 1 - row, 1), in_other)
    vec_sum = (vec_mine + swap(vec_other)).astype(BF)

    vec_pad = 16
    early = jnp.concatenate(
        [
            quartered_rows(grad_in, col_grid),
            quartered_halves(grad_out_w, col_grid)
            if col_grid <= 4
            else quartered_rows(grad_out_w, col_grid),
            quartered_vector(vec_sum, vec_pad),
        ],
        axis=2,
    )
    early, grad_attended = lax.optimization_barrier((early, grad_attended))
    early_parts = spread_dp(reduce_col(reduce_dp(early)))
    down_parts = spread_dp(reduce_col(down_dp))

    first_pass = []
    for pair in range(PAIRS):
        out, logs = attended[pair]
        first_pass.append(
            attend_backward_others(
                table, qkv_low, kv_others[pair], spans, out, logs, grad_attended, blocks, pair
            )
        )
    query_parts = lax.optimization_barrier(tuple(part for part, _ in first_pass))
    grad_pairs, grad_w_pairs, bias_sums = [], [], []
    query_parts = list(query_parts)
    for pair in range(PAIRS):
        out, logs = attended[pair]
        others = first_pass[pair][1]
        if pair:
            query_parts[pair], grad_query = lax.optimization_barrier(
                (query_parts[pair], grad_query)
            )
        grad_query, key_own, value_own = attend_backward_own(
            table, qkv_low, spans, out, logs, grad_attended, query_parts[pair], blocks, pair
        )
        arrived = [
            lax.ppermute(others[(j - 1) * rows : j * rows], "col", group_perm(j, True))
            for j in range(1, group)
        ]
        grad_pair, pair_sums = finish_pair(grad_query, key_own, value_own, arrived)
        grad_pairs.append(grad_pair)
        grad_w_pairs.append(left_inner(input_full, grad_pair).astype(BF))
        bias_sums.append(pair_sums)
    grad_qkv = jnp.concatenate(grad_pairs, axis=1)

    bias_pair = jnp.stack(
        [
            jnp.concatenate([one[:LANES] for one in bias_sums]),
            jnp.concatenate([one[2 * LANES :] for one in bias_sums]),
        ]
    )
    bias_pair = jnp.swapaxes(bias_pair.reshape(2, col_grid, share), 0, 1).reshape(col_grid, -1)
    pairs_dp = reduce_dp(
        jnp.concatenate([quartered_rows(one, col_grid) for one in grad_w_pairs[:-1]], axis=2),
    )
    late = jnp.concatenate(
        [
            quartered_rows(grad_w_pairs[-1], col_grid),
            quartered_vector(bias_pair.astype(BF), vec_pad),
        ],
        axis=2,
    )
    late_dp = jnp.concatenate([pairs_dp, reduce_dp(late)], axis=1)
    late_parts = spread_dp(reduce_col(late_dp))

    partial = right_inner(grad_qkv, w_qkv_half)
    arrived = swap(half_of(partial, 1 - row, 1).astype(BF)).astype(F32)
    grad_input = grad_first_features + half_of(partial, row, 1) + arrived

    cut_in = w_in.shape[0]
    cut_out = cut_in + w_out.shape[0] // 2
    if col_grid > 4:
        down_all = jnp.stack(picked(down_parts, "dp")).astype(F32)
        early_all = jnp.stack(picked(early_parts, "dp")).astype(F32)
        late_all = jnp.stack(picked(late_parts, "dp")).astype(F32)
        grad_down_own = rows_to_lanes(down_all, 2).reshape(w_down.shape)
        grad_in_own = rows_to_lanes(early_all[:, :cut_in], 4).reshape(w_in.shape)
        grad_out_own = rows_to_lanes(early_all[:, cut_in:cut_out], 2).reshape(w_out.shape)
        qkv_own = late_all[:, :-vec_pad].reshape(4, PAIRS, depth, 3, LANES)
        qkv_own = jnp.transpose(qkv_own, (0, 2, 3, 1, 4)).reshape(w_qkv.shape)
    else:
        grad_down_own = local_call(
            down_out_kernel, places, down_parts, jax.ShapeDtypeStruct(w_down.shape, F32)
        )
        grad_in_own, grad_out_own = local_call(
            in_out_kernel,
            places,
            early_parts,
            tuple(jax.ShapeDtypeStruct(one.shape, F32) for one in (w_in, w_out)),
        )
        qkv_own = local_call(
            qkv_out_kernel, places, late_parts, jax.ShapeDtypeStruct((3, w_qkv.shape[0], WIDE), F32)
        )
        qkv_own = jnp.swapaxes(qkv_own, 0, 1)
    vec_own = first_quarter(early_parts, cut_out, vec_pad)
    vecs = [vec_own[i * share : (i + 1) * share] for i in range(6)]
    bias_in_own = vec_own[6 * share : 10 * share]
    bias_own = first_quarter(late_parts, PAIRS * depth, vec_pad)[: 2 * share].reshape(2, share)
    return (
        result,
        grad_input,
        qkv_own,
        bias_own,
        grad_out_own,
        vecs[0],
        vecs[1],
        vecs[2],
        grad_in_own,
        bias_in_own,
        grad_down_own,
        vecs[3],
        vecs[4],
        vecs[5],
    )


def solution(mesh):
    both = P(("row", "col"))
    specs = (
        P("col", None, "row"),
        P(None, ("row", "col")),
        P(("row", "col"), None),
        both,
        both,
        both,
        P("col", "row"),
        both,
        P(("row", "col"), None),
        both,
        both,
        both,
    )
    tokens = P(("dp", "col"), "row")
    return jax.shard_map(
        body,
        mesh=mesh,
        in_specs=(tokens, P("dp", None)) + specs + (tokens,),
        out_specs=(tokens, tokens) + specs,
        check_vma=False,
    )
```

```python
import functools

import jax
import jax.numpy as jnp
from jax import lax
from jax.experimental import pallas as pl
from jax.experimental.pallas import tpu as pltpu
from jax.sharding import PartitionSpec as P


D = 768
HD = 64
LEN = 2048
WIDE = 384
LANES = 128
PAIRS = WIDE // LANES

EPSILON = 1e-12
MASKED = -1e30
HALF_ROOT = 0.7071067811865476
DENSITY = 0.3989422804014327
BF = jnp.bfloat16
F32 = jnp.float32


def matmul(left_mat, right_mat):
    return jnp.dot(left_mat, right_mat, preferred_element_type=F32)


def left_inner(left_mat, right_mat):
    return lax.dot_general(
        left_mat, right_mat, (((0,), (0,)), ((), ())), preferred_element_type=F32
    )


def right_inner(left_mat, right_mat):
    return lax.dot_general(
        left_mat, right_mat, (((1,), (1,)), ((), ())), preferred_element_type=F32
    )


def swap(value):
    return lax.ppermute(value, "row", [(0, 1), (1, 0)])


def ordered(row, mine, other, axis):
    return jnp.where(
        row == 0,
        jnp.concatenate([mine, other], axis=axis),
        jnp.concatenate([other, mine], axis=axis),
    )


def half_of(value, which, axis):
    size = value.shape[axis] // 2
    return lax.dynamic_slice_in_dim(value, which * size, size, axis)


def to_tokens(value, row):
    return half_of(value, row, 0), swap(half_of(value, 1 - row, 0))


def to_features(value, row):
    other = swap(half_of(value, 1 - row, 1))
    return ordered(row, half_of(value, row, 1), other, 0)


def xor_swap(value, axis, mask):
    count = lax.axis_size(axis)
    return lax.ppermute(value, axis, [(i, i ^ mask) for i in range(count)])


def picked(parts, axis):
    stacked = jnp.stack(parts)
    own = lax.axis_index(axis)
    return [
        lax.dynamic_index_in_dim(stacked, own ^ i, 0, keepdims=False) for i in range(len(parts))
    ]


def gathered(value, axis):
    count = lax.axis_size(axis)
    if count > 4:
        return lax.all_gather(value, axis, axis=0)
    parts = [value] + [xor_swap(value, axis, k) for k in range(1, count)]
    return jnp.stack(picked(parts, axis))


def two_level(piece, used):
    arrived = []
    for k in range(1, lax.axis_size("col")):
        arrived.append(xor_swap(piece, "col", k))
    ours = jnp.stack([one[:used] for one in arrived])
    return arrived, [ours] + [xor_swap(ours, "dp", j) for j in range(1, 4)]


def reduce_dp(quarters):
    own = lax.axis_index("dp")

    def part(k):
        return lax.dynamic_index_in_dim(quarters, own ^ k, 1, keepdims=False)

    arrived = []
    for k in range(1, 4):
        arrived.append(xor_swap(part(k), "dp", k))
    total = part(0).astype(F32)
    for one in arrived:
        total = total + one.astype(F32)
    return total.astype(BF)


def reduce_col(ours):
    count = lax.axis_size("col")
    if count > 4:
        return lax.psum_scatter(ours, "col", scatter_dimension=0, tiled=False)
    own = lax.axis_index("col")

    def part(k):
        return lax.dynamic_index_in_dim(ours, own ^ k, 0, keepdims=False)

    arrived = []
    for k in range(1, count):
        arrived.append(xor_swap(part(k), "col", k))
    total = part(0).astype(F32)
    for one in arrived:
        total = total + one.astype(F32)
    return total.astype(BF)


def spread_dp(piece):
    parts = [piece]
    for k in range(1, 4):
        parts.append(xor_swap(piece, "dp", k))
    return parts


def places_of():
    return jnp.stack([lax.axis_index("col"), lax.axis_index("dp")]).astype(jnp.int32)


def at_rows(start, count):
    return pl.ds(pl.multiple_of(start, 16), count)


def local_call(kernel, places, inputs, outs):
    spec = pl.BlockSpec(memory_space=pltpu.VMEM)
    return pl.pallas_call(
        kernel,
        out_shape=outs,
        in_specs=[pl.BlockSpec(memory_space=pltpu.SMEM)] + [spec] * len(inputs),
        out_specs=jax.tree.map(lambda _: spec, outs),
        cost_estimate=pl.CostEstimate(flops=0, bytes_accessed=4 << 20, transcendentals=0),
    )(places, *inputs)


def qkv_kernel(places, own, *refs):
    parts, out = refs[:-1], refs[-1]
    col, dp = places[0], places[1]
    share = own.shape[1]
    depth = share // 4
    for kind in range(3):
        for pair in range(PAIRS):
            lanes = slice((3 * pair + kind) * LANES, (3 * pair + kind + 1) * LANES)
            source = slice(pair * LANES, (pair + 1) * LANES)
            out[at_rows(col * share, share), lanes] = own[kind, :, source]
            for j in range(4):
                for k in range(1, 4):
                    rows = at_rows((col ^ k) * share + (dp ^ j) * depth, depth)
                    out[rows, lanes] = parts[j][
                        k - 1, kind * depth : (kind + 1) * depth, source
                    ]


def later_kernel(places, own_down, own_in, own_out, *refs):
    parts, (down, inner, out) = refs[:-3], refs[-3:]
    col, dp = places[0], places[1]
    wide_rows, deep_rows, out_rows = own_down.shape[0], own_in.shape[0], own_out.shape[0]
    down[at_rows(col * wide_rows, wide_rows), :] = own_down[...]
    inner[at_rows(col * deep_rows, deep_rows), :] = own_in[...]
    out[at_rows(col * out_rows, out_rows), :] = own_out[...]
    for j in range(4):
        there = dp ^ j
        for k in range(1, 4):
            part = parts[j].at[k - 1]
            count, at = wide_rows // 4, 0
            rows = at_rows((col ^ k) * wide_rows + there * count, count)
            for i in range(2):
                down[rows, i * WIDE : (i + 1) * WIDE] = part[at : at + count, :]
                at += count
            count = deep_rows // 4
            rows = at_rows((col ^ k) * deep_rows + there * count, count)
            for i in range(4):
                inner[rows, i * WIDE : (i + 1) * WIDE] = part[at : at + count, :]
                at += count
            count = out_rows // 2
            rows = at_rows((col ^ k) * out_rows + lax.rem(there, 2) * count, count)
            lanes = pl.ds(pl.multiple_of(there // 2 * WIDE, LANES), WIDE)
            out[rows, lanes] = part[at : at + count, :]


def down_out_kernel(places, *refs):
    parts, down = refs[:-1], refs[-1]
    dp = places[1]
    count = down.shape[0] // 4
    for j in range(4):
        for i in range(2):
            down[at_rows((dp ^ j) * count, count), i * WIDE : (i + 1) * WIDE] = parts[j][
                i * count : (i + 1) * count, :
            ].astype(F32)


def in_out_kernel(places, *refs):
    parts, (inner, out) = refs[:-2], refs[-2:]
    dp = places[1]
    for j in range(4):
        there = dp ^ j
        count, at = inner.shape[0] // 4, 0
        for i in range(4):
            inner[at_rows(there * count, count), i * WIDE : (i + 1) * WIDE] = parts[j][
                at : at + count, :
            ].astype(F32)
            at += count
        count = out.shape[0] // 2
        lanes = pl.ds(pl.multiple_of(there // 2 * WIDE, LANES), WIDE)
        out[at_rows(lax.rem(there, 2) * count, count), lanes] = parts[j][
            at : at + count, :
        ].astype(F32)


def qkv_out_kernel(first_row, places, *refs):
    parts, last_parts, out = refs[:4], refs[4:8], refs[8]
    dp = places[1]
    count = out.shape[1] // 4
    for j in range(4):
        rows = at_rows((dp ^ j) * count, count)
        for pair in range(PAIRS):
            source = last_parts[j] if pair == PAIRS - 1 else parts[j]
            start = 0 if pair == PAIRS - 1 else first_row + pair * count
            for kind in range(3):
                out[kind, rows, pair * LANES : (pair + 1) * LANES] = source[
                    start : start + count, kind * LANES : (kind + 1) * LANES
                ].astype(F32)


def quartered_rows(value, count):
    pieces = value.shape[1] // WIDE
    cut = value.reshape(count, 4, -1, value.shape[1])
    return jnp.concatenate(
        [cut[..., i * WIDE : (i + 1) * WIDE] for i in range(pieces)], axis=2
    )


def quartered_halves(value, count):
    cut = value.reshape(count, 2, -1, 2 * WIDE)
    return jnp.concatenate([cut[..., :WIDE], cut[..., WIDE:]], axis=1)


def quartered_vector(flat, rows):
    count, size = flat.shape
    return jnp.pad(flat, ((0, 0), (0, 4 * rows * WIDE - size))).reshape(count, 4, rows, WIDE)


def first_quarter(parts, start, rows):
    stacked = jnp.stack([one[start : start + rows] for one in parts])
    return lax.dynamic_index_in_dim(
        stacked, lax.axis_index("dp"), 0, keepdims=False
    ).astype(F32).reshape(-1)


def stack_heads(value):
    lane = lax.broadcasted_iota(jnp.int32, value.shape, 1)
    zero = jnp.zeros_like(value)
    return jnp.concatenate(
        [jnp.where(lane < HD, value, zero), jnp.where(lane >= HD, value, zero)], axis=0
    )


def join_heads(value, block):
    lane = lax.broadcasted_iota(jnp.int32, (LANES, block), 0)
    return jnp.where(lane < HD, value[:, :block], value[:, block:]).T


def doubled(value):
    return jnp.concatenate([value, value], axis=1)


def mask_bias(key_place, first_key, past_key):
    places = key_place + lax.broadcasted_iota(jnp.int32, (key_place_rows(), first_key.shape[1]), 0)
    inside = (places >= first_key) & (places < past_key)
    return doubled(jnp.where(inside, 0.0, MASKED))


KEY_BLOCK = 256


def key_place_rows():
    return KEY_BLOCK


def copy_blocks(dest, own, others, rows):
    dest[:rows, :] = own[...]
    dest[rows:, :] = others[...]


def forward_kernel(
    blocks, table, q_ref, k_ref, v_ref, ko_ref, vo_ref, span_ref, out_ref, log_ref, keys, values
):
    rows = q_ref.shape[0]
    block = rows // blocks
    copy_blocks(keys, k_ref, ko_ref, rows)
    copy_blocks(values, v_ref, vo_ref, rows)
    slots = keys.shape[0] // KEY_BLOCK
    base = table[2 * blocks]

    @pl.loop(0, blocks)
    def _(at):
        here = pl.ds(pl.multiple_of(at * block, block), block)
        wide = pl.ds(pl.multiple_of(at * 2 * block, 2 * block), 2 * block)
        query = stack_heads((q_ref[here, :].astype(F32) * 0.125).astype(BF))
        first_key = span_ref[0:1, here]
        past_key = span_ref[1:2, here]

        def step(place, running):
            peak, total, summed = running
            slot = lax.rem(place - base + slots, slots)
            rows_at = pl.ds(pl.multiple_of(slot * KEY_BLOCK, KEY_BLOCK), KEY_BLOCK)
            scores = right_inner(keys[rows_at, :], query)
            scores = scores + mask_bias(place * KEY_BLOCK, first_key, past_key)
            higher = jnp.maximum(peak, jnp.max(scores, axis=0, keepdims=True))
            raised = jnp.exp(scores - higher)
            fade = jnp.exp(peak - higher)
            total = total * fade + jnp.sum(raised, axis=0, keepdims=True)
            summed = summed * fade + left_inner(values[rows_at, :], raised.astype(BF))
            return (higher, total, summed)

        init = (
            jnp.full((1, 2 * block), MASKED, F32),
            jnp.zeros((1, 2 * block), F32),
            jnp.zeros((LANES, 2 * block), F32),
        )
        peak, total, summed = lax.fori_loop(table[at], table[blocks + at], step, init)
        out_ref[here, :] = join_heads(summed / total, block).astype(BF)
        log_ref[:, wide] = jnp.broadcast_to(
            peak + jnp.log(total), (8, 2 * block)
        )


def backward_block(blocks, rows, at, refs, key_at, spans_of_keys, before):
    q_ref, span_ref, out_ref, log_ref, grad_ref, keys, values, key_sum, value_sum = refs
    block = rows // blocks
    here = pl.ds(pl.multiple_of(at * block, block), block)
    wide = pl.ds(pl.multiple_of(at * 2 * block, 2 * block), 2 * block)
    query = stack_heads((q_ref[here, :].astype(F32) * 0.125).astype(BF))
    grad = stack_heads(grad_ref[here, :])
    along = (grad_ref[here, :].astype(F32) * out_ref[here, :].astype(F32)).T
    dots = jnp.concatenate(
        [
            jnp.sum(along[:HD], axis=0, keepdims=True),
            jnp.sum(along[HD:], axis=0, keepdims=True),
        ],
        axis=1,
    )
    logs = log_ref[0:1, wide]
    first_key = span_ref[0:1, here]
    past_key = span_ref[1:2, here]

    def step(place, summed):
        rows_at = pl.ds(pl.multiple_of(key_at(place) * KEY_BLOCK, KEY_BLOCK), KEY_BLOCK)
        key = keys[rows_at, :]
        scores = right_inner(key, query)
        scores = scores + mask_bias(place * KEY_BLOCK, first_key, past_key)
        weights = jnp.exp(scores - logs)
        grad_weights = right_inner(values[rows_at, :], grad)
        value_sum[rows_at, :] += matmul(weights.astype(BF), grad)
        grad_scores = (weights * (grad_weights - dots)).astype(BF)
        key_sum[rows_at, :] += matmul(grad_scores, query)
        return summed + left_inner(key, grad_scores)

    for low, high in spans_of_keys:
        before = lax.fori_loop(low, high, step, before)
    return here, before


def backward_others_kernel(
    blocks,
    table,
    q_ref,
    ko_ref,
    vo_ref,
    span_ref,
    out_ref,
    log_ref,
    grad_ref,
    dq_ref,
    others_ref,
    key_sum,
    value_sum,
):
    rows = q_ref.shape[0]
    block = rows // blocks
    own = rows // KEY_BLOCK
    slots = own + ko_ref.shape[0] // KEY_BLOCK
    base = table[2 * blocks]
    key_sum[...] = jnp.zeros_like(key_sum)
    value_sum[...] = jnp.zeros_like(value_sum)
    refs = (q_ref, span_ref, out_ref, log_ref, grad_ref, ko_ref, vo_ref, key_sum, value_sum)

    def key_at(place):
        return lax.rem(place - base + slots, slots) - own

    @pl.loop(0, blocks)
    def _(at):
        low, high = table[at], table[blocks + at]
        ranges = ((low, jnp.minimum(high, base)), (jnp.maximum(low, base + own), high))
        here, summed = backward_block(
            blocks, rows, at, refs, key_at, ranges, jnp.zeros((LANES, 2 * block), F32)
        )
        dq_ref[here, :] = join_heads(summed, block)

    others_ref[:, :LANES] = key_sum[...].astype(BF)
    others_ref[:, LANES:] = value_sum[...].astype(BF)


def backward_own_kernel(
    blocks,
    table,
    q_ref,
    k_ref,
    v_ref,
    span_ref,
    out_ref,
    log_ref,
    grad_ref,
    part_ref,
    dq_ref,
    dk_ref,
    dv_ref,
):
    rows = q_ref.shape[0]
    block = rows // blocks
    own = rows // KEY_BLOCK
    base = table[2 * blocks]
    dk_ref[...] = jnp.zeros_like(dk_ref)
    dv_ref[...] = jnp.zeros_like(dv_ref)
    refs = (q_ref, span_ref, out_ref, log_ref, grad_ref, k_ref, v_ref, dk_ref, dv_ref)

    @pl.loop(0, blocks)
    def _(at):
        low, high = table[at], table[blocks + at]
        ranges = ((jnp.maximum(low, base), jnp.minimum(high, base + own)),)
        here, summed = backward_block(
            blocks,
            rows,
            at,
            refs,
            lambda place: place - base,
            ranges,
            jnp.zeros((LANES, 2 * block), F32),
        )
        dq_ref[here, :] = ((part_ref[here, :] + join_heads(summed, block)) * 0.125).astype(BF)


def attention_specs(rows, others, pair):
    return [
        pl.BlockSpec((rows, LANES), lambda g, t: (0, 3 * pair)),
        pl.BlockSpec((rows, LANES), lambda g, t: (0, 3 * pair + 1)),
        pl.BlockSpec((rows, LANES), lambda g, t: (0, 3 * pair + 2)),
        pl.BlockSpec((others, LANES), lambda g, t: (0, 0)),
        pl.BlockSpec((others, LANES), lambda g, t: (0, 1)),
        pl.BlockSpec((8, rows), lambda g, t: (0, 0)),
    ]


def attend_forward(table, qkv, kv_others, spans, blocks, pair):
    rows, others = qkv.shape[0], kv_others.shape[0]
    return pl.pallas_call(
        functools.partial(forward_kernel, blocks),
        out_shape=(
            jax.ShapeDtypeStruct((rows, LANES), BF),
            jax.ShapeDtypeStruct((8, 2 * rows), F32),
        ),
        grid_spec=pltpu.PrefetchScalarGridSpec(
            num_scalar_prefetch=1,
            grid=(1,),
            in_specs=attention_specs(rows, others, pair),
            out_specs=(
                pl.BlockSpec((rows, LANES), lambda g, t: (0, 0)),
                pl.BlockSpec((8, 2 * rows), lambda g, t: (0, 0)),
            ),
            scratch_shapes=[pltpu.VMEM((rows + others, LANES), BF)] * 2,
        ),
        cost_estimate=pl.CostEstimate(
            flops=8 * rows * LEN * LANES, bytes_accessed=8 * rows * LANES, transcendentals=0
        ),
        name="attend_forward",
    )(table, qkv, qkv, qkv, kv_others, kv_others, spans)


def backward_call(kernel, table, inputs, in_specs, outs, out_specs, scratch, rows):
    return pl.pallas_call(
        kernel,
        out_shape=outs,
        grid_spec=pltpu.PrefetchScalarGridSpec(
            num_scalar_prefetch=1,
            grid=(1,),
            in_specs=in_specs,
            out_specs=out_specs,
            scratch_shapes=scratch,
        ),
        cost_estimate=pl.CostEstimate(
            flops=10 * rows * LEN * LANES, bytes_accessed=16 * rows * LANES, transcendentals=0
        ),
    )(table, *inputs)


def finish_kernel(dq_ref, dk_ref, dv_ref, *refs):
    arrived, (grad_ref, sum_ref) = refs[:-2], refs[-2:]
    key, value = dk_ref[...], dv_ref[...]
    for one in arrived:
        key = key + one[:, :LANES].astype(F32)
        value = value + one[:, LANES:].astype(F32)
    for i, part in enumerate((dq_ref[...], key.astype(BF), value.astype(BF))):
        lanes = slice(i * LANES, (i + 1) * LANES)
        grad_ref[:, lanes] = part
        total = jnp.sum(part.astype(F32), axis=0, keepdims=True)
        sum_ref[:, lanes] = jnp.broadcast_to(total, (8, LANES))


def finish_pair(grad_query, key_own, value_own, arrived):
    rows = grad_query.shape[0]
    spec = pl.BlockSpec(memory_space=pltpu.VMEM)
    grad_pair, sums = pl.pallas_call(
        finish_kernel,
        out_shape=(
            jax.ShapeDtypeStruct((rows, 3 * LANES), BF),
            jax.ShapeDtypeStruct((8, 3 * LANES), F32),
        ),
        in_specs=[spec] * (3 + len(arrived)),
        out_specs=(spec, spec),
        cost_estimate=pl.CostEstimate(flops=0, bytes_accessed=3 << 20, transcendentals=0),
        name="finish_pair",
    )(grad_query, key_own, value_own, *arrived)
    return grad_pair, sums[0]


def attend_backward_others(table, qkv, kv_others, spans, out, logs, grad, blocks, pair):
    rows, others = qkv.shape[0], kv_others.shape[0]
    specs = attention_specs(rows, others, pair)
    whole = pl.BlockSpec((rows, LANES), lambda g, t: (0, 0))
    mine = pl.BlockSpec((rows, LANES), lambda g, t: (0, pair))
    logs_spec = pl.BlockSpec((8, 2 * rows), lambda g, t: (0, 0))
    return backward_call(
        functools.partial(backward_others_kernel, blocks),
        table,
        (qkv, kv_others, kv_others, spans, out, logs, grad),
        [specs[0]] + specs[3:] + [whole, logs_spec, mine],
        (
            jax.ShapeDtypeStruct((rows, LANES), F32),
            jax.ShapeDtypeStruct((others, 2 * LANES), BF),
        ),
        (whole, pl.BlockSpec((others, 2 * LANES), lambda g, t: (0, 0))),
        [pltpu.VMEM((others, LANES), F32)] * 2,
        rows,
    )


def attend_backward_own(table, qkv, spans, out, logs, grad, part, blocks, pair):
    rows = qkv.shape[0]
    specs = attention_specs(rows, rows, pair)
    whole = pl.BlockSpec((rows, LANES), lambda g, t: (0, 0))
    mine = pl.BlockSpec((rows, LANES), lambda g, t: (0, pair))
    logs_spec = pl.BlockSpec((8, 2 * rows), lambda g, t: (0, 0))
    return backward_call(
        functools.partial(backward_own_kernel, blocks),
        table,
        (qkv, qkv, qkv, spans, out, logs, grad, part),
        specs[:3] + [specs[5], whole, logs_spec, mine, whole],
        (
            jax.ShapeDtypeStruct((rows, LANES), BF),
            jax.ShapeDtypeStruct((rows, LANES), F32),
            jax.ShapeDtypeStruct((rows, LANES), F32),
        ),
        (whole, whole, whole),
        [],
        rows,
    )


def norm_forward(summed, gain_vec, shift_vec):
    center = jnp.mean(summed, axis=1, keepdims=True)
    centered = summed - center
    spread = jnp.mean(centered * centered, axis=1, keepdims=True)
    inv_scale = lax.rsqrt(spread + EPSILON)
    normed_hat = centered * inv_scale
    return (normed_hat * gain_vec + shift_vec, normed_hat, inv_scale)


def norm_backward(grad_vals, normed_hat, inv_scale, gain_vec):
    grad_hat = grad_vals * gain_vec
    return inv_scale * (
        grad_hat
        - jnp.mean(grad_hat, axis=1, keepdims=True)
        - normed_hat * jnp.mean(grad_hat * normed_hat, axis=1, keepdims=True)
    )


def gelu_value(hidden):
    return 0.5 * hidden * (1.0 + lax.erf(hidden * HALF_ROOT))


def gelu_slope(hidden):
    return (
        0.5 * (1.0 + lax.erf(hidden * HALF_ROOT))
        + hidden * jnp.exp(-0.5 * hidden * hidden) * DENSITY
    )


def lanes_to_rows(value):
    pieces = value.shape[2] // WIDE
    return jnp.concatenate(
        [value[:, :, i * WIDE : (i + 1) * WIDE] for i in range(pieces)], axis=1
    )


def rows_to_lanes(value, pieces):
    rows = value.shape[-2] // pieces
    return jnp.concatenate(
        [value[..., i * rows : (i + 1) * rows, :] for i in range(pieces)], axis=-1
    )


def dp_part(value, own, axis=0):
    size = value.shape[axis] // 4
    return lax.dynamic_slice_in_dim(value, own * size, size, axis)


def padded_rows(flat, rows):
    count, size = flat.shape
    return jnp.pad(flat, ((0, 0), (0, rows * WIDE - size))).reshape(count, rows, WIDE)


def body(
    layer_input,
    lengths,
    w_qkv,
    bias_qv,
    w_out,
    bias_out,
    gain_attn,
    shift_attn,
    w_in,
    bias_in,
    w_down,
    bias_down,
    gain_ffn,
    shift_ffn,
    cotangent,
):
    col_grid = lax.axis_size("col")
    rows = layer_input.shape[0]
    row = lax.axis_index("row")
    own_dp = lax.axis_index("dp")
    own_col = lax.axis_index("col")
    group = LEN // rows
    start_row = own_col * rows
    block = min(512, rows)
    blocks = rows // block

    qkv_piece = jnp.swapaxes(dp_part(w_qkv, own_dp), 0, 1)
    depth = qkv_piece.shape[1]
    vectors = jnp.concatenate(
        [bias_out, gain_attn, shift_attn, bias_down, gain_ffn, shift_ffn, bias_in]
    )
    share = bias_out.shape[0]
    vector_rows = 16
    first_piece = jnp.concatenate(
        [
            qkv_piece.reshape(3 * depth, WIDE),
            jnp.pad(bias_qv, ((0, vector_rows - 2), (0, WIDE - share))),
        ],
        axis=0,
    )
    places = places_of()
    if col_grid > 4:
        first_cols = gathered(first_piece, "col")
        bias_col = first_cols[:, 3 * depth :]
        qkv_parts = gathered(first_cols[:, : 3 * depth], "dp")
        w_qkv_half = jnp.transpose(
            qkv_parts.reshape(4, col_grid, 3, depth, PAIRS, LANES), (1, 0, 3, 4, 2, 5)
        ).reshape(D, 3 * WIDE)
    else:
        first_arrived, first_parts = two_level(first_piece, 3 * depth)
        bias_col = jnp.stack(
            picked([one[3 * depth :] for one in [first_piece] + first_arrived], "col")
        )
        w_qkv_half = local_call(
            qkv_kernel,
            places,
            [jnp.swapaxes(w_qkv, 0, 1)] + first_parts,
            jax.ShapeDtypeStruct((D, 3 * WIDE), BF),
        )
    bias_q = bias_col[:, 0, :share].reshape(-1).astype(F32)
    bias_v = bias_col[:, 1, :share].reshape(-1).astype(F32)

    input_full = ordered(row, layer_input, swap(layer_input), 1)
    input_tokens = half_of(input_full, row, 0).astype(F32)
    cot_mine, cot_other = to_tokens(cotangent, row)
    grad_out = ordered(row, cot_mine, cot_other, 1).astype(F32)

    bias_rows = jnp.stack(
        [
            bias_q.reshape(PAIRS, LANES),
            jnp.zeros((PAIRS, LANES), F32),
            bias_v.reshape(PAIRS, LANES),
        ],
        axis=1,
    ).reshape(-1)
    qkv_low = (matmul(input_full, w_qkv_half) + bias_rows[None]).astype(BF)

    def group_perm(offset, back):
        pairs = []
        for i in range(col_grid):
            source = i // group * group + (i + offset) % group
            pairs.append((i, source) if back else (source, i))
        return pairs

    kv_others = []
    for pair in range(PAIRS):
        kv_local = qkv_low[:, (3 * pair + 1) * LANES : (3 * pair + 3) * LANES]
        arrived = [lax.ppermute(kv_local, "col", group_perm(j, False)) for j in range(1, group)]
        kv_others.append(jnp.concatenate(arrived, axis=0))

    down_piece = lanes_to_rows(dp_part(w_down, own_dp)[None])[0]
    in_piece = lanes_to_rows(dp_part(w_in, own_dp)[None])[0]
    if col_grid > 4:
        out_piece = lanes_to_rows(dp_part(w_out, own_dp)[None])[0]
        later_piece = jnp.concatenate([down_piece, in_piece, out_piece], axis=0)
        later_parts = gathered(gathered(later_piece, "col"), "dp")
        vectors_col = gathered(vectors, "col")
        cut_down = down_piece.shape[0]
        cut_in = cut_down + in_piece.shape[0]

        def whole_half(parts, pieces):
            joined = jnp.swapaxes(rows_to_lanes(parts, pieces), 0, 1)
            return joined.reshape(-1, joined.shape[-1])

        w_down_mine = whole_half(later_parts[:, :, :cut_down], 2)
        w_in_mine = whole_half(later_parts[:, :, cut_down:cut_in], 4)
        w_out_mine = whole_half(later_parts[:, :, cut_in:], 2)
    else:
        out_half = w_out.shape[0] // 2
        out_piece = lax.dynamic_slice(
            w_out, (own_dp % 2 * out_half, own_dp // 2 * WIDE), (out_half, WIDE)
        )
        used = down_piece.shape[0] + in_piece.shape[0] + out_half
        later_piece = jnp.concatenate(
            [down_piece, in_piece, out_piece, padded_rows(vectors[None], vector_rows)[0]], axis=0
        )
        later_arrived, later_parts = two_level(later_piece, used)
        vectors_col = jnp.stack(
            picked([one[used:] for one in [later_piece] + later_arrived], "col")
        )
        vectors_col = vectors_col.reshape(col_grid, -1)[:, : vectors.shape[0]]
        w_down_mine, w_in_mine, w_out_mine = local_call(
            later_kernel,
            places,
            [w_down, w_in, w_out] + later_parts,
            (
                jax.ShapeDtypeStruct((4 * w_down.shape[0], D), BF),
                jax.ShapeDtypeStruct((4 * w_in.shape[0], w_in.shape[1]), BF),
                jax.ShapeDtypeStruct((4 * w_out.shape[0], D), BF),
            ),
        )
    vectors_both = swap(vectors_col)

    def vector(at, count=1):
        mine = vectors_col[:, at * share : (at + count) * share].reshape(-1)
        other = vectors_both[:, at * share : (at + count) * share].reshape(-1)
        return mine.astype(F32), other.astype(F32)

    def whole_vector(at):
        mine, other = vector(at)
        return ordered(row, mine, other, 0)[None]

    bias_out_f = whole_vector(0)
    gain_attn_f = whole_vector(1)
    shift_attn_f = whole_vector(2)
    bias_down_f = whole_vector(3)
    gain_ffn_f = whole_vector(4)
    shift_ffn_f = whole_vector(5)
    bias_in_mine, bias_in_other = vector(6, 4)

    w_out_other, w_in_other, w_down_other = swap(w_out_mine), swap(w_in_mine), swap(w_down_mine)

    own_lengths = lax.dynamic_index_in_dim(lengths, start_row // LEN, 0, keepdims=False)
    ends = jnp.cumsum(own_lengths)
    first_place = start_row % LEN
    spots = first_place + jnp.arange(rows, dtype=jnp.int32)
    past = spots[:, None] >= ends[None, :]
    first_key = jnp.max(jnp.where(past, ends[None, :], 0), axis=1)
    past_key = jnp.min(jnp.where(past, LEN, ends[None, :]), axis=1)
    spans = jnp.pad(jnp.stack([first_key, past_key]), ((0, 6), (0, 0)))
    table = jnp.concatenate(
        [
            first_key[::block] // KEY_BLOCK,
            (past_key[block - 1 :: block] + (KEY_BLOCK - 1)) // KEY_BLOCK,
            (first_place // KEY_BLOCK)[None],
        ]
    ).astype(jnp.int32)

    attended = [
        attend_forward(table, qkv_low, kv_others[pair], spans, blocks, pair)
        for pair in range(PAIRS)
    ]
    att_mine, att_other = to_tokens(jnp.concatenate([out for out, _ in attended], axis=1), row)

    projected = matmul(att_mine, w_out_mine) + matmul(att_other, w_out_other)
    first_sum = input_tokens + projected + bias_out_f
    normed, first_hat, first_scale = norm_forward(first_sum, gain_attn_f, shift_attn_f)
    normed_low = normed.astype(BF)
    hidden_mine = matmul(normed_low, w_in_mine) + bias_in_mine[None]
    hidden_other = matmul(normed_low, w_in_other) + bias_in_other[None]
    act_mine = gelu_value(hidden_mine).astype(BF)
    act_other = gelu_value(hidden_other).astype(BF)
    second_sum = (
        normed
        + matmul(act_mine, w_down_mine)
        + matmul(act_other, w_down_other)
        + bias_down_f
    )
    result, second_hat, second_scale = norm_forward(second_sum, gain_ffn_f, shift_ffn_f)
    result = to_features(result.astype(BF), row)

    grad_gain_ffn = jnp.sum(grad_out * second_hat, axis=0)
    grad_shift_ffn = jnp.sum(grad_out, axis=0)
    grad_second = norm_backward(grad_out, second_hat, second_scale, gain_ffn_f)
    grad_bias_down = jnp.sum(grad_second, axis=0)
    grad_ffn = grad_second.astype(BF)
    grad_hidden_mine = (right_inner(grad_ffn, w_down_mine) * gelu_slope(hidden_mine)).astype(BF)
    grad_hidden_other = (right_inner(grad_ffn, w_down_other) * gelu_slope(hidden_other)).astype(BF)
    grad_normed = (
        grad_second
        + right_inner(grad_hidden_mine, w_in_mine)
        + right_inner(grad_hidden_other, w_in_other)
    )
    grad_gain_attn = jnp.sum(grad_normed * first_hat, axis=0)
    grad_shift_attn = jnp.sum(grad_normed, axis=0)
    grad_first = norm_backward(grad_normed, first_hat, first_scale, gain_attn_f)
    grad_bias_out = jnp.sum(grad_first, axis=0)
    grad_proj = grad_first.astype(BF)
    grad_att_mine = right_inner(grad_proj, w_out_mine).astype(BF)
    grad_att_other = right_inner(grad_proj, w_out_other).astype(BF)
    grad_attended = ordered(row, grad_att_mine, swap(grad_att_other), 0)
    grad_first_features = to_features(grad_first, row)

    def both_tokens(mine, other):
        return (mine + swap(other.astype(BF)).astype(F32)).astype(BF)

    grad_down = both_tokens(left_inner(act_mine, grad_ffn), left_inner(act_other, grad_ffn))
    down_dp = reduce_dp(quartered_rows(grad_down, col_grid))
    grad_in_mine = left_inner(normed_low, grad_hidden_mine)
    grad_in_other = left_inner(normed_low, grad_hidden_other).astype(BF)
    grad_in = both_tokens(grad_in_mine, grad_in_other)
    grad_out_w = both_tokens(left_inner(att_mine, grad_proj), left_inner(att_other, grad_proj))
    by_row = jnp.stack(
        [
            grad_bias_out,
            grad_gain_attn,
            grad_shift_attn,
            grad_bias_down,
            grad_gain_ffn,
            grad_shift_ffn,
        ]
    )
    in_mine = jnp.sum(grad_hidden_mine, axis=0, dtype=F32)
    in_other = jnp.sum(grad_hidden_other, axis=0, dtype=F32)

    def vector_block(six, inner):
        split = jnp.swapaxes(six.reshape(6, col_grid, share), 0, 1).reshape(col_grid, -1)
        return jnp.concatenate([split, inner.reshape(col_grid, -1)], axis=1)

    vec_mine = vector_block(half_of(by_row, row, 1), in_mine)
    vec_other = vector_block(half_of(by_row, 1 - row, 1), in_other)
    vec_sum = (vec_mine + swap(vec_other)).astype(BF)

    vec_pad = 16
    early = jnp.concatenate(
        [
            quartered_rows(grad_in, col_grid),
            quartered_halves(grad_out_w, col_grid)
            if col_grid <= 4
            else quartered_rows(grad_out_w, col_grid),
            quartered_vector(vec_sum, vec_pad),
        ],
        axis=2,
    )
    early, grad_attended = lax.optimization_barrier((early, grad_attended))
    early_dp = reduce_dp(early)
    down_parts = spread_dp(reduce_col(down_dp))

    first_pass = []
    for pair in range(PAIRS):
        out, logs = attended[pair]
        first_pass.append(
            attend_backward_others(
                table, qkv_low, kv_others[pair], spans, out, logs, grad_attended, blocks, pair
            )
        )
    query_parts = lax.optimization_barrier(tuple(part for part, _ in first_pass))
    grad_pairs, grad_w_pairs, bias_sums = [], [], []
    query_parts = list(query_parts)
    for pair in range(PAIRS):
        out, logs = attended[pair]
        others = first_pass[pair][1]
        if pair:
            query_parts[pair], grad_query = lax.optimization_barrier(
                (query_parts[pair], grad_query)
            )
        grad_query, key_own, value_own = attend_backward_own(
            table, qkv_low, spans, out, logs, grad_attended, query_parts[pair], blocks, pair
        )
        arrived = [
            lax.ppermute(others[(j - 1) * rows : j * rows], "col", group_perm(j, True))
            for j in range(1, group)
        ]
        grad_pair, pair_sums = finish_pair(grad_query, key_own, value_own, arrived)
        grad_pairs.append(grad_pair)
        grad_w_pairs.append(left_inner(input_full, grad_pair).astype(BF))
        bias_sums.append(pair_sums)
    grad_qkv = jnp.concatenate(grad_pairs, axis=1)

    bias_pair = jnp.stack(
        [
            jnp.concatenate([one[:LANES] for one in bias_sums]),
            jnp.concatenate([one[2 * LANES :] for one in bias_sums]),
        ]
    )
    bias_pair = jnp.swapaxes(bias_pair.reshape(2, col_grid, share), 0, 1).reshape(col_grid, -1)
    pairs_dp = reduce_dp(
        jnp.concatenate([quartered_rows(one, col_grid) for one in grad_w_pairs[:-1]], axis=2),
    )
    early_piece = reduce_col(jnp.concatenate([early_dp, pairs_dp], axis=1))
    early_parts = spread_dp(early_piece)
    late = jnp.concatenate(
        [
            quartered_rows(grad_w_pairs[-1], col_grid),
            quartered_vector(bias_pair.astype(BF), vec_pad),
        ],
        axis=2,
    )
    late_parts = spread_dp(reduce_col(reduce_dp(late)))

    partial = right_inner(grad_qkv, w_qkv_half)
    arrived = swap(half_of(partial, 1 - row, 1).astype(BF)).astype(F32)
    grad_input = grad_first_features + half_of(partial, row, 1) + arrived

    cut_in = w_in.shape[0]
    cut_out = cut_in + w_out.shape[0] // 2
    cut_vec = cut_out + vec_pad
    if col_grid > 4:
        down_all = jnp.stack(picked(down_parts, "dp")).astype(F32)
        early_all = jnp.stack(picked(early_parts, "dp")).astype(F32)
        late_all = jnp.stack(picked(late_parts, "dp")).astype(F32)
        grad_down_own = rows_to_lanes(down_all, 2).reshape(w_down.shape)
        grad_in_own = rows_to_lanes(early_all[:, :cut_in], 4).reshape(w_in.shape)
        grad_out_own = rows_to_lanes(early_all[:, cut_in:cut_out], 2).reshape(w_out.shape)
        qkv_own = jnp.concatenate([early_all[:, cut_vec:], late_all[:, :-vec_pad]], axis=1)
        qkv_own = qkv_own.reshape(4, PAIRS, depth, 3, LANES)
        qkv_own = jnp.transpose(qkv_own, (0, 2, 3, 1, 4)).reshape(w_qkv.shape)
    else:
        grad_down_own = local_call(
            down_out_kernel, places, down_parts, jax.ShapeDtypeStruct(w_down.shape, F32)
        )
        grad_in_own, grad_out_own = local_call(
            in_out_kernel,
            places,
            early_parts,
            tuple(jax.ShapeDtypeStruct(one.shape, F32) for one in (w_in, w_out)),
        )
        qkv_own = local_call(
            functools.partial(qkv_out_kernel, cut_vec),
            places,
            early_parts + late_parts,
            jax.ShapeDtypeStruct((3, w_qkv.shape[0], WIDE), F32),
        )
        qkv_own = jnp.swapaxes(qkv_own, 0, 1)
    vec_own = first_quarter(early_parts, cut_out, vec_pad)
    vecs = [vec_own[i * share : (i + 1) * share] for i in range(6)]
    bias_in_own = vec_own[6 * share : 10 * share]
    bias_own = first_quarter(late_parts, depth, vec_pad)[: 2 * share].reshape(2, share)
    return (
        result,
        grad_input,
        qkv_own,
        bias_own,
        grad_out_own,
        vecs[0],
        vecs[1],
        vecs[2],
        grad_in_own,
        bias_in_own,
        grad_down_own,
        vecs[3],
        vecs[4],
        vecs[5],
    )


def solution(mesh):
    both = P(("row", "col"))
    specs = (
        P("col", None, "row"),
        P(None, ("row", "col")),
        P(("row", "col"), None),
        both,
        both,
        both,
        P("col", "row"),
        both,
        P(("row", "col"), None),
        both,
        both,
        both,
    )
    tokens = P(("dp", "col"), "row")
    return jax.shard_map(
        body,
        mesh=mesh,
        in_specs=(tokens, P("dp", None)) + specs + (tokens,),
        out_specs=(tokens, tokens) + specs,
        check_vma=False,
    )
```
